256 devices in a mesh: group: 2 (over z_lo), row: 8 (over y, core), col: 16 (over z_hi, x).
Axes of the slice: x: 4, y: 4, z: 8 (z_hi: 4, z_lo: 2; z = z_hi * 2 + z_lo), core: 2. Of those that a mesh axis runs over, the one named last changes fastest.
Arguments:
- pair_repr: bfloat16 [256, 256, 128], P(('group', 'row'), 'col'), may hold values from -6 to 6
- pair_mask: int32 [256, 256], P(('group', 'row'), 'col'), may hold values 0 or 1
- chain_id: int32 [256], replicated, may hold values from 0 to 7, never falling along the last dimension, each value on 1 to 64 neighbouring positions
- tri_in_gain: float32 [128], replicated, may hold values from 0.5 to 1.5
- tri_proj: bfloat16 [128, 512], replicated, may hold values from -0.5 to 0.5
- tri_gate: bfloat16 [128, 128], replicated, may hold values from -0.5 to 0.5
- tri_out_gain: float32 [128], replicated, may hold values from 0.5 to 1.5
- tri_out: bfloat16 [128, 128], replicated, may hold values from -0.5 to 0.5
- bias_gain: float32 [128], replicated, may hold values from 0.5 to 1.5
- bias_weight: bfloat16 [128, 16], replicated, may hold values from -0.5 to 0.5
- chain_bias: float32 [16], replicated, may hold values from -2 to 2
- tokens: bfloat16 [48, 256, 768], P(('group', 'row')), may hold values from -6 to 6
- noise_level: int32 [48], P(('group', 'row')), may hold values from 0 to 199
- attn_gain: float32 [768], replicated, may hold values from 0.5 to 1.5
- attn_weight: bfloat16 [4, 768, 768], P(None, None, 'col'), may hold values from -0.21875 to 0.21875
- out_weight: bfloat16 [768, 768], P('col'), may hold values from -0.21875 to 0.21875
- cotangent: bfloat16 [48, 256, 768], P(('group', 'row')), may hold values from -6 to 6
Outputs:
- pair_next: bfloat16 [256, 256, 128], P(('group', 'row'), 'col')
- pair_grad: float32 [256, 256, 128], P(('group', 'row'), 'col')
- bias_weight_grad: float32 [128, 16], replicated
- denoised: bfloat16 [48, 256, 768], P(('group', 'row'), 'col')
- token_grad: bfloat16 [48, 256, 768], P(('group', 'row'), 'col')
- attn_weight_grad: float32 [4, 768, 768], P(None, ('group', 'row'), 'col')
- out_weight_grad: float32 [768, 768], P('col', ('group', 'row'))
The draws below stay inside these ranges and needn't reach their ends.
Inputs may be any that keep to these rules, and one draw needn't show every extreme that they name: `chain_id`: chain numbers never fall along the tokens.
All inputs are finite; a program needn't handle non-finite values. No bound on the sum of `pair_mask` on one device may be relied on, other than what follows from the above.
Results may differ from the reference program's by a relative error of at most 0.014.
Values may be sent and summed in bfloat16 or wider, within the bound.
A program may use at most 64 MiB of HBM per device.

```python
import math
import jax
import jax.numpy as jnp
import numpy as np
from jax import lax

C = 128
H = 16
D = 768
LEVELS = 200
CHAINS = 8
N = 256
COPIES = 48


def touch_ends(result, rng, least, largest):
    place = [jax.random.randint(jax.random.fold_in(rng, axis), (), 0, length) for axis, length in enumerate(result.shape)]
    longest = result.shape.index(max(result.shape))
    neighbour = place[:longest] + [(place[longest] + 1) % result.shape[longest]] + place[longest + 1:]
    return result.at[tuple(place)].set(least).at[tuple(neighbour)].set(largest)


def shard_levels(rng, dims, split, least, high):
    factor_of, own = 1.0, jax.random.fold_in(rng, 6)
    for dim, blocks in split:
        steps = jnp.exp(jax.random.uniform(jax.random.fold_in(own, dim), (blocks,), jnp.float32, least / len(split), high / len(split)))
        factor_of = factor_of * jnp.repeat(steps, dims[dim] // blocks).reshape([-1 if axis == dim else 1 for axis in range(len(dims))])
    return factor_of


def split_up(number_of, total, reach, lean):
    loads = [(1 << 20) // math.isqrt(standing ** lean) + 1 for standing in range(2, number_of + 1)]
    spare, counts = total - reach - (number_of - 1), [1] * (number_of - 1)
    while spare > 0:
        candidates = [i for i in range(number_of - 1) if counts[i] < reach]
        pool, left = sum([loads[i] for i in candidates]), spare
        for i in candidates:
            more = min(reach - counts[i], max(1, left * loads[i] // pool), spare)
            counts[i] = counts[i] + more
            spare = spare - more
    return np.array([reach] + counts)


def ragged_sizes(key, amount, total, reach, lean):
    if amount == 2:
        one = jax.random.randint(key, (), max(1, total - reach), min(reach, total - 1) + 1)
        return jnp.stack([one, total - one])
    lengths = jnp.asarray(split_up(amount, total, reach, lean), jnp.int32)
    pairs = (amount - 1) // 2
    giver, sink = lengths[1:1 + 2 * pairs:2], lengths[2:2 + 2 * pairs:2]
    margin = jnp.minimum(giver - 1, reach - sink)
    passed = jax.random.randint(jax.random.fold_in(key, 1), (pairs,), 0, 1 << 20) % (margin + 1)
    lengths = lengths.at[1:1 + 2 * pairs:2].set(giver - passed).at[2:2 + 2 * pairs:2].set(sink + passed)
    return lengths[jax.random.permutation(jax.random.fold_in(key, 2), amount)]


def normal_values(rng, dims, width, most, shards=(), kind=jnp.bfloat16):
    gain = shard_levels(rng, dims, shards, -0.22, 0.18) if shards else 1.0
    entries = jax.random.normal(rng, dims, jnp.float32) * width * gain
    return jnp.minimum(jnp.maximum(entries, -most), most).astype(kind)


def setup_inputs(seed: int = 0) -> dict:
    arg_keys = jax.random.split(jax.random.key(seed), 18)
    return {
        "pair_repr": normal_values(arg_keys[0], (N, N, C), 1.0, 6.0, ((0, 16), (1, 16))),
        "pair_mask": touch_ends((jax.random.randint(arg_keys[1], (N, N), 0, 4) < 3).astype(jnp.int32), jax.random.fold_in(arg_keys[1], 1), 0, 1),
        "chain_id": jnp.searchsorted(jnp.cumsum(ragged_sizes(arg_keys[2], CHAINS, N, N // 4, 1)), jnp.arange(N), side="right").astype(jnp.int32),
        "tri_in_gain": jnp.clip(1.0 + 0.1 * jax.random.normal(arg_keys[3], (C,), jnp.float32), 0.5, 1.5),
        "tri_proj": normal_values(arg_keys[4], (C, 4 * C), C ** -0.5, 0.5),
        "tri_gate": normal_values(arg_keys[5], (C, C), C ** -0.5, 0.5),
        "tri_out_gain": jnp.clip(1.0 + 0.1 * jax.random.normal(arg_keys[6], (C,), jnp.float32), 0.5, 1.5),
        "tri_out": normal_values(arg_keys[7], (C, C), C ** -0.5, 0.5),
        "bias_gain": jnp.clip(1.0 + 0.1 * jax.random.normal(arg_keys[8], (C,), jnp.float32), 0.5, 1.5),
        "bias_weight": normal_values(arg_keys[9], (C, H), C ** -0.5, 0.5),
        "chain_bias": jnp.clip(jax.random.uniform(arg_keys[10], (H,), jnp.float32, -2.0, 2.0), -2.0, 2.0),
        "tokens": normal_values(arg_keys[11], (COPIES, N, D), 1.0, 6.0, ((0, 16),)),
        "noise_level": touch_ends(jax.random.randint(arg_keys[12], (COPIES,), 0, LEVELS), jax.random.fold_in(arg_keys[12], 1), 0, LEVELS - 1).astype(jnp.int32),
        "attn_gain": jnp.clip(1.0 + 0.1 * jax.random.normal(arg_keys[13], (D,), jnp.float32), 0.5, 1.5),
        "attn_weight": normal_values(arg_keys[14], (4, D, D), D ** -0.5, 0.21875, ((2, 16),)),
        "out_weight": normal_values(arg_keys[15], (D, D), D ** -0.5, 0.21875, ((0, 16),)),
        "cotangent": normal_values(arg_keys[16], (COPIES, N, D), 1.0, 6.0, ((0, 16),)),
    }


EPSILON = 1e-05
SIGMA_LOW = 0.1
SIGMA_SPAN = 100.0

def normalize(values):
    average = lax.optimization_barrier(jnp.mean(values, -1, keepdims=True))
    centred = values - average
    return centred * lax.rsqrt(lax.optimization_barrier(jnp.mean(centred * centred, -1, keepdims=True)) + EPSILON)

def norm_back(gradient, values, norm_gain):
    average = lax.optimization_barrier(jnp.mean(values, -1, keepdims=True))
    centred = values - average
    inverse = lax.rsqrt(lax.optimization_barrier(jnp.mean(centred * centred, -1, keepdims=True)) + EPSILON)
    normed = centred * inverse
    weighted = gradient * norm_gain
    return inverse * (weighted - lax.optimization_barrier(jnp.mean(weighted, -1, keepdims=True)) - normed * lax.optimization_barrier(jnp.mean(weighted * normed, -1, keepdims=True)))

def noise_scale(levels):
    sigma_vals = SIGMA_LOW * SIGMA_SPAN ** (levels.astype(jnp.float32) / (LEVELS - 1))
    return lax.rsqrt(1.0 + sigma_vals * sigma_vals)

def reference(pair_repr, pair_mask, chain_id, tri_in_gain, tri_proj, tri_gate, tri_out_gain, tri_out, bias_gain, bias_weight, chain_bias, tokens, noise_level, attn_gain, attn_weight, out_weight, cotangent):
    highest_precision = lax.Precision.HIGHEST
    token_count = pair_repr.shape[0]
    channels = pair_repr.shape[2]
    heads_all = bias_weight.shape[1]
    hidden_width = attn_gain.shape[0]
    head_size = hidden_width // heads_all
    inverse_square_root = 1.0 / jnp.sqrt(jnp.float32(head_size))
    pair_tile = pair_repr.astype(jnp.float32)
    pair_in = (normalize(pair_tile) * tri_in_gain).astype(jnp.bfloat16)
    flat_in = pair_in.reshape(-1, channels)
    projected = jnp.dot(flat_in, tri_proj, preferred_element_type=jnp.float32).reshape(token_count, token_count, 4, channels)
    mask_tile = pair_mask.astype(jnp.float32)[:, :, None]
    left_proj = (jax.nn.sigmoid(projected[:, :, 0]) * projected[:, :, 1] * mask_tile).astype(jnp.bfloat16)
    right_proj = (jax.nn.sigmoid(projected[:, :, 2]) * projected[:, :, 3] * mask_tile).astype(jnp.bfloat16)
    gate_act = jax.nn.sigmoid(jnp.dot(flat_in, tri_gate, preferred_element_type=jnp.float32)).reshape(token_count, token_count, channels)
    triangle = jnp.einsum('ikc,jkc->ijc', left_proj.astype(jnp.float32), right_proj.astype(jnp.float32), precision=highest_precision)
    tri_normed = (normalize(triangle) * tri_out_gain).astype(jnp.bfloat16)
    update = jnp.dot(tri_normed.reshape(-1, channels), tri_out, preferred_element_type=jnp.float32).reshape(token_count, token_count, channels)
    updated = pair_tile + gate_act * update
    bias_in = (normalize(updated) * bias_gain).astype(jnp.bfloat16)
    flat_bias = bias_in.reshape(-1, channels)
    bias_tile = jnp.dot(flat_bias, bias_weight, preferred_element_type=jnp.float32).reshape(token_count, token_count, heads_all)
    same_chain = (chain_id[:, None] == chain_id[None, :]).astype(jnp.float32)
    bias_tile = bias_tile + same_chain[:, :, None] * chain_bias
    per_head_bias = jnp.transpose(bias_tile.astype(jnp.bfloat16), (2, 0, 1)).astype(jnp.float32)
    scales = noise_scale(noise_level)
    weight_f = attn_weight.astype(jnp.float32)

    def one_copy(carried, inputs):
        bias_sums, weight_sums, output_sums = carried
        token_rows, cot_rows, scaling = inputs
        sequence_length = token_rows.shape[0]
        scaled = scaling * token_rows.astype(jnp.float32)
        hidden = (normalize(scaled) * attn_gain).astype(jnp.bfloat16)
        projections = jnp.einsum('nd,gde->gne', hidden.astype(jnp.float32), weight_f, precision=highest_precision)
        query_rows = projections[0].astype(jnp.bfloat16).astype(jnp.float32).reshape(sequence_length, heads_all, head_size)
        key_matrix = projections[1].astype(jnp.bfloat16).astype(jnp.float32).reshape(sequence_length, heads_all, head_size)
        value_rows = projections[2].astype(jnp.bfloat16).astype(jnp.float32).reshape(sequence_length, heads_all, head_size)
        gate_sig = jax.nn.sigmoid(projections[3])
        logit_scores = jnp.einsum('fuc,suc->ufs', query_rows, key_matrix, precision=highest_precision) * inverse_square_root + per_head_bias
        exponent = jnp.exp(logit_scores)
        attention = exponent / lax.optimization_barrier(jnp.sum(exponent, -1, keepdims=True))
        attention_probs = attention.astype(jnp.bfloat16).astype(jnp.float32)
        attended_rows = jnp.einsum('vkq,qvy->kvy', attention_probs, value_rows, precision=highest_precision).reshape(sequence_length, hidden_width)
        gated_out = (gate_sig * attended_rows).astype(jnp.bfloat16)
        attn_out = jnp.dot(gated_out, out_weight, preferred_element_type=jnp.float32)
        denoised = (scaled + attn_out).astype(jnp.bfloat16)
        grad_gated = jnp.dot(cot_rows, out_weight.T, preferred_element_type=jnp.float32)
        grad_gate = grad_gated * attended_rows * gate_sig * (1.0 - gate_sig)
        attended_gradient = (grad_gated * gate_sig).astype(jnp.bfloat16).astype(jnp.float32).reshape(sequence_length, heads_all, head_size)
        probability_gradient = jnp.einsum('fuc,suc->ufs', attended_gradient, value_rows, precision=highest_precision)
        value_gradient = jnp.einsum('avj,vat->jat', attention_probs, attended_gradient, precision=highest_precision)
        grad_score = attention * (probability_gradient - lax.optimization_barrier(jnp.sum(attention * probability_gradient, -1, keepdims=True)))
        score_gradient = grad_score.astype(jnp.bfloat16).astype(jnp.float32)
        query_gradient = jnp.einsum('vkq,qvy->kvy', score_gradient, key_matrix, precision=highest_precision) * inverse_square_root
        key_gradient = jnp.einsum('avj,vat->jat', score_gradient, query_rows, precision=highest_precision) * inverse_square_root
        grads = jnp.stack([query_gradient.reshape(sequence_length, hidden_width), key_gradient.reshape(sequence_length, hidden_width), value_gradient.reshape(sequence_length, hidden_width), grad_gate]).astype(jnp.bfloat16).astype(jnp.float32)
        grad_hidden = jnp.einsum('gne,gde->nd', grads, weight_f, precision=highest_precision)
        grad_scaled = cot_rows.astype(jnp.float32) + norm_back(grad_hidden, scaled, attn_gain)
        token_grad = (scaling * grad_scaled).astype(jnp.bfloat16)
        weight_sums = weight_sums + jnp.einsum('nd,gne->gde', hidden.astype(jnp.float32), grads, precision=highest_precision)
        output_sums = output_sums + jnp.dot(gated_out.T, cot_rows, preferred_element_type=jnp.float32)
        return ((bias_sums + grad_score, weight_sums, output_sums), (denoised, token_grad))
    start_sums = (jnp.zeros((heads_all, token_count, token_count), jnp.float32), jnp.zeros(attn_weight.shape, jnp.float32), jnp.zeros(out_weight.shape, jnp.float32))
    final_sums, stacked = lax.scan(one_copy, start_sums, (tokens, cotangent, scales))
    bias_sums, weight_sums, output_sums = final_sums
    denoised, token_grad = stacked
    grad_bias = jnp.transpose(bias_sums, (1, 2, 0)).reshape(-1, heads_all)
    grad_in = jnp.dot(grad_bias, bias_weight.astype(jnp.float32).T, precision=highest_precision).reshape(token_count, token_count, channels)
    pair_grad = norm_back(grad_in, updated, bias_gain)
    bias_weight_grad = jnp.dot(flat_bias.astype(jnp.float32).T, grad_bias, precision=highest_precision)
    return (updated.astype(jnp.bfloat16), pair_grad, bias_weight_grad, denoised, token_grad, weight_sums, output_sums)
```

```python
import math

import jax
import jax.numpy as jnp
from jax import lax
from jax.experimental import pallas as pl
from jax.experimental.pallas import tpu as pltpu
from jax.sharding import PartitionSpec as P

MESH = pl.DeviceIdType.MESH
LEVELS = 200
EPSILON = 1e-05
SIGMA_LOW = 0.1
SIGMA_SPAN = 100.0
F32 = jnp.float32
BF16 = jnp.bfloat16
S = 16
C = 128
E = 48
D = 768
N = 256
T = 3
NT = (((1,), (1,)), ((), ()))
TN = (((0,), (0,)), ((), ()))


def iota(shape, dim):
    return lax.broadcasted_iota(jnp.int32, shape, dim)


def dot(a, b):
    return jnp.dot(a, b, preferred_element_type=F32)


def dot_nt(a, b):
    return lax.dot_general(a, b, NT, preferred_element_type=F32)


def dot_tn(a, b):
    return lax.dot_general(a, b, TN, preferred_element_type=F32)


def sigmoid(v):
    return 1.0 / (1.0 + jnp.exp(-v))


def centred_inverse(v):
    centred = v - jnp.mean(v, -1, keepdims=True)
    return centred, lax.rsqrt(jnp.mean(centred * centred, -1, keepdims=True) + EPSILON)


def norm_back(gradient, values, gain):
    centred, inverse = centred_inverse(values)
    normed = centred * inverse
    weighted = gradient * gain
    return inverse * (
        weighted
        - jnp.mean(weighted, -1, keepdims=True)
        - normed * jnp.mean(weighted * normed, -1, keepdims=True)
    )


def swap_blocks(x, unit):
    arr = iota(x.shape, 0) // S
    blk = iota(x.shape, 1) // unit
    for bit in (1, 2, 4, 8):
        rows = bit * S
        other = jnp.concatenate(
            [x[(k ^ 1) * rows : (k ^ 1) * rows + rows] for k in range(N // rows)], axis=0
        )
        up = pltpu.roll(other, bit * unit, 1)
        down = pltpu.roll(other, C - bit * unit, 1)
        in_arr, in_blk = (arr & bit) != 0, (blk & bit) != 0
        x = jnp.where(in_arr == in_blk, x, jnp.where(in_blk, up, down))
    return x


def kernel(
    pair, mask, chain, tri_in_gain, tri_proj, tri_gate, tri_out_gain, tri_out, bias_gain,
    bias_weight, chain_bias, tokens, level, attn_gain, attn_weight, out_weight, cot,
    pair_next, pair_grad, bias_weight_grad, denoised, token_grad, weight_grad,
    gate_scr, r_send, l_send, r_own, l_own, r_all, left_t, t_send, t_recv, row_scr, upd_scr,
    bias_in_scr, bw_pad, b_send, b_recv, b_all, w_four, ow_pad, place, w_all, hid_scr, qkv_scr,
    sig_scr, gg_scr, raw, raw_z, part, part_x, bs_send, bs_recv, bb_send, bb_recv, ws_send,
    ws_recv, ar_one, ar_all, ar_two, ar_fin,
    sem_r, sem_l, sem_ag, sem_fw, sem_t, sem_b, sem_ba, sem_w, sem_z, sem_x, sem_bs, sem_bb,
    sem_ws, sem_a1, sem_a2,
):
    group, row, col = lax.axis_index("group"), lax.axis_index("row"), lax.axis_index("col")
    mine = group * 8 + row
    core, high = row % 2, row // 2
    quad = group * 4 + high
    zed, ex = col // 4, col % 4
    pending = []

    def send(src, dst, sem, at, device):
        copy = pltpu.make_async_remote_copy(
            src_ref=src, dst_ref=dst, send_sem=sem.at[0, at], recv_sem=sem.at[1, at],
            device_id=device, device_id_type=MESH,
        )
        copy.start()
        pending.append(copy)
        return copy

    def to_col(step):
        return {"col": (col + step) % S}

    def to_line(step):
        there = (mine + step) % S
        return {"group": there // 8, "row": there % 8}

    barrier = pltpu.get_barrier_semaphore()
    for step in range(1, S):
        pl.semaphore_signal(barrier, inc=1, device_id=to_col(step), device_id_type=MESH)
        pl.semaphore_signal(barrier, inc=1, device_id=to_line(step), device_id_type=MESH)

    tile = pair[...].astype(F32).reshape(N, C)
    centred, inverse = centred_inverse(tile)
    pair_in = (centred * inverse * tri_in_gain[...]).astype(BF16)
    pick = (iota((N, S), 0) // S == iota((N, S), 1)).astype(BF16)
    spread = dot(pick, mask[...].astype(F32).astype(BF16))
    mask_col = jnp.sum(
        jnp.where(iota((N, S), 0) % S == iota((N, S), 1), spread, 0.0), -1, keepdims=True
    )
    right = dot(pair_in, tri_proj[:, 2 * C : 4 * C])
    right = sigmoid(right[:, :C]) * right[:, C:] * mask_col
    r_send[...] = swap_blocks(right, 8).astype(BF16).reshape(S, S, C)
    pl.semaphore_wait(barrier, 2 * (S - 1))
    r_copies = [
        send(r_send.at[(col + d) % S], r_own.at[col], sem_r, d, to_col(d)) for d in range(1, S)
    ]
    r_own[col] = r_send[col]
    left = dot(pair_in, tri_proj[:, : 2 * C])
    left = sigmoid(left[:, :C]) * left[:, C:] * mask_col
    l_send[...] = swap_blocks(left, 8).astype(BF16).reshape(S, S, C)
    l_copies = [
        send(l_send.at[(col + d) % S], l_own.at[col], sem_l, d, to_col(d)) for d in range(1, S)
    ]
    l_own[col] = l_send[col]
    gate_scr[...] = sigmoid(dot(pair_in, tri_gate[...]))

    w_four[...] = jnp.zeros_like(w_four)
    for g in range(4):
        w_four[:, g * C : g * C + E] = attn_weight[g]
    ow_pad[...] = jnp.zeros_like(ow_pad)
    ow_pad[:E, :] = out_weight[...]
    bw_pad[...] = jnp.zeros_like(bw_pad)
    bw_pad[:, :S] = bias_weight[...]
    place_row = iota((5 * C, N), 0)
    inner = place_row % C
    place[...] = jnp.where(
        (inner < E) & (iota((5 * C, N), 1) == place_row // C * E + inner), 1.0, 0.0
    ).astype(BF16)

    scale_of = []
    for t in range(T):
        power = jnp.full((1, C), level[t].astype(F32)) * (math.log(SIGMA_SPAN) / (LEVELS - 1))
        sigma = SIGMA_LOW * jnp.exp(power)
        scale_of.append(lax.rsqrt(1.0 + sigma * sigma)[:, :1])
    inverse_root = 1.0 / math.sqrt(E)

    def before_bias(t):
        scaled = tokens[t].astype(F32) * scale_of[t]
        mid, inv = centred_inverse(scaled)
        hidden = (mid * inv * attn_gain[...]).astype(BF16)
        hid_scr[t] = hidden
        projections = dot(hidden, w_four[...])
        for g in range(3):
            qkv_scr[t, g] = projections[:, g * C : (g + 1) * C].astype(BF16)
        sig_scr[t] = sigmoid(projections[:, 3 * C :])
        gg_scr[t] = dot_nt(cot[t], ow_pad[...])

    before_bias(0)

    for copy in r_copies:
        copy.wait_recv()
    ag = {
        k: send(
            r_own, r_all.at[mine], sem_ag, k,
            {"group": (quad + k) % 8 // 4, "row": (quad + k) % 4 * 2 + core},
        )
        for k in range(1, 8)
    }
    partner = {"row": high * 2 + 1 - core}
    fw = {0: send(r_own, r_all.at[mine], sem_fw, 0, partner)}
    before_bias(1)
    for copy in l_copies:
        copy.wait_recv()
    left_t[...] = l_own[...].reshape(N, C).astype(F32).T.astype(BF16)
    diagonal = iota((C, C), 0) % 8 == iota((C, C), 1) % 8

    def triangle(at, block):
        product = dot(left_t[...], block.reshape(N, C))
        product = jnp.where(diagonal, product, 0.0).reshape(S, 8, C)
        t_send[at] = jnp.sum(product, axis=1).astype(BF16)

    def from_quad(k, side):
        there = (quad + 8 - k) % 8
        return there // 4 * 8 + there % 4 * 2 + side

    triangle(mine, r_own[...])
    fw[0].wait_recv()
    triangle(from_quad(0, 1 - core), r_all[from_quad(0, 1 - core)])
    before_bias(2)
    for k in range(1, 8):
        ag[k].wait_recv()
        at = from_quad(k, core)
        fw[k] = send(r_all.at[at], r_all.at[at], sem_fw, k, partner)
        triangle(at, r_all[at])
    for k in range(1, 8):
        fw[k].wait_recv()
        at = from_quad(k, 1 - core)
        triangle(at, r_all[at])
    t_copies = [
        send(t_send.at[(col + d) % S], t_recv.at[col], sem_t, d, to_col(d)) for d in range(1, S)
    ]
    t_recv[col] = t_send[col]

    packed = dot(w_four[...], place[: 4 * C, :]) + dot_tn(ow_pad[...], place[4 * C :, :])
    w_all[zed] = packed.astype(BF16)

    for copy in t_copies:
        copy.wait_recv()
    moved = swap_blocks(t_recv[...].astype(F32).reshape(N, C), 8)
    for j in range(S):
        row_scr[pl.ds(j, S, stride=S), :] = moved[j * S : (j + 1) * S]
    centred, inverse = centred_inverse(row_scr[...])
    tri_normed = (centred * inverse * tri_out_gain[...]).astype(BF16)
    tile = pair[...].astype(F32).reshape(N, C)
    updated = tile + gate_scr[...] * dot(tri_normed, tri_out[...])
    upd_scr[...] = updated
    centred, inverse = centred_inverse(updated)
    bias_in = (centred * inverse * bias_gain[...]).astype(BF16)
    bias_in_scr[...] = bias_in
    row_scr[...] = dot(bias_in, bw_pad[...])
    by_col = jnp.concatenate([row_scr[pl.ds(j, S, stride=S), :] for j in range(S)], axis=0)
    by_head = swap_blocks(by_col, 1)
    ids = chain[...].astype(F32)
    here = mine * S + iota((N, N), 0) % S
    row_chain = jnp.sum(jnp.where(iota((N, N), 1) == here, ids, 0.0), -1, keepdims=True)
    ids_col = jnp.sum(
        jnp.where(iota((N, N), 1) == iota((N, N), 0), ids, 0.0), -1, keepdims=True
    )
    there = col * S + iota((N, C), 1)
    col_chain = jnp.sum(jnp.where(iota((N, C), 0) == there, ids_col, 0.0), 0, keepdims=True)
    head_bias = jnp.sum(
        jnp.where(iota((N, S), 1) == iota((N, S), 0) // S, chain_bias[...], 0.0),
        -1, keepdims=True,
    )
    by_head = by_head + jnp.where(row_chain == col_chain, head_bias, 0.0)
    b_send[...] = by_head.astype(BF16).reshape(S, S, C)
    b_copies = [
        send(b_send.at[(col + d) % S], b_recv.at[col], sem_b, d, to_col(d)) for d in range(1, S)
    ]
    b_recv[col] = b_send[col]
    pair_next[...] = updated.astype(BF16)
    lane_block = iota((S, C), 1) // S
    for copy in b_copies:
        copy.wait_recv()
    halves = []
    for half in range(2):
        joined = jnp.zeros((S, C), F32)
        for k in range(8):
            piece = b_recv[half * 8 + k].astype(F32)
            piece = pltpu.roll(piece, k * S, 1) if k else piece
            joined = jnp.where(lane_block == k, piece, joined)
        halves.append(joined)
    b_all[mine] = jnp.concatenate(halves, axis=1).astype(BF16)
    ba_copies = [
        send(b_all.at[mine], b_all.at[mine], sem_ba, d, to_line(d)) for d in range(1, S)
    ]
    w_copies = [
        send(w_all.at[zed], w_all.at[zed], sem_w, d, {"col": (zed + d) % 4 * 4 + ex})
        for d in range(1, 4)
    ]
    for copy in ba_copies:
        copy.wait_recv()

    bias_sum = None
    z_copies, x_copies = {}, {}
    for t in range(T):
        queries, keys, values = qkv_scr[t, 0], qkv_scr[t, 1], qkv_scr[t, 2]
        gate_sig, grad_gated = sig_scr[t], gg_scr[t]
        bias = b_all[...].reshape(N, N).astype(F32)
        exponent = jnp.exp(dot_nt(queries, keys) * inverse_root + bias)
        attention = exponent / jnp.sum(exponent, -1, keepdims=True)
        attention_b = attention.astype(BF16)
        attended = dot(attention_b, values)
        gated = (gate_sig * attended).astype(BF16)
        grad_gate = (grad_gated * attended * gate_sig * (1.0 - gate_sig)).astype(BF16)
        grad_attended = (grad_gated * gate_sig).astype(BF16)
        grad_prob = dot_nt(grad_attended, values)
        grad_values = dot_tn(attention_b, grad_attended).astype(BF16)
        grad_score = attention * (
            grad_prob - jnp.sum(attention * grad_prob, -1, keepdims=True)
        )
        score_b = grad_score.astype(BF16)
        bias_sum = grad_score if bias_sum is None else bias_sum + grad_score
        grad_queries = (dot(score_b, keys) * inverse_root).astype(BF16)
        grad_keys = (dot_tn(score_b, queries) * inverse_root).astype(BF16)
        side = jnp.concatenate([grad_queries, grad_keys, grad_values, grad_gate, gated], axis=1)
        raw[t] = dot(side, place[...]).astype(BF16).reshape(4, 64, N)
        z_copies[t] = [
            send(
                raw.at[t, (zed + d) % 4], raw_z.at[t, zed], sem_z, t * 4 + d,
                {"col": (zed + d) % 4 * 4 + ex},
            )
            for d in range(1, 4)
        ]
        raw_z[t, zed] = raw[t, zed]
    bs_send[...] = bias_sum.astype(BF16).reshape(S, S, N)
    bs_copies = [
        send(bs_send.at[(mine + d) % S], bs_recv.at[mine], sem_bs, d, to_line(d))
        for d in range(1, S)
    ]
    bs_recv[mine] = bs_send[mine]

    raw_t = raw[...].reshape(T * N, N).astype(F32).T.astype(BF16)
    grads_part = dot(raw_t[: 4 * E], hid_scr[...].reshape(T * N, D))
    out_part = dot(raw_t[4 * E :], cot[...].reshape(T * N, D))
    turned = jnp.concatenate([grads_part, out_part], axis=0).T
    ws_send[...] = turned.astype(BF16).reshape(S, E, N)
    ws_copies = [
        send(ws_send.at[(mine + d) % S], ws_recv.at[mine], sem_ws, d, to_line(d))
        for d in range(1, S)
    ]
    ws_recv[mine] = ws_send[mine]
    for copy in w_copies:
        copy.wait_recv()

    def project(t):
        for copy in z_copies[t]:
            copy.wait_recv()
        total = jnp.zeros((C, D), F32)
        first = iota((64, N), 1) < 4 * E
        for z in range(4):
            piece = raw_z[t, z].astype(F32)
            both = jnp.concatenate(
                [jnp.where(first, piece, 0.0), jnp.where(first, 0.0, piece)], axis=0
            ).astype(BF16)
            total = total + dot_nt(both, w_all[z])
        total = total.astype(BF16)
        for x in range(4):
            part[t, x, 0] = total[x * S : (x + 1) * S]
            part[t, x, 1] = total[64 + x * S : 64 + (x + 1) * S]
        x_copies[t] = [
            send(
                part.at[t, (ex + d) % 4], part_x.at[t, d - 1], sem_x, t * 4 + d,
                {"col": zed * 4 + (ex + d) % 4},
            )
            for d in range(1, 4)
        ]

    def finish(t):
        for copy in x_copies[t]:
            copy.wait_recv()
        sums = part[t, ex].astype(F32)
        for d in range(3):
            sums = sums + part_x[t, d].astype(F32)
        first = pl.multiple_of(col * S, S)
        scaled = tokens[t, pl.ds(first, S), :].astype(F32) * scale_of[t]
        cot_mine = cot[t, pl.ds(first, S), :].astype(F32)
        denoised[t] = (scaled + sums[1]).astype(BF16)
        back = norm_back(sums[0], scaled, attn_gain[...])
        token_grad[t] = (scale_of[t] * (cot_mine + back)).astype(BF16)

    project(0)
    for copy in bs_copies:
        copy.wait_recv()
    bias_rows = jnp.sum(bs_recv[...].astype(F32), axis=0)
    narrow = iota((S, C), 1) < S
    for k in range(S):
        piece = bias_rows[:, :C] if k < 8 else bias_rows[:, C:]
        piece = pltpu.roll(piece, C - k % 8 * S, 1) if k % 8 else piece
        bb_send[k] = jnp.where(narrow, piece, 0.0).astype(BF16)
    bb_copies = [
        send(bb_send.at[(col + d) % S], bb_recv.at[col], sem_bb, d, to_col(d))
        for d in range(1, S)
    ]
    bb_recv[col] = bb_send[col]
    project(1)
    project(2)
    for copy in bb_copies:
        copy.wait_recv()
    back = swap_blocks(bb_recv[...].astype(F32).reshape(N, C), 1)
    back = jnp.where(iota((N, C), 1) < S, back, 0.0)
    for j in range(S):
        row_scr[pl.ds(j, S, stride=S), :] = back[j * S : (j + 1) * S]
    grad_bias = row_scr[...].astype(BF16)
    ar_one[...] = dot_tn(grad_bias, bias_in_scr[...])[:S]
    a1_copies = [
        send(ar_one, ar_all.at[mine], sem_a1, d, to_line(d)) for d in range(1, S)
    ]
    ar_all[mine] = ar_one[...]
    grad_in = dot_nt(grad_bias, bw_pad[...])
    pair_grad[...] = norm_back(grad_in, upd_scr[...], bias_gain[...])
    finish(0)
    for copy in a1_copies:
        copy.wait_recv()
    ar_two[...] = jnp.sum(ar_all[...], axis=0)
    a2_copies = [
        send(ar_two, ar_fin.at[col], sem_a2, d, to_col(d)) for d in range(1, S)
    ]
    ar_fin[col] = ar_two[...]
    finish(1)
    finish(2)
    for copy in ws_copies:
        copy.wait_recv()
    weight_grad[...] = jnp.sum(ws_recv[...].astype(F32), axis=0)
    for copy in a2_copies:
        copy.wait_recv()
    bias_weight_grad[...] = jnp.sum(ar_fin[...], axis=0)
    for copy in pending:
        copy.wait_send()


def shards(
    pair_repr, pair_mask, chain_id, tri_in_gain, tri_proj, tri_gate, tri_out_gain, tri_out,
    bias_gain, bias_weight, chain_bias, tokens, noise_level, attn_gain, attn_weight, out_weight,
    cotangent,
):
    vmem = pl.BlockSpec(memory_space=pltpu.VMEM)
    smem = pl.BlockSpec(memory_space=pltpu.SMEM)

    def buf(*shape, kind=BF16):
        return pltpu.VMEM(shape, kind)

    def sems(count):
        return pltpu.SemaphoreType.DMA((2, count))

    outs = pl.pallas_call(
        kernel,
        out_shape=(
            jax.ShapeDtypeStruct((N, C), BF16),
            jax.ShapeDtypeStruct((N, C), F32),
            jax.ShapeDtypeStruct((S, C), F32),
            jax.ShapeDtypeStruct((T, S, D), BF16),
            jax.ShapeDtypeStruct((T, S, D), BF16),
            jax.ShapeDtypeStruct((E, N), F32),
        ),
        in_specs=[vmem] * 12 + [smem] + [vmem] * 4,
        out_specs=(vmem,) * 6,
        scratch_shapes=[
            buf(N, C, kind=F32),
            buf(S, S, C), buf(S, S, C), buf(S, S, C), buf(S, S, C),
            buf(S, S, S, C),
            buf(C, N),
            buf(S, S, C), buf(S, S, C),
            buf(N, C, kind=F32), buf(N, C, kind=F32),
            buf(N, C), buf(C, C),
            buf(S, S, C), buf(S, S, C), buf(S, S, N),
            buf(D, 4 * C), buf(C, D), buf(5 * C, N), buf(4, D, N),
            buf(T, N, D), buf(T, 3, N, C),
            buf(T, N, C, kind=F32), buf(T, N, C, kind=F32),
            buf(T, 4, 64, N), buf(T, 4, 64, N),
            buf(T, 4, 2, S, D), buf(T, 3, 2, S, D),
            buf(S, S, N), buf(S, S, N), buf(S, S, C), buf(S, S, C),
            buf(S, E, N), buf(S, E, N),
            buf(S, C, kind=F32), buf(S, S, C, kind=F32),
            buf(S, C, kind=F32), buf(S, S, C, kind=F32),
            sems(S), sems(S), sems(8), sems(8), sems(S), sems(S), sems(S), sems(4),
            sems(12), sems(12), sems(S), sems(S), sems(S), sems(S), sems(S),
        ],
        compiler_params=pltpu.CompilerParams(
            collective_id=0, has_side_effects=True, vmem_limit_bytes=60 * 1024 * 1024
        ),
    )(
        pair_repr, pair_mask, chain_id.reshape(1, N), tri_in_gain.reshape(1, C), tri_proj,
        tri_gate, tri_out_gain.reshape(1, C), tri_out, bias_gain.reshape(1, C), bias_weight,
        chain_bias.reshape(1, S), tokens, noise_level, attn_gain.reshape(1, D), attn_weight,
        out_weight, cotangent,
    )
    pair_next, pair_grad, bias_weight_grad, denoised, token_grad, weight_grad = outs
    grads = weight_grad[:, : 4 * E].reshape(E, 4, E)
    return (
        pair_next.reshape(S, S, C),
        pair_grad.reshape(S, S, C),
        bias_weight_grad.T,
        denoised,
        token_grad,
        jnp.transpose(grads, (1, 0, 2)),
        weight_grad[:, 4 * E : 5 * E].T,
    )


def solution(mesh):
    line, col = ("group", "row"), "col"
    return jax.shard_map(
        shards,
        mesh=mesh,
        in_specs=(
            P(line, col, None), P(line, col), P(), P(), P(), P(), P(), P(), P(), P(), P(),
            P(line, None, None), P(line), P(), P(None, None, col), P(col, None),
            P(line, None, None),
        ),
        out_specs=(
            P(line, col, None), P(line, col, None), P(), P(line, col, None),
            P(line, col, None), P(None, line, col), P(col, line),
        ),
        check_vma=False,
    )
```

```python
import math

import jax
import jax.numpy as jnp
from jax import lax
from jax.experimental import pallas as pl
from jax.experimental.pallas import tpu as pltpu
from jax.sharding import PartitionSpec as P

MESH = pl.DeviceIdType.MESH
LEVELS = 200
EPSILON = 1e-05
SIGMA_LOW = 0.1
SIGMA_SPAN = 100.0
F32 = jnp.float32
BF16 = jnp.bfloat16
S = 16
C = 128
E = 48
D = 768
N = 256
T = 3
NT = (((1,), (1,)), ((), ()))
TN = (((0,), (0,)), ((), ()))


def iota(shape, dim):
    return lax.broadcasted_iota(jnp.int32, shape, dim)


def dot(a, b):
    return jnp.dot(a, b, preferred_element_type=F32)


def dot_nt(a, b):
    return lax.dot_general(a, b, NT, preferred_element_type=F32)


def dot_tn(a, b):
    return lax.dot_general(a, b, TN, preferred_element_type=F32)


def sigmoid(v):
    return 1.0 / (1.0 + jnp.exp(-v))


def centred_inverse(v):
    centred = v - jnp.mean(v, -1, keepdims=True)
    return centred, lax.rsqrt(jnp.mean(centred * centred, -1, keepdims=True) + EPSILON)


def norm_back(gradient, values, gain):
    centred, inverse = centred_inverse(values)
    normed = centred * inverse
    weighted = gradient * gain
    return inverse * (
        weighted
        - jnp.mean(weighted, -1, keepdims=True)
        - normed * jnp.mean(weighted * normed, -1, keepdims=True)
    )


def swap_blocks(x, unit):
    arr = iota(x.shape, 0) // S
    blk = iota(x.shape, 1) // unit
    for bit in (1, 2, 4, 8):
        rows = bit * S
        other = jnp.concatenate(
            [x[(k ^ 1) * rows : (k ^ 1) * rows + rows] for k in range(N // rows)], axis=0
        )
        up = pltpu.roll(other, bit * unit, 1)
        down = pltpu.roll(other, C - bit * unit, 1)
        in_arr, in_blk = (arr & bit) != 0, (blk & bit) != 0
        x = jnp.where(in_arr == in_blk, x, jnp.where(in_blk, up, down))
    return x


def kernel(
    pair, mask, chain, tri_in_gain, tri_proj, tri_gate, tri_out_gain, tri_out, bias_gain,
    bias_weight, chain_bias, tokens, level, attn_gain, attn_weight, out_weight, cot,
    pair_next, pair_grad, bias_weight_grad, denoised, token_grad, weight_grad,
    gate_scr, r_send, l_send, r_own, l_own, r_all, left_t, t_send, t_recv, row_scr, upd_scr,
    bias_in_scr, bw_pad, b_send, b_recv, b_all, w_four, ow_pad, place, w_own, w_rem, hid_scr, qkv_scr,
    sig_scr, gg_scr, raw, raw_z, part, part_x, bs_send, bs_recv, bb_send, bb_recv, ws_send,
    ws_recv, ar_one, ar_all, ar_two, ar_fin,
    sem_r, sem_l, sem_ag, sem_fw, sem_t, sem_b, sem_ba, sem_w, sem_wg, sem_wf, sem_z, sem_x,
    sem_bs, sem_bb, sem_ws, sem_a1, sem_a2,
):
    group, row, col = lax.axis_index("group"), lax.axis_index("row"), lax.axis_index("col")
    mine = group * 8 + row
    core, high = row % 2, row // 2
    quad = group * 4 + high
    zed, ex = col // 4, col % 4
    pending = []

    def send(src, dst, sem, at, device):
        copy = pltpu.make_async_remote_copy(
            src_ref=src, dst_ref=dst, send_sem=sem.at[0, at], recv_sem=sem.at[1, at],
            device_id=device, device_id_type=MESH,
        )
        copy.start()
        pending.append(copy)
        return copy

    def to_col(step):
        return {"col": (col + step) % S}

    def to_line(step):
        there = (mine + step) % S
        return {"group": there // 8, "row": there % 8}

    barrier = pltpu.get_barrier_semaphore()
    for step in range(1, S):
        pl.semaphore_signal(barrier, inc=1, device_id=to_col(step), device_id_type=MESH)
        pl.semaphore_signal(barrier, inc=1, device_id=to_line(step), device_id_type=MESH)

    tile = pair[...].astype(F32).reshape(N, C)
    centred, inverse = centred_inverse(tile)
    pair_in = (centred * inverse * tri_in_gain[...]).astype(BF16)
    pick = (iota((N, S), 0) // S == iota((N, S), 1)).astype(BF16)
    spread = dot(pick, mask[...].astype(F32).astype(BF16))
    mask_col = jnp.sum(
        jnp.where(iota((N, S), 0) % S == iota((N, S), 1), spread, 0.0), -1, keepdims=True
    )
    right = dot(pair_in, tri_proj[:, 2 * C : 4 * C])
    right = sigmoid(right[:, :C]) * right[:, C:] * mask_col
    r_send[...] = swap_blocks(right, 8).astype(BF16).reshape(S, S, C)
    pl.semaphore_wait(barrier, 2 * (S - 1))
    r_copies = [
        send(r_send.at[(col + d) % S], r_own.at[col], sem_r, d, to_col(d)) for d in range(1, S)
    ]
    r_own[col] = r_send[col]
    left = dot(pair_in, tri_proj[:, : 2 * C])
    left = sigmoid(left[:, :C]) * left[:, C:] * mask_col
    l_send[...] = swap_blocks(left, 8).astype(BF16).reshape(S, S, C)
    l_copies = [
        send(l_send.at[(col + d) % S], l_own.at[col], sem_l, d, to_col(d)) for d in range(1, S)
    ]
    l_own[col] = l_send[col]
    gate_scr[...] = sigmoid(dot(pair_in, tri_gate[...]))

    for g in range(4):
        w_own[3 * g : 3 * g + 3] = attn_weight[g].reshape(3, S, D)
    w_own[12:15] = out_weight[...].reshape(3, S, D)
    w_own[15] = jnp.zeros((S, D), BF16)
    w_copies = [
        send(w_own.at[mine], w_rem.at[mine, d - 1], sem_w, d, {"col": (zed + 4 - d) % 4 * 4 + ex})
        for d in range(1, 4)
    ]
    w_four[...] = jnp.zeros_like(w_four)
    for g in range(4):
        w_four[g * C : g * C + E, :] = attn_weight[g]
    ow_pad[...] = jnp.zeros_like(ow_pad)
    ow_pad[:E, :] = out_weight[...]
    bw_pad[...] = jnp.zeros_like(bw_pad)
    bw_pad[:S, :] = bias_weight[...]
    place_row = iota((5 * C, N), 0)
    inner = place_row % C
    place[...] = jnp.where(
        (inner < E) & (iota((5 * C, N), 1) == place_row // C * E + inner), 1.0, 0.0
    ).astype(BF16)

    scale_of = []
    for t in range(T):
        power = jnp.full((1, C), level[t].astype(F32)) * (math.log(SIGMA_SPAN) / (LEVELS - 1))
        sigma = SIGMA_LOW * jnp.exp(power)
        scale_of.append(lax.rsqrt(1.0 + sigma * sigma)[:, :1])
    inverse_root = 1.0 / math.sqrt(E)

    def before_bias(t):
        scaled = tokens[t].astype(F32) * scale_of[t]
        mid, inv = centred_inverse(scaled)
        hidden = (mid * inv * attn_gain[...].reshape(1, D)).astype(BF16)
        hid_scr[t] = hidden
        projections = dot_nt(hidden, w_four[...])
        for g in range(3):
            qkv_scr[t, g] = projections[:, g * C : (g + 1) * C].astype(BF16)
        sig_scr[t] = sigmoid(projections[:, 3 * C :])
        gg_scr[t] = dot_nt(cot[t], ow_pad[...])

    before_bias(0)

    for copy in r_copies:
        copy.wait_recv()
    ag = {
        k: send(
            r_own, r_all.at[mine], sem_ag, k,
            {"group": (quad + k) % 8 // 4, "row": (quad + k) % 4 * 2 + core},
        )
        for k in range(1, 8)
    }
    partner = {"row": high * 2 + 1 - core}
    fw = {0: send(r_own, r_all.at[mine], sem_fw, 0, partner)}
    before_bias(1)
    for copy in l_copies:
        copy.wait_recv()
    left_t[...] = l_own[...].reshape(N, C).astype(F32).T.astype(BF16)
    diagonal = iota((C, C), 0) % 8 == iota((C, C), 1) % 8

    def triangle(at, block):
        product = dot(left_t[...], block.reshape(N, C))
        product = jnp.where(diagonal, product, 0.0).reshape(S, 8, C)
        t_send[at] = jnp.sum(product, axis=1).astype(BF16)

    def from_quad(k, side):
        there = (quad + 8 - k) % 8
        return there // 4 * 8 + there % 4 * 2 + side

    triangle(mine, r_own[...])
    fw[0].wait_recv()
    triangle(from_quad(0, 1 - core), r_all[from_quad(0, 1 - core)])
    before_bias(2)
    for k in range(1, 8):
        ag[k].wait_recv()
        at = from_quad(k, core)
        fw[k] = send(r_all.at[at], r_all.at[at], sem_fw, k, partner)
        triangle(at, r_all[at])
    for k in range(1, 8):
        fw[k].wait_recv()
        at = from_quad(k, 1 - core)
        triangle(at, r_all[at])
    t_copies = [
        send(t_send.at[(col + d) % S], t_recv.at[col], sem_t, d, to_col(d)) for d in range(1, S)
    ]
    t_recv[col] = t_send[col]

    for copy in w_copies:
        copy.wait_recv()
    wg = [
        send(
            w_rem.at[mine], w_rem.at[mine], sem_wg, k,
            {"group": (quad + k) % 8 // 4, "row": (quad + k) % 4 * 2 + core},
        )
        for k in range(1, 8)
    ]
    wf = [send(w_rem.at[mine], w_rem.at[mine], sem_wf, 0, partner)]

    for copy in t_copies:
        copy.wait_recv()
    moved = swap_blocks(t_recv[...].astype(F32).reshape(N, C), 8)
    for j in range(S):
        row_scr[pl.ds(j, S, stride=S), :] = moved[j * S : (j + 1) * S]
    centred, inverse = centred_inverse(row_scr[...])
    tri_normed = (centred * inverse * tri_out_gain[...]).astype(BF16)
    tile = pair[...].astype(F32).reshape(N, C)
    updated = tile + gate_scr[...] * dot(tri_normed, tri_out[...])
    upd_scr[...] = updated
    centred, inverse = centred_inverse(updated)
    bias_in = (centred * inverse * bias_gain[...]).astype(BF16)
    bias_in_scr[...] = bias_in
    row_scr[...] = dot_nt(bias_in, bw_pad[...])
    by_col = jnp.concatenate([row_scr[pl.ds(j, S, stride=S), :] for j in range(S)], axis=0)
    by_head = swap_blocks(by_col, 1)
    ids = chain[...].astype(F32)
    here = mine * S + iota((N, N), 0) % S
    row_chain = jnp.sum(jnp.where(iota((N, N), 1) == here, ids, 0.0), -1, keepdims=True)
    ids_col = jnp.sum(
        jnp.where(iota((N, N), 1) == iota((N, N), 0), ids, 0.0), -1, keepdims=True
    )
    there = col * S + iota((N, C), 1)
    col_chain = jnp.sum(jnp.where(iota((N, C), 0) == there, ids_col, 0.0), 0, keepdims=True)
    head_bias = jnp.sum(
        jnp.where(iota((N, S), 1) == iota((N, S), 0) // S, chain_bias[...], 0.0),
        -1, keepdims=True,
    )
    by_head = by_head + jnp.where(row_chain == col_chain, head_bias, 0.0)
    b_send[...] = by_head.astype(BF16).reshape(S, S, C)
    b_copies = [
        send(b_send.at[(col + d) % S], b_recv.at[col], sem_b, d, to_col(d)) for d in range(1, S)
    ]
    b_recv[col] = b_send[col]
    pair_next[...] = updated.astype(BF16)
    lane_block = iota((S, C), 1) // S
    for copy in b_copies:
        copy.wait_recv()
    halves = []
    for half in range(2):
        joined = jnp.zeros((S, C), F32)
        for k in range(8):
            piece = b_recv[half * 8 + k].astype(F32)
            piece = pltpu.roll(piece, k * S, 1) if k else piece
            joined = jnp.where(lane_block == k, piece, joined)
        halves.append(joined)
    b_all[mine] = jnp.concatenate(halves, axis=1).astype(BF16)
    ba_copies = [
        send(b_all.at[mine], b_all.at[mine], sem_ba, d, to_line(d)) for d in range(1, S)
    ]
    for k in range(1, 8):
        wg[k - 1].wait_recv()
        at = from_quad(k, core)
        wf.append(send(w_rem.at[at], w_rem.at[at], sem_wf, k, partner))
    for copy in ba_copies:
        copy.wait_recv()

    bias_sum = None
    z_copies, x_copies = {}, {}
    for t in range(T):
        queries, keys, values = qkv_scr[t, 0], qkv_scr[t, 1], qkv_scr[t, 2]
        gate_sig, grad_gated = sig_scr[t], gg_scr[t]
        bias = b_all[...].reshape(N, N).astype(F32)
        exponent = jnp.exp(dot_nt(queries, keys) * inverse_root + bias)
        attention = exponent / jnp.sum(exponent, -1, keepdims=True)
        attention_b = attention.astype(BF16)
        attended = dot(attention_b, values)
        gated = (gate_sig * attended).astype(BF16)
        grad_gate = (grad_gated * attended * gate_sig * (1.0 - gate_sig)).astype(BF16)
        grad_attended = (grad_gated * gate_sig).astype(BF16)
        grad_prob = dot_nt(grad_attended, values)
        grad_values = dot_tn(attention_b, grad_attended).astype(BF16)
        grad_score = attention * (
            grad_prob - jnp.sum(attention * grad_prob, -1, keepdims=True)
        )
        score_b = grad_score.astype(BF16)
        bias_sum = grad_score if bias_sum is None else bias_sum + grad_score
        grad_queries = (dot(score_b, keys) * inverse_root).astype(BF16)
        grad_keys = (dot_tn(score_b, queries) * inverse_root).astype(BF16)
        side = jnp.concatenate([grad_queries, grad_keys, grad_values, grad_gate, gated], axis=1)
        raw[t] = dot(side, place[...]).astype(BF16).reshape(4, 64, N)
        if t == T - 1:
            bs_send[...] = bias_sum.astype(BF16).reshape(S, S, N)
            bs_copies = [
                send(bs_send.at[(mine + d) % S], bs_recv.at[mine], sem_bs, d, to_line(d))
                for d in range(1, S)
            ]
            bs_recv[mine] = bs_send[mine]
        z_copies[t] = [
            send(
                raw.at[t, (zed + 4 - d) % 4], raw_z.at[t, d - 1], sem_z, t * 4 + d,
                {"col": (zed + 4 - d) % 4 * 4 + ex},
            )
            for d in range(1, 4)
        ]

    raw_t = raw[...].reshape(T * N, N).astype(F32).T.astype(BF16)
    grads_part = dot(raw_t[: 4 * E], hid_scr[...].reshape(T * N, D))
    out_part = dot(raw_t[4 * E :], cot[...].reshape(T * N, D))
    turned = jnp.concatenate([grads_part, out_part], axis=0).T
    ws_send[...] = turned.astype(BF16).reshape(S, E, N)
    ws_copies = [
        send(ws_send.at[(mine + d) % S], ws_recv.at[mine], sem_ws, d, to_line(d))
        for d in range(1, S)
    ]
    ws_recv[mine] = ws_send[mine]
    for copy in wf:
        copy.wait_recv()

    def project(t):
        for copy in z_copies[t]:
            copy.wait_recv()
        total = jnp.zeros((C, D), F32)
        first = iota((64, N), 1) < 4 * E
        for d in range(4):
            piece = (raw_z[t, d - 1] if d else raw[t, zed]).astype(F32)
            weights = w_rem[:, d - 1] if d else w_own[...]
            both = jnp.concatenate(
                [jnp.where(first, piece, 0.0), jnp.where(first, 0.0, piece)], axis=0
            ).astype(BF16)
            total = total + dot(both, weights.reshape(N, D))
        total = total.astype(BF16)
        for x in range(4):
            part[t, x, 0] = total[x * S : (x + 1) * S]
            part[t, x, 1] = total[64 + x * S : 64 + (x + 1) * S]
        x_copies[t] = [
            send(
                part.at[t, (ex + d) % 4], part_x.at[t, d - 1], sem_x, t * 4 + d,
                {"col": zed * 4 + (ex + d) % 4},
            )
            for d in range(1, 4)
        ]

    def finish(t):
        for copy in x_copies[t]:
            copy.wait_recv()
        sums = part[t, ex].astype(F32)
        for d in range(3):
            sums = sums + part_x[t, d].astype(F32)
        first = pl.multiple_of(col * S, S)
        scaled = tokens[t, pl.ds(first, S), :].astype(F32) * scale_of[t]
        cot_mine = cot[t, pl.ds(first, S), :].astype(F32)
        denoised[t] = (scaled + sums[1]).astype(BF16)
        back = norm_back(sums[0], scaled, attn_gain[...].reshape(1, D))
        token_grad[t] = (scale_of[t] * (cot_mine + back)).astype(BF16)

    project(0)
    for copy in bs_copies:
        copy.wait_recv()
    bias_rows = jnp.sum(bs_recv[...].astype(F32), axis=0)
    narrow = iota((S, C), 1) < S
    for k in range(S):
        piece = bias_rows[:, :C] if k < 8 else bias_rows[:, C:]
        piece = pltpu.roll(piece, C - k % 8 * S, 1) if k % 8 else piece
        bb_send[k] = jnp.where(narrow, piece, 0.0).astype(BF16)
    bb_copies = [
        send(bb_send.at[(col + d) % S], bb_recv.at[col], sem_bb, d, to_col(d))
        for d in range(1, S)
    ]
    bb_recv[col] = bb_send[col]
    project(1)
    project(2)
    for copy in bb_copies:
        copy.wait_recv()
    back = swap_blocks(bb_recv[...].astype(F32).reshape(N, C), 1)
    back = jnp.where(iota((N, C), 1) < S, back, 0.0)
    for j in range(S):
        row_scr[pl.ds(j, S, stride=S), :] = back[j * S : (j + 1) * S]
    grad_bias = row_scr[...].astype(BF16)
    ar_one[...] = dot_tn(grad_bias, bias_in_scr[...])[:S]
    a1_copies = [
        send(ar_one, ar_all.at[mine], sem_a1, d, to_line(d)) for d in range(1, S)
    ]
    ar_all[mine] = ar_one[...]
    grad_in = dot(grad_bias, bw_pad[...])
    pair_grad[...] = norm_back(grad_in, upd_scr[...], bias_gain[...])
    finish(0)
    for copy in a1_copies:
        copy.wait_recv()
    ar_two[...] = jnp.sum(ar_all[...], axis=0)
    a2_copies = [
        send(ar_two, ar_fin.at[col], sem_a2, d, to_col(d)) for d in range(1, S)
    ]
    ar_fin[col] = ar_two[...]
    finish(1)
    finish(2)
    for copy in ws_copies:
        copy.wait_recv()
    weight_grad[...] = jnp.sum(ws_recv[...].astype(F32), axis=0)
    for copy in a2_copies:
        copy.wait_recv()
    bias_weight_grad[...] = jnp.sum(ar_fin[...], axis=0)
    for copy in pending:
        copy.wait_send()


def finisher(*refs):
    sums = refs[5]
    for at in range(5):
        refs[6 + at][...] = refs[at][...]
    for g in range(4):
        refs[11][g] = sums[:, g * E : (g + 1) * E]
    refs[12][...] = pltpu.roll(sums[:, C:], C // 2, 1).T[:E]


def shards(
    pair_repr, pair_mask, chain_id, tri_in_gain, tri_proj, tri_gate, tri_out_gain, tri_out,
    bias_gain, bias_weight, chain_bias, tokens, noise_level, attn_gain, attn_weight, out_weight,
    cotangent,
):
    vmem = pl.BlockSpec(memory_space=pltpu.VMEM)
    smem = pl.BlockSpec(memory_space=pltpu.SMEM)

    def buf(*shape, kind=BF16):
        return pltpu.VMEM(shape, kind)

    def sems(count):
        return pltpu.SemaphoreType.DMA((2, count))

    outs = pl.pallas_call(
        kernel,
        out_shape=(
            jax.ShapeDtypeStruct((N, C), BF16),
            jax.ShapeDtypeStruct((N, C), F32),
            jax.ShapeDtypeStruct((S, C), F32),
            jax.ShapeDtypeStruct((T, S, D), BF16),
            jax.ShapeDtypeStruct((T, S, D), BF16),
            jax.ShapeDtypeStruct((E, N), F32),
        ),
        in_specs=[vmem] * 12 + [smem] + [vmem] * 4,
        out_specs=(vmem,) * 6,
        scratch_shapes=[
            buf(N, C, kind=F32),
            buf(S, S, C), buf(S, S, C), buf(S, S, C), buf(S, S, C),
            buf(S, S, S, C),
            buf(C, N),
            buf(S, S, C), buf(S, S, C),
            buf(N, C, kind=F32), buf(N, C, kind=F32),
            buf(N, C), buf(C, C),
            buf(S, S, C), buf(S, S, C), buf(S, S, N),
            buf(4 * C, D), buf(C, D), buf(5 * C, N),
            buf(S, S, D), buf(S, 3, S, D),
            buf(T, N, D), buf(T, 3, N, C),
            buf(T, N, C, kind=F32), buf(T, N, C, kind=F32),
            buf(T, 4, 64, N), buf(T, 3, 64, N),
            buf(T, 4, 2, S, D), buf(T, 3, 2, S, D),
            buf(S, S, N), buf(S, S, N), buf(S, S, C), buf(S, S, C),
            buf(S, E, N), buf(S, E, N),
            buf(S, C, kind=F32), buf(S, S, C, kind=F32),
            buf(S, C, kind=F32), buf(S, S, C, kind=F32),
            sems(S), sems(S), sems(8), sems(8), sems(S), sems(S), sems(S), sems(4), sems(8),
            sems(8), sems(12), sems(12), sems(S), sems(S), sems(S), sems(S), sems(S),
        ],
        compiler_params=pltpu.CompilerParams(
            collective_id=0, has_side_effects=True, vmem_limit_bytes=60 * 1024 * 1024
        ),
    )(
        pair_repr, pair_mask, chain_id.reshape(1, N), tri_in_gain.reshape(1, C), tri_proj,
        tri_gate, tri_out_gain.reshape(1, C), tri_out, bias_gain.reshape(1, C), bias_weight.T,
        chain_bias.reshape(1, S), tokens, noise_level, attn_gain,
        jnp.transpose(attn_weight, (0, 2, 1)), out_weight, cotangent,
    )
    outs = pl.pallas_call(
        finisher,
        out_shape=(
            jax.ShapeDtypeStruct((N, C), BF16),
            jax.ShapeDtypeStruct((N, C), F32),
            jax.ShapeDtypeStruct((S, C), F32),
            jax.ShapeDtypeStruct((T, S, D), BF16),
            jax.ShapeDtypeStruct((T, S, D), BF16),
            jax.ShapeDtypeStruct((4, E, E), F32),
            jax.ShapeDtypeStruct((E, E), F32),
        ),
        in_specs=[vmem] * 6,
        out_specs=(vmem,) * 7,
    )(*outs)
    pair_next, pair_grad, bias_weight_grad, denoised, token_grad, weight_grad, out_grad = outs
    return (
        pair_next.reshape(S, S, C),
        pair_grad.reshape(S, S, C),
        bias_weight_grad.T,
        denoised,
        token_grad,
        weight_grad,
        out_grad,
    )


def solution(mesh):
    line, col = ("group", "row"), "col"
    return jax.shard_map(
        shards,
        mesh=mesh,
        in_specs=(
            P(line, col, None), P(line, col), P(), P(), P(), P(), P(), P(), P(), P(), P(),
            P(line, None, None), P(line), P(), P(None, None, col), P(col, None),
            P(line, None, None),
        ),
        out_specs=(
            P(line, col, None), P(line, col, None), P(), P(line, col, None),
            P(line, col, None), P(None, line, col), P(col, line),
        ),
        check_vma=False,
    )
```

```python
import math

import jax
import jax.numpy as jnp
from jax import lax
from jax.experimental import pallas as pl
from jax.experimental.pallas import tpu as pltpu
from jax.sharding import PartitionSpec as P

MESH = pl.DeviceIdType.MESH
LEVELS = 200
EPSILON = 1e-05
SIGMA_LOW = 0.1
SIGMA_SPAN = 100.0
F32 = jnp.float32
BF16 = jnp.bfloat16
S = 16
C = 128
E = 48
D = 768
N = 256
T = 3
NT = (((1,), (1,)), ((), ()))
TN = (((0,), (0,)), ((), ()))


def iota(shape, dim):
    return lax.broadcasted_iota(jnp.int32, shape, dim)


def dot(a, b):
    return jnp.dot(a, b, preferred_element_type=F32)


def dot_nt(a, b):
    return lax.dot_general(a, b, NT, preferred_element_type=F32)


def dot_tn(a, b):
    return lax.dot_general(a, b, TN, preferred_element_type=F32)


def sigmoid(v):
    return 1.0 / (1.0 + jnp.exp(-v))


def centred_inverse(v):
    centred = v - jnp.mean(v, -1, keepdims=True)
    return centred, lax.rsqrt(jnp.mean(centred * centred, -1, keepdims=True) + EPSILON)


def norm_back(gradient, values, gain):
    centred, inverse = centred_inverse(values)
    normed = centred * inverse
    weighted = gradient * gain
    return inverse * (
        weighted
        - jnp.mean(weighted, -1, keepdims=True)
        - normed * jnp.mean(weighted * normed, -1, keepdims=True)
    )


def swap_blocks(x, unit):
    arr = iota(x.shape, 0) // S
    blk = iota(x.shape, 1) // unit
    for bit in (1, 2, 4, 8):
        rows = bit * S
        other = jnp.concatenate(
            [x[(k ^ 1) * rows : (k ^ 1) * rows + rows] for k in range(N // rows)], axis=0
        )
        up = pltpu.roll(other, bit * unit, 1)
        down = pltpu.roll(other, C - bit * unit, 1)
        in_arr, in_blk = (arr & bit) != 0, (blk & bit) != 0
        x = jnp.where(in_arr == in_blk, x, jnp.where(in_blk, up, down))
    return x


def swap_rows(x):
    arr, blk = iota(x.shape, 0), iota(x.shape, 1) // S
    for bit in (1, 2, 4, 8):
        in_arr, in_blk = (arr & bit) != 0, (blk & bit) != 0
        other = jnp.where(in_arr, pltpu.roll(x, bit, 0), pltpu.roll(x, S - bit, 0))
        up = pltpu.roll(other, bit * S, 1)
        down = pltpu.roll(other, N - bit * S, 1)
        x = jnp.where(in_arr == in_blk, x, jnp.where(in_blk, up, down))
    return x


def kernel(
    *refs,
):
    (
        pair, mask, chain, tri_in_gain, tri_proj, tri_gate, tri_out_gain, tri_out, bias_gain,
        bias_weight, chain_bias, tokens, level, attn_gain, attn_weight, out_weight, cot,
    ) = refs[23:40]
    results, sem_out = refs[-7:-1], refs[-1]
    pair_next, pair_grad, bias_weight_grad, denoised, token_grad, weight_grad = results
    work(
        refs[:17], refs[23:40], refs[40], refs[17:23], results, sem_out,
        pair, mask, chain, tri_in_gain, tri_proj, tri_gate, tri_out_gain, tri_out, bias_gain,
        bias_weight, chain_bias, tokens, level, attn_gain, attn_weight, out_weight, cot,
        pair_next, pair_grad, bias_weight_grad, denoised, token_grad, weight_grad, *refs[41:-7],
    )


def work(
    stored, loaded, sem_in, given, results, sem_out,
    pair, mask, chain, tri_in_gain, tri_proj, tri_gate, tri_out_gain, tri_out, bias_gain,
    bias_weight, chain_bias, tokens, level, attn_gain, attn_weight, out_weight, cot,
    pair_next, pair_grad, bias_weight_grad, denoised, token_grad, weight_grad,
    gate_scr, r_send, l_send, r_own, l_own, r_all, left_t, t_send, t_recv, row_scr, upd_scr,
    bias_in_scr, bw_pad, b_send, b_recv, b_all, w_four, ow_pad, place, w_own, w_rem, hid_scr, qkv_scr,
    sig_scr, slope_scr, ga_scr, score_scr, prob_scr, raw, raw_z, part, part_x, bs_send, bs_recv, bb_send, bb_recv, ws_send,
    ws_recv, ar_one, ar_all, ar_two, ar_fin,
    sems,
):
    group, row, col = lax.axis_index("group"), lax.axis_index("row"), lax.axis_index("col")
    mine = group * 8 + row
    core, high = row % 2, row // 2
    quad = group * 4 + high
    zed, ex = col // 4, col % 4
    keys, bulks = {}, {}

    def send(src, dst, key, device):
        at = keys.setdefault(key, len(keys))
        pltpu.make_async_remote_copy(
            src_ref=src, dst_ref=dst, send_sem=sems.at[0, at], recv_sem=sems.at[1, at],
            device_id=device, device_id_type=MESH,
        ).start()

    def arrive(key, bulk):
        bulks[key] = bulk
        pltpu.make_async_copy(bulk, bulk, sems.at[1, keys[key]]).wait()

    def col_at(step):
        return (zed + step // 4) % 4 * 4 + (ex + step % 4) % 4

    def to_col(step):
        return {"col": col_at(step)}

    def to_line(step):
        there = (mine + step) % S
        return {"group": there // 8, "row": there % 8}

    stores = [
        pltpu.make_async_copy(src, dst, sem_out.at[k])
        for k, (src, dst) in enumerate(zip(results, given, strict=True))
    ]
    barrier = pltpu.get_barrier_semaphore()
    for step in range(1, S):
        pl.semaphore_signal(barrier, inc=1, device_id=to_col(step), device_id_type=MESH)
        pl.semaphore_signal(barrier, inc=1, device_id=to_line(step), device_id_type=MESH)

    loads = [
        pltpu.make_async_copy(src, dst, sem_in.at[k])
        for k, (src, dst) in enumerate(zip(stored, loaded, strict=True))
    ]
    first, second = (0, 1, 3, 4, 5), (14, 15, 9, 11, 12, 13, 16, 2, 6, 7, 8, 10)
    for k in first + second:
        loads[k].start()
    for k in first:
        loads[k].wait()
    tile = pair[...].astype(F32).reshape(N, C)
    centred, inverse = centred_inverse(tile)
    pair_in = (centred * inverse * tri_in_gain[...]).astype(BF16)
    pick = (iota((N, S), 0) // S == iota((N, S), 1)).astype(BF16)
    spread = dot(pick, mask[...].astype(F32).astype(BF16))
    mask_col = jnp.sum(
        jnp.where(iota((N, S), 0) % S == iota((N, S), 1), spread, 0.0), -1, keepdims=True
    )
    right = dot(pair_in, tri_proj[:, 2 * C : 4 * C])
    right = sigmoid(right[:, :C]) * right[:, C:] * mask_col
    r_send[...] = swap_blocks(right, 8).astype(BF16).reshape(S, S, C)
    pl.semaphore_wait(barrier, 2 * (S - 1))
    for d in range(1, S):
        send(r_send.at[col_at(d)], r_own.at[col], ("r", d // 4), to_col(d))
    r_own[col] = r_send[col]
    left = dot(pair_in, tri_proj[:, : 2 * C])
    left = sigmoid(left[:, :C]) * left[:, C:] * mask_col
    l_send[...] = swap_blocks(left, 8).astype(BF16).reshape(S, S, C)
    for d in range(1, S):
        send(l_send.at[col_at(d)], l_own.at[col], "l", to_col(d))
    l_own[col] = l_send[col]
    gate_scr[...] = sigmoid(dot(pair_in, tri_gate[...]))

    for k in second:
        loads[k].wait()
    for g in range(4):
        w_own[3 * g : 3 * g + 3] = attn_weight[g].reshape(3, S, D)
    w_own[12:15] = out_weight[...].reshape(3, S, D)
    w_own[15] = jnp.zeros((S, D), BF16)
    w_four[...] = jnp.zeros_like(w_four)
    for g in range(4):
        w_four[g * C : g * C + E, :] = attn_weight[g]
    ow_pad[...] = jnp.zeros_like(ow_pad)
    ow_pad[:E, :] = out_weight[...]
    bw_pad[...] = jnp.zeros_like(bw_pad)
    bw_pad[:S, :] = bias_weight[...]
    place_row = iota((5 * C, N), 0)
    inner = place_row % C
    place[...] = jnp.where(
        (inner < E) & (iota((5 * C, N), 1) == place_row // C * E + inner), 1.0, 0.0
    ).astype(BF16)

    scale_of = []
    for t in range(T):
        power = jnp.full((1, C), level[t].astype(F32)) * (math.log(SIGMA_SPAN) / (LEVELS - 1))
        sigma = SIGMA_LOW * jnp.exp(power)
        scale_of.append(lax.rsqrt(1.0 + sigma * sigma)[:, :1])
    inverse_root = 1.0 / math.sqrt(E)

    def before_bias(t):
        scaled = tokens[t].astype(F32) * scale_of[t]
        mid, inv = centred_inverse(scaled)
        hidden = (mid * inv * attn_gain[...].reshape(1, D)).astype(BF16)
        hid_scr[t] = hidden
        projections = dot_nt(hidden, w_four[...])
        for g in range(3):
            qkv_scr[t, g] = projections[:, g * C : (g + 1) * C].astype(BF16)
        gate_sig = sigmoid(projections[:, 3 * C :])
        grad_gated = dot_nt(cot[t], ow_pad[...])
        grad_attended = (grad_gated * gate_sig).astype(BF16)
        sig_scr[t] = gate_sig
        slope_scr[t] = grad_gated * gate_sig * (1.0 - gate_sig)
        ga_scr[t] = grad_attended
        score_scr[t] = dot_nt(qkv_scr[t, 0], qkv_scr[t, 1]) * inverse_root
        prob_scr[t] = dot_nt(grad_attended, qkv_scr[t, 2])

    before_bias(0)

    partner = {"row": high * 2 + 1 - core}

    def to_quad(k):
        return {"group": (quad + k) % 8 // 4, "row": (quad + k) % 4 * 2 + core}

    def from_quad(k, side):
        there = (quad + 8 - k) % 8
        return there // 4 * 8 + there % 4 * 2 + side

    def z_block(dz):
        return pl.ds((zed + 4 - dz) % 4 * 4, 4)

    def ag_key(dz, k):
        return ("ag", dz, k) if dz == 2 else ("ag", dz)

    def fw_key(dz, k):
        return ("fw", dz, k) if dz == 2 else ("fw", dz)

    def spread_right(dz):
        arrive(("r", dz), r_own.at[pl.ds(0, 4 if dz else 3)])
        block = r_own.at[z_block(dz)]
        there = r_all.at[mine, z_block(dz)]
        for k in range(1, 8):
            send(block, there, ag_key(dz, k), to_quad(k))
        send(block, there, fw_key(dz, 0), partner)

    def relay(dz, k):
        block = r_all.at[from_quad(k, core), z_block(dz)]
        send(block, block, fw_key(dz, k), partner)

    spread_right(0)
    spread_right(1)
    spread_right(3)
    spread_right(2)
    before_bias(1)
    arrive("l", l_own.at[pl.ds(0, S - 1)])
    for d in range(1, 4):
        send(w_own.at[mine], w_rem.at[mine, d - 1], "w", {"col": (zed + 4 - d) % 4 * 4 + ex})
    left_t[...] = l_own[...].reshape(N, C).astype(F32).T.astype(BF16)
    diagonal = iota((C, C), 0) % 8 == iota((C, C), 1) % 8

    def triangle(at, block):
        product = dot(left_t[...], block.reshape(N, C))
        product = jnp.where(diagonal, product, 0.0).reshape(S, 8, C)
        t_send[at] = jnp.sum(product, axis=1).astype(BF16)

    triangle(mine, r_own[...])
    for dz in (0, 1, 3):
        arrive(("ag", dz), r_all.at[pl.ds(0, 7), pl.ds(0, 4)])
        for k in range(1, 8):
            relay(dz, k)
    before_bias(2)
    for k in range(1, 8):
        arrive(("ag", 2, k), r_all.at[0, pl.ds(0, 4)])
        relay(2, k)
        triangle(from_quad(k, core), r_all[from_quad(k, core)])
    for dz in (0, 1, 3):
        arrive(("fw", dz), r_all.at[pl.ds(0, 8), pl.ds(0, 4)])
    for k in range(8):
        arrive(("fw", 2, k), r_all.at[0, pl.ds(0, 4)])
        triangle(from_quad(k, 1 - core), r_all[from_quad(k, 1 - core)])
    for d in range(1, S):
        send(t_send.at[col_at(d)], t_recv.at[col], "t", to_col(d))
    t_recv[col] = t_send[col]

    arrive("w", w_rem.at[0])
    for k in range(1, 8):
        send(w_rem.at[mine], w_rem.at[mine], "wg", to_quad(k))
    send(w_rem.at[mine], w_rem.at[mine], "wf", partner)

    arrive("t", t_recv.at[pl.ds(0, S - 1)])
    moved = swap_blocks(t_recv[...].astype(F32).reshape(N, C), 8)
    for j in range(S):
        row_scr[pl.ds(j, S, stride=S), :] = moved[j * S : (j + 1) * S]
    centred, inverse = centred_inverse(row_scr[...])
    tri_normed = (centred * inverse * tri_out_gain[...]).astype(BF16)
    tile = pair[...].astype(F32).reshape(N, C)
    updated = tile + gate_scr[...] * dot(tri_normed, tri_out[...])
    upd_scr[...] = updated
    centred, inverse = centred_inverse(updated)
    bias_in = (centred * inverse * bias_gain[...]).astype(BF16)
    bias_in_scr[...] = bias_in
    by_head = dot_nt(bw_pad[:S, :], bias_in)
    ids = chain[...].astype(F32)
    eye = iota((N, N), 0) == iota((N, N), 1)
    ids_col = jnp.sum(jnp.where(eye, ids, 0.0), -1, keepdims=True)
    lane = iota((N, N), 1)
    row_of = mine * S + lane // S == iota((N, N), 0)
    row_chain = jnp.sum(jnp.where(row_of, ids_col, 0.0), 0, keepdims=True)
    col_of = col * S + lane % S == iota((N, N), 0)
    col_chain = jnp.sum(jnp.where(col_of, ids_col, 0.0), 0, keepdims=True)
    head_bias = jnp.sum(
        jnp.where(iota((S, S), 1) == iota((S, S), 0), chain_bias[...], 0.0), -1, keepdims=True
    )
    by_head = by_head + jnp.where(row_chain == col_chain, head_bias, 0.0)
    for k in range(S):
        b_send[k] = by_head[k : k + 1]
    for d in range(1, S):
        send(b_send.at[col_at(d)], b_recv.at[col], "b", to_col(d))
    b_recv[col] = b_send[col]
    pair_next[...] = updated.astype(BF16)
    stores[0].start()
    arrive("b", b_recv.at[pl.ds(0, S - 1)])
    by_row = swap_rows(jnp.concatenate([b_recv[k] for k in range(S)], axis=0))
    b_all[mine] = by_row.astype(BF16)
    for d in range(1, S):
        send(b_all.at[mine], b_all.at[mine], "ba", to_line(d))
    arrive("wg", w_rem.at[pl.ds(0, 7)])
    for k in range(1, 8):
        at = from_quad(k, core)
        send(w_rem.at[at], w_rem.at[at], "wf", partner)
    arrive("ba", b_all.at[pl.ds(0, S - 1)])

    bias = b_all[...].reshape(N, N).astype(F32)
    copies = range(T)
    exponent = [jnp.exp(score_scr[t] + bias) for t in copies]
    attention = [e / jnp.sum(e, -1, keepdims=True) for e in exponent]
    attention_b = [a.astype(BF16) for a in attention]
    grad_score = [
        a * (prob_scr[t] - jnp.sum(a * prob_scr[t], -1, keepdims=True))
        for t, a in enumerate(attention)
    ]
    bs_send[...] = sum(grad_score[1:], grad_score[0]).astype(BF16).reshape(S, S, N)
    for d in range(1, S):
        send(bs_send.at[(mine + d) % S], bs_recv.at[mine], "bs", to_line(d))
    bs_recv[mine] = bs_send[mine]
    score_b = [g.astype(BF16) for g in grad_score]
    attended = [dot(attention_b[t], qkv_scr[t, 2]) for t in copies]
    grad_values = [dot_tn(attention_b[t], ga_scr[t]).astype(BF16) for t in copies]
    grad_queries = [(dot(score_b[t], qkv_scr[t, 1]) * inverse_root).astype(BF16) for t in copies]
    grad_keys = [(dot_tn(score_b[t], qkv_scr[t, 0]) * inverse_root).astype(BF16) for t in copies]
    gated = [(sig_scr[t] * attended[t]).astype(BF16) for t in copies]
    grad_gate = [(slope_scr[t] * attended[t]).astype(BF16) for t in copies]
    for t in copies:
        side = jnp.concatenate(
            [grad_queries[t], grad_keys[t], grad_values[t], grad_gate[t], gated[t]], axis=1
        )
        raw[t] = dot(side, place[...]).astype(BF16).reshape(4, 64, N)
    def spread_raw(t):
        for d in (2, 1, 3):
            there = (zed + 4 - d) % 4
            send(raw.at[t, there], raw_z.at[t, d - 1], ("z", t), {"col": there * 4 + ex})

    spread_raw(0)
    raw_t = raw[...].reshape(T * N, N).astype(F32).T.astype(BF16)
    grads_part = dot(raw_t[: 4 * E], hid_scr[...].reshape(T * N, D))
    out_part = dot(raw_t[4 * E :], cot[...].reshape(T * N, D))
    turned = jnp.concatenate([grads_part, out_part], axis=0).T
    ws_send[...] = turned.astype(BF16).reshape(S, E, N)
    for d in range(1, S):
        send(ws_send.at[(mine + d) % S], ws_recv.at[mine], "ws", to_line(d))
    ws_recv[mine] = ws_send[mine]
    def project(t):
        arrive(("z", t), raw_z.at[t])
        total = jnp.zeros((C, D), F32)
        first = iota((64, N), 1) < 4 * E
        for d in range(4):
            piece = (raw_z[t, d - 1] if d else raw[t, zed]).astype(F32)
            weights = w_rem[:, d - 1] if d else w_own[...]
            both = jnp.concatenate(
                [jnp.where(first, piece, 0.0), jnp.where(first, 0.0, piece)], axis=0
            ).astype(BF16)
            total = total + dot(both, weights.reshape(N, D))
        total = total.astype(BF16)
        for x in range(4):
            part[t, x, 0] = total[x * S : (x + 1) * S]
            part[t, x, 1] = total[64 + x * S : 64 + (x + 1) * S]
        for d in range(1, 4):
            there = (ex + d) % 4
            send(part.at[t, there], part_x.at[t, d - 1], ("x", t), {"col": zed * 4 + there})

    def finish(t):
        arrive(("x", t), part_x.at[t])
        sums = part[t, ex].astype(F32)
        for d in range(3):
            sums = sums + part_x[t, d].astype(F32)
        first = pl.multiple_of(col * S, S)
        scaled = tokens[t, pl.ds(first, S), :].astype(F32) * scale_of[t]
        cot_mine = cot[t, pl.ds(first, S), :].astype(F32)
        denoised[t] = (scaled + sums[1]).astype(BF16)
        back = norm_back(sums[0], scaled, attn_gain[...].reshape(1, D))
        token_grad[t] = (scale_of[t] * (cot_mine + back)).astype(BF16)

    arrive("bs", bs_recv.at[pl.ds(0, S - 1)])
    by_tile = swap_rows(jnp.sum(bs_recv[...].astype(F32), axis=0))
    for k in range(S):
        bb_send[k] = by_tile[k : k + 1]
    for d in range(1, S):
        send(bb_send.at[col_at(d)], bb_recv.at[col], "bb", to_col(d))
    bb_recv[col] = bb_send[col]
    arrive("wf", w_rem.at[pl.ds(0, 8)])
    project(0)
    spread_raw(1)
    spread_raw(2)
    arrive("bb", bb_recv.at[pl.ds(0, S - 1)])
    grad_bias = jnp.concatenate([bb_recv[k] for k in range(S)], axis=0).astype(BF16)
    ar_one[...] = dot(grad_bias, bias_in_scr[...]).astype(BF16)
    for d in range(1, S):
        send(ar_one, ar_all.at[mine], "a1", to_line(d))
    ar_all[mine] = ar_one[...]
    grad_in = dot_tn(grad_bias, bw_pad[:S, :])
    pair_grad[...] = norm_back(grad_in, upd_scr[...], bias_gain[...])
    stores[1].start()
    project(1)
    arrive("a1", ar_all.at[pl.ds(0, S - 1)])
    ar_two[...] = jnp.sum(ar_all[...].astype(F32), axis=0).astype(BF16)
    for d in range(1, S):
        send(ar_two, ar_fin.at[col], "a2", to_col(d))
    ar_fin[col] = ar_two[...]
    project(2)
    finish(0)
    finish(1)
    finish(2)
    stores[3].start()
    stores[4].start()
    arrive("ws", ws_recv.at[pl.ds(0, S - 1)])
    weight_grad[...] = jnp.sum(ws_recv[...].astype(F32), axis=0)
    stores[5].start()
    arrive("a2", ar_fin.at[pl.ds(0, S - 1)])
    bias_weight_grad[...] = jnp.sum(ar_fin[...].astype(F32), axis=0)
    stores[2].start()
    for key, bulk in bulks.items():
        pltpu.make_async_copy(bulk, bulk, sems.at[0, keys[key]]).wait()
    for copy in stores:
        copy.wait()


def finisher(*refs):
    sums = refs[5]
    for at in range(5):
        refs[6 + at][...] = refs[at][...]
    for g in range(4):
        refs[11][g] = sums[:, g * E : (g + 1) * E]
    refs[12][...] = pltpu.roll(sums[:, C:], C // 2, 1).T[:E]


def shards(
    pair_repr, pair_mask, chain_id, tri_in_gain, tri_proj, tri_gate, tri_out_gain, tri_out,
    bias_gain, bias_weight, chain_bias, tokens, noise_level, attn_gain, attn_weight, out_weight,
    cotangent,
):
    vmem = pl.BlockSpec(memory_space=pltpu.VMEM)
    hbm = pl.BlockSpec(memory_space=pltpu.HBM)

    def buf(*shape, kind=BF16):
        return pltpu.VMEM(shape, kind)

    outs = pl.pallas_call(
        kernel,
        out_shape=(
            jax.ShapeDtypeStruct((N, C), BF16),
            jax.ShapeDtypeStruct((N, C), F32),
            jax.ShapeDtypeStruct((S, C), F32),
            jax.ShapeDtypeStruct((T, S, D), BF16),
            jax.ShapeDtypeStruct((T, S, D), BF16),
            jax.ShapeDtypeStruct((E, N), F32),
        ),
        in_specs=[hbm] * 17,
        out_specs=(hbm,) * 6,
        scratch_shapes=[
            buf(S, S, C), buf(S, S, kind=jnp.int32), buf(1, N, kind=jnp.int32),
            buf(1, C, kind=F32), buf(C, 4 * C), buf(C, C), buf(1, C, kind=F32), buf(C, C),
            buf(1, C, kind=F32), buf(S, C), buf(1, S, kind=F32), buf(T, N, D),
            pltpu.SMEM((T,), jnp.int32), buf(D, kind=F32), buf(4, E, D), buf(E, D), buf(T, N, D),
            pltpu.SemaphoreType.DMA((17,)),
            buf(N, C, kind=F32),
            buf(S, S, C), buf(S, S, C), buf(S, S, C), buf(S, S, C),
            buf(S, S, S, C),
            buf(C, N),
            buf(S, S, C), buf(S, S, C),
            buf(N, C, kind=F32), buf(N, C, kind=F32),
            buf(N, C), buf(C, C),
            buf(S, 1, N, kind=F32), buf(S, 1, N, kind=F32), buf(S, S, N),
            buf(4 * C, D), buf(C, D), buf(5 * C, N),
            buf(S, S, D), buf(S, 3, S, D),
            buf(T, N, D), buf(T, 3, N, C),
            buf(T, N, C, kind=F32), buf(T, N, C, kind=F32), buf(T, N, C),
            buf(T, N, N, kind=F32), buf(T, N, N, kind=F32),
            buf(T, 4, 64, N), buf(T, 3, 64, N),
            buf(T, 4, 2, S, D), buf(T, 3, 2, S, D),
            buf(S, S, N), buf(S, S, N),
            buf(S, 1, N, kind=F32), buf(S, 1, N, kind=F32),
            buf(S, E, N), buf(S, E, N),
            buf(S, C), buf(S, S, C), buf(S, C), buf(S, S, C),
            pltpu.SemaphoreType.DMA((2, 44)),
            buf(N, C), buf(N, C, kind=F32), buf(S, C, kind=F32), buf(T, S, D), buf(T, S, D),
            buf(E, N, kind=F32), pltpu.SemaphoreType.DMA((6,)),
        ],
        compiler_params=pltpu.CompilerParams(
            collective_id=0, has_side_effects=True, vmem_limit_bytes=60 * 1024 * 1024
        ),
    )(
        pair_repr, pair_mask, chain_id.reshape(1, N), tri_in_gain.reshape(1, C), tri_proj,
        tri_gate, tri_out_gain.reshape(1, C), tri_out, bias_gain.reshape(1, C), bias_weight.T,
        chain_bias.reshape(1, S), tokens, noise_level, attn_gain,
        jnp.transpose(attn_weight, (0, 2, 1)), out_weight, cotangent,
    )
    outs = pl.pallas_call(
        finisher,
        out_shape=(
            jax.ShapeDtypeStruct((N, C), BF16),
            jax.ShapeDtypeStruct((N, C), F32),
            jax.ShapeDtypeStruct((S, C), F32),
            jax.ShapeDtypeStruct((T, S, D), BF16),
            jax.ShapeDtypeStruct((T, S, D), BF16),
            jax.ShapeDtypeStruct((4, E, E), F32),
            jax.ShapeDtypeStruct((E, E), F32),
        ),
        in_specs=[vmem] * 6,
        out_specs=(vmem,) * 7,
    )(*outs)
    pair_next, pair_grad, bias_weight_grad, denoised, token_grad, weight_grad, out_grad = outs
    return (
        pair_next.reshape(S, S, C),
        pair_grad.reshape(S, S, C),
        bias_weight_grad.T,
        denoised,
        token_grad,
        weight_grad,
        out_grad,
    )


def solution(mesh):
    line, col = ("group", "row"), "col"
    return jax.shard_map(
        shards,
        mesh=mesh,
        in_specs=(
            P(line, col, None), P(line, col), P(), P(), P(), P(), P(), P(), P(), P(), P(),
            P(line, None, None), P(line), P(), P(None, None, col), P(col, None),
            P(line, None, None),
        ),
        out_specs=(
            P(line, col, None), P(line, col, None), P(), P(line, col, None),
            P(line, col, None), P(None, line, col), P(col, line),
        ),
        check_vma=False,
    )
```

```python
import math

import jax
import jax.numpy as jnp
from jax import lax
from jax.experimental import pallas as pl
from jax.experimental.pallas import tpu as pltpu
from jax.sharding import PartitionSpec as P

MESH = pl.DeviceIdType.MESH
LEVELS = 200
EPSILON = 1e-05
SIGMA_LOW = 0.1
SIGMA_SPAN = 100.0
F32 = jnp.float32
BF16 = jnp.bfloat16
S = 16
C = 128
E = 48
D = 768
N = 256
T = 3
NT = (((1,), (1,)), ((), ()))
TN = (((0,), (0,)), ((), ()))


def iota(shape, dim):
    return lax.broadcasted_iota(jnp.int32, shape, dim)


def dot(a, b):
    return jnp.dot(a, b, preferred_element_type=F32)


def dot_nt(a, b):
    return lax.dot_general(a, b, NT, preferred_element_type=F32)


def dot_tn(a, b):
    return lax.dot_general(a, b, TN, preferred_element_type=F32)


def sigmoid(v):
    return 1.0 / (1.0 + jnp.exp(-v))


def centred_inverse(v):
    centred = v - jnp.mean(v, -1, keepdims=True)
    return centred, lax.rsqrt(jnp.mean(centred * centred, -1, keepdims=True) + EPSILON)


def norm_back(gradient, values, gain):
    centred, inverse = centred_inverse(values)
    normed = centred * inverse
    weighted = gradient * gain
    return inverse * (
        weighted
        - jnp.mean(weighted, -1, keepdims=True)
        - normed * jnp.mean(weighted * normed, -1, keepdims=True)
    )


def swap_blocks(x, unit):
    arr = iota(x.shape, 0) // S
    blk = iota(x.shape, 1) // unit
    for bit in (1, 2, 4, 8):
        rows = bit * S
        other = jnp.concatenate(
            [x[(k ^ 1) * rows : (k ^ 1) * rows + rows] for k in range(N // rows)], axis=0
        )
        up = pltpu.roll(other, bit * unit, 1)
        down = pltpu.roll(other, C - bit * unit, 1)
        in_arr, in_blk = (arr & bit) != 0, (blk & bit) != 0
        x = jnp.where(in_arr == in_blk, x, jnp.where(in_blk, up, down))
    return x


def swap_rows(x):
    arr, blk = iota(x.shape, 0), iota(x.shape, 1) // S
    for bit in (1, 2, 4, 8):
        in_arr, in_blk = (arr & bit) != 0, (blk & bit) != 0
        other = jnp.where(in_arr, pltpu.roll(x, bit, 0), pltpu.roll(x, S - bit, 0))
        up = pltpu.roll(other, bit * S, 1)
        down = pltpu.roll(other, N - bit * S, 1)
        x = jnp.where(in_arr == in_blk, x, jnp.where(in_blk, up, down))
    return x


def kernel(
    *refs,
):
    (
        pair, mask, chain, tri_in_gain, tri_proj, tri_gate, tri_out_gain, tri_out, bias_gain,
        bias_weight, chain_bias, tokens, level, attn_gain, attn_weight, out_weight, cot,
    ) = refs[23:40]
    results, sem_out = refs[-7:-1], refs[-1]
    pair_next, pair_grad, bias_weight_grad, denoised, token_grad, weight_grad = results
    work(
        refs[:17], refs[23:40], refs[40], refs[17:23], results, sem_out,
        pair, mask, chain, tri_in_gain, tri_proj, tri_gate, tri_out_gain, tri_out, bias_gain,
        bias_weight, chain_bias, tokens, level, attn_gain, attn_weight, out_weight, cot,
        pair_next, pair_grad, bias_weight_grad, denoised, token_grad, weight_grad, *refs[41:-7],
    )


def work(
    stored, loaded, sem_in, given, results, sem_out,
    pair, mask, chain, tri_in_gain, tri_proj, tri_gate, tri_out_gain, tri_out, bias_gain,
    bias_weight, chain_bias, tokens, level, attn_gain, attn_weight, out_weight, cot,
    pair_next, pair_grad, bias_weight_grad, denoised, token_grad, weight_grad,
    gate_scr, r_send, l_send, r_own, l_own, r_all, left_t, t_send, t_recv, row_scr, upd_scr,
    bias_in_scr, bw_pad, b_send, b_recv, b_all, w_four, ow_pad, place, w_own, w_rem, hid_scr, qkv_scr,
    sig_scr, slope_scr, ga_scr, score_scr, prob_scr, raw, raw_z, part, part_x, bs_send, bs_recv, bb_send, bb_recv, ws_send,
    ws_half, ws_sum, ws_recv, ar_one, ar_all, ar_two, ar_fin,
    sems,
):
    group, row, col = lax.axis_index("group"), lax.axis_index("row"), lax.axis_index("col")
    mine = group * 8 + row
    core, high = row % 2, row // 2
    quad = group * 4 + high
    zed, ex = col // 4, col % 4
    keys, bulks = {}, {}

    def send(src, dst, key, device):
        at = keys.setdefault(key, len(keys))
        pltpu.make_async_remote_copy(
            src_ref=src, dst_ref=dst, send_sem=sems.at[0, at], recv_sem=sems.at[1, at],
            device_id=device, device_id_type=MESH,
        ).start()

    def arrive(key, bulk):
        bulks[key] = bulk
        pltpu.make_async_copy(bulk, bulk, sems.at[1, keys[key]]).wait()

    def col_at(step):
        return (zed + step // 4) % 4 * 4 + (ex + step % 4) % 4

    def to_col(step):
        return {"col": col_at(step)}

    def to_line(step):
        there = (mine + step) % S
        return {"group": there // 8, "row": there % 8}

    stores = [
        pltpu.make_async_copy(src, dst, sem_out.at[k])
        for k, (src, dst) in enumerate(zip(results, given, strict=True))
    ]
    barrier = pltpu.get_barrier_semaphore()
    for step in range(1, S):
        pl.semaphore_signal(barrier, inc=1, device_id=to_col(step), device_id_type=MESH)
        pl.semaphore_signal(barrier, inc=1, device_id=to_line(step), device_id_type=MESH)

    loads = [
        pltpu.make_async_copy(src, dst, sem_in.at[k])
        for k, (src, dst) in enumerate(zip(stored, loaded, strict=True))
    ]
    first, second = (0, 1, 3, 4, 5), (14, 15, 9, 11, 12, 13, 16, 2, 6, 7, 8, 10)
    for k in first + second:
        loads[k].start()
    for k in first:
        loads[k].wait()
    tile = pair[...].astype(F32).reshape(N, C)
    centred, inverse = centred_inverse(tile)
    pair_in = (centred * inverse * tri_in_gain[...]).astype(BF16)
    pick = (iota((N, S), 0) // S == iota((N, S), 1)).astype(BF16)
    spread = dot(pick, mask[...].astype(F32).astype(BF16))
    mask_col = jnp.sum(
        jnp.where(iota((N, S), 0) % S == iota((N, S), 1), spread, 0.0), -1, keepdims=True
    )
    right = dot(pair_in, tri_proj[:, 2 * C : 4 * C])
    right = sigmoid(right[:, :C]) * right[:, C:] * mask_col
    r_send[...] = swap_blocks(right, 8).astype(BF16).reshape(S, S, C)
    pl.semaphore_wait(barrier, 2 * (S - 1))
    for d in range(1, S):
        send(r_send.at[col_at(d)], r_own.at[col], ("r", d // 4), to_col(d))
    r_own[col] = r_send[col]
    left = dot(pair_in, tri_proj[:, : 2 * C])
    left = sigmoid(left[:, :C]) * left[:, C:] * mask_col
    l_send[...] = swap_blocks(left, 8).astype(BF16).reshape(S, S, C)
    for d in range(1, S):
        send(l_send.at[col_at(d)], l_own.at[col], "l", to_col(d))
    l_own[col] = l_send[col]
    gate_scr[...] = sigmoid(dot(pair_in, tri_gate[...]))

    for k in second:
        loads[k].wait()
    for g in range(4):
        w_own[3 * g : 3 * g + 3] = attn_weight[g].reshape(3, S, D)
    w_own[12:15] = out_weight[...].reshape(3, S, D)
    w_own[15] = jnp.zeros((S, D), BF16)
    w_four[...] = jnp.zeros_like(w_four)
    for g in range(4):
        w_four[g * C : g * C + E, :] = attn_weight[g]
    ow_pad[...] = jnp.zeros_like(ow_pad)
    ow_pad[:E, :] = out_weight[...]
    bw_pad[...] = jnp.zeros_like(bw_pad)
    bw_pad[:S, :] = bias_weight[...]
    place_row = iota((5 * C, N), 0)
    inner = place_row % C
    place[...] = jnp.where(
        (inner < E) & (iota((5 * C, N), 1) == place_row // C * E + inner), 1.0, 0.0
    ).astype(BF16)

    scale_of = []
    for t in range(T):
        power = jnp.full((1, C), level[t].astype(F32)) * (math.log(SIGMA_SPAN) / (LEVELS - 1))
        sigma = SIGMA_LOW * jnp.exp(power)
        scale_of.append(lax.rsqrt(1.0 + sigma * sigma)[:, :1])
    inverse_root = 1.0 / math.sqrt(E)

    def before_bias(t):
        scaled = tokens[t].astype(F32) * scale_of[t]
        mid, inv = centred_inverse(scaled)
        hidden = (mid * inv * attn_gain[...].reshape(1, D)).astype(BF16)
        hid_scr[t] = hidden
        projections = dot_nt(hidden, w_four[...])
        for g in range(3):
            qkv_scr[t, g] = projections[:, g * C : (g + 1) * C].astype(BF16)
        gate_sig = sigmoid(projections[:, 3 * C :])
        grad_gated = dot_nt(cot[t], ow_pad[...])
        grad_attended = (grad_gated * gate_sig).astype(BF16)
        sig_scr[t] = gate_sig
        slope_scr[t] = grad_gated * gate_sig * (1.0 - gate_sig)
        ga_scr[t] = grad_attended
        score_scr[t] = dot_nt(qkv_scr[t, 0], qkv_scr[t, 1]) * inverse_root
        prob_scr[t] = dot_nt(grad_attended, qkv_scr[t, 2])

    before_bias(0)

    partner = {"row": high * 2 + 1 - core}

    def to_quad(k):
        return {"group": (quad + k) % 8 // 4, "row": (quad + k) % 4 * 2 + core}

    def from_quad(k, side):
        there = (quad + 8 - k) % 8
        return there // 4 * 8 + there % 4 * 2 + side

    def z_block(dz):
        return pl.ds((zed + 4 - dz) % 4 * 4, 4)

    def ag_key(dz, k):
        return ("ag", dz, k) if dz == 2 else ("ag", dz)

    def fw_key(dz, k):
        return ("fw", dz, k) if dz == 2 else ("fw", dz)

    def spread_right(dz):
        arrive(("r", dz), r_own.at[pl.ds(0, 4 if dz else 3)])
        block = r_own.at[z_block(dz)]
        there = r_all.at[mine, z_block(dz)]
        for k in range(1, 8):
            send(block, there, ag_key(dz, k), to_quad(k))
        send(block, there, fw_key(dz, 0), partner)

    def relay(dz, k):
        block = r_all.at[from_quad(k, core), z_block(dz)]
        send(block, block, fw_key(dz, k), partner)

    spread_right(0)
    spread_right(1)
    spread_right(3)
    spread_right(2)
    before_bias(1)
    arrive("l", l_own.at[pl.ds(0, S - 1)])
    for d in range(1, 4):
        send(w_own.at[mine], w_rem.at[mine, d - 1], "w", {"col": (zed + 4 - d) % 4 * 4 + ex})
    left_t[...] = l_own[...].reshape(N, C).astype(F32).T.astype(BF16)
    diagonal = iota((C, C), 0) % 8 == iota((C, C), 1) % 8

    def triangle(at, block):
        product = dot(left_t[...], block.reshape(N, C))
        product = jnp.where(diagonal, product, 0.0).reshape(S, 8, C)
        t_send[at] = jnp.sum(product, axis=1).astype(BF16)

    triangle(mine, r_own[...])
    for dz in (0, 1, 3):
        arrive(("ag", dz), r_all.at[pl.ds(0, 7), pl.ds(0, 4)])
        for k in range(1, 8):
            relay(dz, k)
    before_bias(2)
    for k in range(1, 8):
        arrive(("ag", 2, k), r_all.at[0, pl.ds(0, 4)])
        relay(2, k)
        triangle(from_quad(k, core), r_all[from_quad(k, core)])
    for dz in (0, 1, 3):
        arrive(("fw", dz), r_all.at[pl.ds(0, 8), pl.ds(0, 4)])
    for k in range(8):
        arrive(("fw", 2, k), r_all.at[0, pl.ds(0, 4)])
        triangle(from_quad(k, 1 - core), r_all[from_quad(k, 1 - core)])
    for d in range(1, S):
        send(t_send.at[col_at(d)], t_recv.at[col], "t", to_col(d))
    t_recv[col] = t_send[col]

    arrive("t", t_recv.at[pl.ds(0, S - 1)])
    moved = swap_blocks(t_recv[...].astype(F32).reshape(N, C), 8)
    for j in range(S):
        row_scr[pl.ds(j, S, stride=S), :] = moved[j * S : (j + 1) * S]
    centred, inverse = centred_inverse(row_scr[...])
    tri_normed = (centred * inverse * tri_out_gain[...]).astype(BF16)
    tile = pair[...].astype(F32).reshape(N, C)
    updated = tile + gate_scr[...] * dot(tri_normed, tri_out[...])
    upd_scr[...] = updated
    centred, inverse = centred_inverse(updated)
    bias_in = (centred * inverse * bias_gain[...]).astype(BF16)
    bias_in_scr[...] = bias_in
    by_head = dot_nt(bw_pad[:S, :], bias_in)
    ids = chain[...].astype(F32)
    eye = iota((N, N), 0) == iota((N, N), 1)
    ids_col = jnp.sum(jnp.where(eye, ids, 0.0), -1, keepdims=True)
    lane = iota((N, N), 1)
    row_of = mine * S + lane // S == iota((N, N), 0)
    row_chain = jnp.sum(jnp.where(row_of, ids_col, 0.0), 0, keepdims=True)
    col_of = col * S + lane % S == iota((N, N), 0)
    col_chain = jnp.sum(jnp.where(col_of, ids_col, 0.0), 0, keepdims=True)
    head_bias = jnp.sum(
        jnp.where(iota((S, S), 1) == iota((S, S), 0), chain_bias[...], 0.0), -1, keepdims=True
    )
    by_head = by_head + jnp.where(row_chain == col_chain, head_bias, 0.0)
    for k in range(S):
        b_send[k] = by_head[k : k + 1]
    for d in range(1, S):
        send(b_send.at[col_at(d)], b_recv.at[col], "b", to_col(d))
    arrive("w", w_rem.at[0])
    for k in range(1, 8):
        send(w_rem.at[mine], w_rem.at[mine], "wg", to_quad(k))
    send(w_rem.at[mine], w_rem.at[mine], "wf", partner)
    b_recv[col] = b_send[col]
    pair_next[...] = updated.astype(BF16)
    stores[0].start()
    arrive("b", b_recv.at[pl.ds(0, S - 1)])
    by_row = swap_rows(jnp.concatenate([b_recv[k] for k in range(S)], axis=0))
    b_all[mine] = by_row.astype(BF16)
    for d in range(1, S):
        send(b_all.at[mine], b_all.at[mine], "ba", to_line(d))
    arrive("ba", b_all.at[pl.ds(0, S - 1)])

    bias = b_all[...].reshape(N, N).astype(F32)
    copies = range(T)
    exponent = [jnp.exp(score_scr[t] + bias) for t in copies]
    attention = [e / jnp.sum(e, -1, keepdims=True) for e in exponent]
    attention_b = [a.astype(BF16) for a in attention]
    grad_score = [
        a * (prob_scr[t] - jnp.sum(a * prob_scr[t], -1, keepdims=True))
        for t, a in enumerate(attention)
    ]
    bs_send[...] = sum(grad_score[1:], grad_score[0]).astype(BF16).reshape(S, S, N)
    for d in range(1, S):
        send(bs_send.at[(mine + d) % S], bs_recv.at[mine], "bs", to_line(d))
    bs_recv[mine] = bs_send[mine]
    score_b = [g.astype(BF16) for g in grad_score]
    attended = [dot(attention_b[t], qkv_scr[t, 2]) for t in copies]
    grad_values = [dot_tn(attention_b[t], ga_scr[t]).astype(BF16) for t in copies]
    grad_queries = [(dot(score_b[t], qkv_scr[t, 1]) * inverse_root).astype(BF16) for t in copies]
    grad_keys = [(dot_tn(score_b[t], qkv_scr[t, 0]) * inverse_root).astype(BF16) for t in copies]
    gated = [(sig_scr[t] * attended[t]).astype(BF16) for t in copies]
    grad_gate = [(slope_scr[t] * attended[t]).astype(BF16) for t in copies]
    for t in copies:
        side = jnp.concatenate(
            [grad_queries[t], grad_keys[t], grad_values[t], grad_gate[t], gated[t]], axis=1
        )
        raw[t] = dot(side, place[...]).astype(BF16).reshape(4, 64, N)
    def spread_raw(t):
        for d in (2, 1, 3):
            there = (zed + 4 - d) % 4
            send(raw.at[t, there], raw_z.at[t, d - 1], ("z", t), {"col": there * 4 + ex})

    spread_raw(0)
    raw_t = raw[...].reshape(T * N, N).astype(F32).T.astype(BF16)
    grads_part = dot(raw_t[: 4 * E], hid_scr[...].reshape(T * N, D))
    out_part = dot(raw_t[4 * E :], cot[...].reshape(T * N, D))
    turned = jnp.concatenate([grads_part, out_part], axis=0).T
    for k in range(S):
        ws_send[k % 2, k // 2] = turned[k * E : (k + 1) * E].astype(BF16)
    send(ws_send.at[1 - core], ws_half, "wh", partner)
    arrive("wg", w_rem.at[pl.ds(0, 7)])
    for k in range(1, 8):
        at = from_quad(k, core)
        send(w_rem.at[at], w_rem.at[at], "wf", partner)
    def project(t):
        arrive(("z", t), raw_z.at[t])
        total = jnp.zeros((C, D), F32)
        first = iota((64, N), 1) < 4 * E
        for d in range(4):
            piece = (raw_z[t, d - 1] if d else raw[t, zed]).astype(F32)
            weights = w_rem[:, d - 1] if d else w_own[...]
            both = jnp.concatenate(
                [jnp.where(first, piece, 0.0), jnp.where(first, 0.0, piece)], axis=0
            ).astype(BF16)
            total = total + dot(both, weights.reshape(N, D))
        total = total.astype(BF16)
        for x in range(4):
            part[t, x, 0] = total[x * S : (x + 1) * S]
            part[t, x, 1] = total[64 + x * S : 64 + (x + 1) * S]
        for d in range(1, 4):
            there = (ex + d) % 4
            send(part.at[t, there], part_x.at[t, d - 1], ("x", t), {"col": zed * 4 + there})

    def finish(t):
        arrive(("x", t), part_x.at[t])
        sums = part[t, ex].astype(F32)
        for d in range(3):
            sums = sums + part_x[t, d].astype(F32)
        first = pl.multiple_of(col * S, S)
        scaled = tokens[t, pl.ds(first, S), :].astype(F32) * scale_of[t]
        cot_mine = cot[t, pl.ds(first, S), :].astype(F32)
        denoised[t] = (scaled + sums[1]).astype(BF16)
        back = norm_back(sums[0], scaled, attn_gain[...].reshape(1, D))
        token_grad[t] = (scale_of[t] * (cot_mine + back)).astype(BF16)

    arrive("bs", bs_recv.at[pl.ds(0, S - 1)])
    by_tile = swap_rows(jnp.sum(bs_recv[...].astype(F32), axis=0))
    for k in range(S):
        bb_send[k] = by_tile[k : k + 1]
    for d in range(1, S):
        send(bb_send.at[col_at(d)], bb_recv.at[col], "bb", to_col(d))
    bb_recv[col] = bb_send[col]
    spread_raw(1)
    spread_raw(2)
    arrive("wh", ws_half)
    ws_sum[...] = (ws_send[core].astype(F32) + ws_half[...].astype(F32)).astype(BF16)
    arrive("wf", w_rem.at[pl.ds(0, 8)])
    project(0)
    arrive("bb", bb_recv.at[pl.ds(0, S - 1)])
    grad_bias = jnp.concatenate([bb_recv[k] for k in range(S)], axis=0).astype(BF16)
    ar_one[...] = dot(grad_bias, bias_in_scr[...]).astype(BF16)
    for d in range(1, S):
        send(ar_one, ar_all.at[mine], "a1", to_line(d))
    ar_all[mine] = ar_one[...]
    grad_in = dot_tn(grad_bias, bw_pad[:S, :])
    pair_grad[...] = norm_back(grad_in, upd_scr[...], bias_gain[...])
    stores[1].start()
    for k in range(1, 8):
        send(ws_sum.at[(quad + k) % 8], ws_recv.at[quad], "ws", to_quad(k))
    ws_recv[quad] = ws_sum[quad]
    project(1)
    project(2)
    arrive("a1", ar_all.at[pl.ds(0, S - 1)])
    ar_two[...] = jnp.sum(ar_all[...].astype(F32), axis=0).astype(BF16)
    for d in range(1, S):
        send(ar_two, ar_fin.at[col], "a2", to_col(d))
    ar_fin[col] = ar_two[...]
    finish(0)
    finish(1)
    finish(2)
    stores[3].start()
    stores[4].start()
    arrive("ws", ws_recv.at[pl.ds(0, 7)])
    weight_grad[...] = jnp.sum(ws_recv[...].astype(F32), axis=0)
    stores[5].start()
    arrive("a2", ar_fin.at[pl.ds(0, S - 1)])
    bias_weight_grad[...] = jnp.sum(ar_fin[...].astype(F32), axis=0)
    stores[2].start()
    for key, bulk in bulks.items():
        pltpu.make_async_copy(bulk, bulk, sems.at[0, keys[key]]).wait()
    for copy in stores:
        copy.wait()


def finisher(*refs):
    sums = refs[5]
    for at in range(5):
        refs[6 + at][...] = refs[at][...]
    for g in range(4):
        refs[11][g] = sums[:, g * E : (g + 1) * E]
    refs[12][...] = pltpu.roll(sums[:, C:], C // 2, 1).T[:E]


def shards(
    pair_repr, pair_mask, chain_id, tri_in_gain, tri_proj, tri_gate, tri_out_gain, tri_out,
    bias_gain, bias_weight, chain_bias, tokens, noise_level, attn_gain, attn_weight, out_weight,
    cotangent,
):
    vmem = pl.BlockSpec(memory_space=pltpu.VMEM)
    hbm = pl.BlockSpec(memory_space=pltpu.HBM)

    def buf(*shape, kind=BF16):
        return pltpu.VMEM(shape, kind)

    outs = pl.pallas_call(
        kernel,
        out_shape=(
            jax.ShapeDtypeStruct((N, C), BF16),
            jax.ShapeDtypeStruct((N, C), F32),
            jax.ShapeDtypeStruct((S, C), F32),
            jax.ShapeDtypeStruct((T, S, D), BF16),
            jax.ShapeDtypeStruct((T, S, D), BF16),
            jax.ShapeDtypeStruct((E, N), F32),
        ),
        in_specs=[hbm] * 17,
        out_specs=(hbm,) * 6,
        scratch_shapes=[
            buf(S, S, C), buf(S, S, kind=jnp.int32), buf(1, N, kind=jnp.int32),
            buf(1, C, kind=F32), buf(C, 4 * C), buf(C, C), buf(1, C, kind=F32), buf(C, C),
            buf(1, C, kind=F32), buf(S, C), buf(1, S, kind=F32), buf(T, N, D),
            pltpu.SMEM((T,), jnp.int32), buf(D, kind=F32), buf(4, E, D), buf(E, D), buf(T, N, D),
            pltpu.SemaphoreType.DMA((17,)),
            buf(N, C, kind=F32),
            buf(S, S, C), buf(S, S, C), buf(S, S, C), buf(S, S, C),
            buf(S, S, S, C),
            buf(C, N),
            buf(S, S, C), buf(S, S, C),
            buf(N, C, kind=F32), buf(N, C, kind=F32),
            buf(N, C), buf(C, C),
            buf(S, 1, N, kind=F32), buf(S, 1, N, kind=F32), buf(S, S, N),
            buf(4 * C, D), buf(C, D), buf(5 * C, N),
            buf(S, S, D), buf(S, 3, S, D),
            buf(T, N, D), buf(T, 3, N, C),
            buf(T, N, C, kind=F32), buf(T, N, C, kind=F32), buf(T, N, C),
            buf(T, N, N, kind=F32), buf(T, N, N, kind=F32),
            buf(T, 4, 64, N), buf(T, 3, 64, N),
            buf(T, 4, 2, S, D), buf(T, 3, 2, S, D),
            buf(S, S, N), buf(S, S, N),
            buf(S, 1, N, kind=F32), buf(S, 1, N, kind=F32),
            buf(2, 8, E, N), buf(8, E, N), buf(8, E, N), buf(8, E, N),
            buf(S, C), buf(S, S, C), buf(S, C), buf(S, S, C),
            pltpu.SemaphoreType.DMA((2, 45)),
            buf(N, C), buf(N, C, kind=F32), buf(S, C, kind=F32), buf(T, S, D), buf(T, S, D),
            buf(E, N, kind=F32), pltpu.SemaphoreType.DMA((6,)),
        ],
        compiler_params=pltpu.CompilerParams(
            collective_id=0, has_side_effects=True, vmem_limit_bytes=30 * 1024 * 1024
        ),
    )(*[pltpu.with_memory_space_constraint(array, pltpu.HBM) for array in (
        pair_repr, pair_mask, chain_id.reshape(1, N), tri_in_gain.reshape(1, C), tri_proj,
        tri_gate, tri_out_gain.reshape(1, C), tri_out, bias_gain.reshape(1, C), bias_weight.T,
        chain_bias.reshape(1, S), tokens, noise_level, attn_gain,
        jnp.transpose(attn_weight, (0, 2, 1)), out_weight, cotangent,
    )])
    outs = pl.pallas_call(
        finisher,
        out_shape=(
            jax.ShapeDtypeStruct((N, C), BF16),
            jax.ShapeDtypeStruct((N, C), F32),
            jax.ShapeDtypeStruct((S, C), F32),
            jax.ShapeDtypeStruct((T, S, D), BF16),
            jax.ShapeDtypeStruct((T, S, D), BF16),
            jax.ShapeDtypeStruct((4, E, E), F32),
            jax.ShapeDtypeStruct((E, E), F32),
        ),
        in_specs=[vmem] * 6,
        out_specs=(vmem,) * 7,
        compiler_params=pltpu.CompilerParams(vmem_limit_bytes=4 * 1024 * 1024),
    )(*outs)
    pair_next, pair_grad, bias_weight_grad, denoised, token_grad, weight_grad, out_grad = outs
    return (
        pair_next.reshape(S, S, C),
        pair_grad.reshape(S, S, C),
        bias_weight_grad.T,
        denoised,
        token_grad,
        weight_grad,
        out_grad,
    )


def solution(mesh):
    line, col = ("group", "row"), "col"
    return jax.shard_map(
        shards,
        mesh=mesh,
        in_specs=(
            P(line, col, None), P(line, col), P(), P(), P(), P(), P(), P(), P(), P(), P(),
            P(line, None, None), P(line), P(), P(None, None, col), P(col, None),
            P(line, None, None),
        ),
        out_specs=(
            P(line, col, None), P(line, col, None), P(), P(line, col, None),
            P(line, col, None), P(None, line, col), P(col, line),
        ),
        check_vma=False,
    )
```

```python
import math

import jax
import jax.numpy as jnp
from jax import lax
from jax.experimental import pallas as pl
from jax.experimental.pallas import tpu as pltpu
from jax.sharding import PartitionSpec as P

MESH = pl.DeviceIdType.MESH
LEVELS = 200
EPSILON = 1e-05
SIGMA_LOW = 0.1
SIGMA_SPAN = 100.0
F32 = jnp.float32
BF16 = jnp.bfloat16
S = 16
C = 128
E = 48
D = 768
N = 256
T = 3
NT = (((1,), (1,)), ((), ()))
TN = (((0,), (0,)), ((), ()))


def iota(shape, dim):
    return lax.broadcasted_iota(jnp.int32, shape, dim)


def dot(a, b):
    return jnp.dot(a, b, preferred_element_type=F32)


def dot_nt(a, b):
    return lax.dot_general(a, b, NT, preferred_element_type=F32)


def dot_tn(a, b):
    return lax.dot_general(a, b, TN, preferred_element_type=F32)


def sigmoid(v):
    return 1.0 / (1.0 + jnp.exp(-v))


def centred_inverse(v):
    centred = v - jnp.mean(v, -1, keepdims=True)
    return centred, lax.rsqrt(jnp.mean(centred * centred, -1, keepdims=True) + EPSILON)


def norm_back(gradient, values, gain):
    centred, inverse = centred_inverse(values)
    normed = centred * inverse
    weighted = gradient * gain
    return inverse * (
        weighted
        - jnp.mean(weighted, -1, keepdims=True)
        - normed * jnp.mean(weighted * normed, -1, keepdims=True)
    )


def swap_blocks(x, unit):
    arr = iota(x.shape, 0) // S
    blk = iota(x.shape, 1) // unit
    for bit in (1, 2, 4, 8):
        rows = bit * S
        other = jnp.concatenate(
            [x[(k ^ 1) * rows : (k ^ 1) * rows + rows] for k in range(N // rows)], axis=0
        )
        up = pltpu.roll(other, bit * unit, 1)
        down = pltpu.roll(other, C - bit * unit, 1)
        in_arr, in_blk = (arr & bit) != 0, (blk & bit) != 0
        x = jnp.where(in_arr == in_blk, x, jnp.where(in_blk, up, down))
    return x


def swap_rows(x):
    arr, blk = iota(x.shape, 0), iota(x.shape, 1) // S
    for bit in (1, 2, 4, 8):
        in_arr, in_blk = (arr & bit) != 0, (blk & bit) != 0
        other = jnp.where(in_arr, pltpu.roll(x, bit, 0), pltpu.roll(x, S - bit, 0))
        up = pltpu.roll(other, bit * S, 1)
        down = pltpu.roll(other, N - bit * S, 1)
        x = jnp.where(in_arr == in_blk, x, jnp.where(in_blk, up, down))
    return x


def kernel(
    *refs,
):
    (
        pair, mask, chain, tri_in_gain, tri_proj, tri_gate, tri_out_gain, tri_out, bias_gain,
        bias_weight, chain_bias, tokens, level, attn_gain, attn_weight, out_weight, cot,
    ) = refs[23:40]
    results, sem_out = refs[-7:-1], refs[-1]
    pair_next, pair_grad, bias_weight_grad, denoised, token_grad, weight_grad = results
    work(
        refs[:17], refs[23:40], refs[40], refs[17:23], results, sem_out,
        pair, mask, chain, tri_in_gain, tri_proj, tri_gate, tri_out_gain, tri_out, bias_gain,
        bias_weight, chain_bias, tokens, level, attn_gain, attn_weight, out_weight, cot,
        pair_next, pair_grad, bias_weight_grad, denoised, token_grad, weight_grad, *refs[41:-7],
    )


def work(
    stored, loaded, sem_in, given, results, sem_out,
    pair, mask, chain, tri_in_gain, tri_proj, tri_gate, tri_out_gain, tri_out, bias_gain,
    bias_weight, chain_bias, tokens, level, attn_gain, attn_weight, out_weight, cot,
    pair_next, pair_grad, bias_weight_grad, denoised, token_grad, weight_grad,
    gate_scr, r_send, l_send, r_own, l_own, r_all, left_t, t_send, t_recv, row_scr, upd_scr,
    bias_in_scr, bw_pad, b_send, b_recv, b_all, w_four, ow_pad, place, w_own, w_rem, hid_scr, qkv_scr,
    sig_scr, slope_scr, ga_scr, score_scr, prob_scr, raw, raw_z, part, part_x, bs_send, bs_recv, bb_send, bb_recv, ws_send,
    ws_half, ws_sum, ws_recv, ar_one, ar_all, ar_two, ar_fin,
    sems,
):
    group, row, col = lax.axis_index("group"), lax.axis_index("row"), lax.axis_index("col")
    mine = group * 8 + row
    core, high = row % 2, row // 2
    quad = group * 4 + high
    zed, ex = col // 4, col % 4
    keys, bulks = {}, {}

    def send(src, dst, key, device):
        at = keys.setdefault(key, len(keys))
        pltpu.make_async_remote_copy(
            src_ref=src, dst_ref=dst, send_sem=sems.at[0, at], recv_sem=sems.at[1, at],
            device_id=device, device_id_type=MESH,
        ).start()

    def arrive(key, bulk):
        bulks[key] = bulk
        pltpu.make_async_copy(bulk, bulk, sems.at[1, keys[key]]).wait()

    def col_at(step):
        return (zed + step // 4) % 4 * 4 + (ex + step % 4) % 4

    def to_col(step):
        return {"col": col_at(step)}

    def to_line(step):
        there = (mine + step) % S
        return {"group": there // 8, "row": there % 8}

    stores = [
        pltpu.make_async_copy(src, dst, sem_out.at[k])
        for k, (src, dst) in enumerate(zip(results, given, strict=True))
    ]
    def to_plane(step):
        return {"row": (row + step % 8) % 8, "col": zed * 4 + (ex + step // 8) % 4}

    def to_depth(step):
        return {"group": (group + step) % 2, "col": (zed + step // 2) % 4 * 4 + ex}

    barrier = pltpu.get_barrier_semaphore()
    for step in range(1, S):
        pl.semaphore_signal(barrier, inc=1, device_id=to_col(step), device_id_type=MESH)
        pl.semaphore_signal(barrier, inc=1, device_id=to_line(step), device_id_type=MESH)
    greeted = 2 * (S - 1)
    others = [to_plane(k) for k in range(9, 32) if k % 8]
    others += [to_depth(k) for k in (3, 5, 7)]
    others += [{"row": high * 2 + 1 - core, "col": col_at(d)} for d in range(4, S)]
    for there in others:
        pl.semaphore_signal(barrier, inc=1, device_id=there, device_id_type=MESH)
    greeted += len(others)

    loads = [
        pltpu.make_async_copy(src, dst, sem_in.at[k])
        for k, (src, dst) in enumerate(zip(stored, loaded, strict=True))
    ]
    first, second = (0, 1, 3, 4, 5), (14, 15, 9, 11, 12, 13, 16, 2, 6, 7, 8, 10)
    for k in first + second:
        loads[k].start()
    for k in first:
        loads[k].wait()
    tile = pair[...].astype(F32).reshape(N, C)
    centred, inverse = centred_inverse(tile)
    pair_in = (centred * inverse * tri_in_gain[...]).astype(BF16)
    pick = (iota((N, S), 0) // S == iota((N, S), 1)).astype(BF16)
    spread = dot(pick, mask[...].astype(F32).astype(BF16))
    mask_col = jnp.sum(
        jnp.where(iota((N, S), 0) % S == iota((N, S), 1), spread, 0.0), -1, keepdims=True
    )
    right = dot(pair_in, tri_proj[:, 2 * C : 4 * C])
    right = sigmoid(right[:, :C]) * right[:, C:] * mask_col
    r_send[...] = swap_blocks(right, 8).astype(BF16).reshape(S, S, C)
    pl.semaphore_wait(barrier, greeted)
    for d in range(1, S):
        send(r_send.at[col_at(d)], r_own.at[col], ("r", d // 4), to_col(d))
    r_own[col] = r_send[col]
    left = dot(pair_in, tri_proj[:, : 2 * C])
    left = sigmoid(left[:, :C]) * left[:, C:] * mask_col
    l_send[...] = swap_blocks(left, 8).astype(BF16).reshape(S, S, C)
    for d in range(1, S):
        send(l_send.at[col_at(d)], l_own.at[col], "l", to_col(d))
    l_own[col] = l_send[col]
    gate_scr[...] = sigmoid(dot(pair_in, tri_gate[...]))

    for k in second:
        loads[k].wait()
    for g in range(4):
        w_own[3 * g : 3 * g + 3] = attn_weight[g].reshape(3, S, D)
    w_own[12:15] = out_weight[...].reshape(3, S, D)
    w_own[15] = jnp.zeros((S, D), BF16)
    w_four[...] = jnp.zeros_like(w_four)
    for g in range(4):
        w_four[g * C : g * C + E, :] = attn_weight[g]
    ow_pad[...] = jnp.zeros_like(ow_pad)
    ow_pad[:E, :] = out_weight[...]
    bw_pad[...] = jnp.zeros_like(bw_pad)
    bw_pad[:S, :] = bias_weight[...]
    place_row = iota((5 * C, N), 0)
    inner = place_row % C
    place[...] = jnp.where(
        (inner < E) & (iota((5 * C, N), 1) == place_row // C * E + inner), 1.0, 0.0
    ).astype(BF16)

    scale_of = []
    for t in range(T):
        power = jnp.full((1, C), level[t].astype(F32)) * (math.log(SIGMA_SPAN) / (LEVELS - 1))
        sigma = SIGMA_LOW * jnp.exp(power)
        scale_of.append(lax.rsqrt(1.0 + sigma * sigma)[:, :1])
    inverse_root = 1.0 / math.sqrt(E)

    def before_bias(t):
        scaled = tokens[t].astype(F32) * scale_of[t]
        mid, inv = centred_inverse(scaled)
        hidden = (mid * inv * attn_gain[...].reshape(1, D)).astype(BF16)
        hid_scr[t] = hidden
        projections = dot_nt(hidden, w_four[...])
        for g in range(3):
            qkv_scr[t, g] = projections[:, g * C : (g + 1) * C].astype(BF16)
        gate_sig = sigmoid(projections[:, 3 * C :])
        grad_gated = dot_nt(cot[t], ow_pad[...])
        grad_attended = (grad_gated * gate_sig).astype(BF16)
        sig_scr[t] = gate_sig
        slope_scr[t] = grad_gated * gate_sig * (1.0 - gate_sig)
        ga_scr[t] = grad_attended
        score_scr[t] = dot_nt(qkv_scr[t, 0], qkv_scr[t, 1]) * inverse_root
        prob_scr[t] = dot_nt(grad_attended, qkv_scr[t, 2])

    before_bias(0)

    partner = {"row": high * 2 + 1 - core}

    def to_quad(k):
        return {"group": (quad + k) % 8 // 4, "row": (quad + k) % 4 * 2 + core}

    def from_quad(k, side):
        there = (quad + 8 - k) % 8
        return there // 4 * 8 + there % 4 * 2 + side

    def z_block(dz):
        return pl.ds((zed + 4 - dz) % 4 * 4, 4)

    def ag_key(dz, k):
        return ("ag", dz, k) if dz == 2 else ("ag", dz)

    def spread_right(dz):
        arrive(("r", dz), r_own.at[pl.ds(0, 4 if dz else 3)])
        for k in range(1, 8):
            send(r_own.at[z_block(dz)], r_all.at[quad, z_block(dz)], ag_key(dz, k), to_quad(k))

    spread_right(0)
    spread_right(1)
    spread_right(3)
    spread_right(2)
    before_bias(1)
    arrive("l", l_own.at[pl.ds(0, S - 1)])
    for d in range(1, 4):
        send(w_own.at[mine], w_rem.at[mine, d - 1], "w", {"col": (zed + 4 - d) % 4 * 4 + ex})
    left_t[core] = l_own[...].reshape(N, C).astype(F32).T.astype(BF16)
    send(left_t.at[core], left_t.at[core], "lt", partner)
    diagonal = iota((2 * C, C), 0) % 8 == iota((2 * C, C), 1) % 8

    def triangle(at, block):
        product = dot(left_t[...].reshape(2 * C, N), block.reshape(N, C))
        product = jnp.where(diagonal, product, 0.0).reshape(2 * S, 8, C)
        product = jnp.sum(product, axis=1).astype(BF16)
        t_send[0, at] = product[:S]
        t_send[1, at] = product[S:]

    before_bias(2)
    arrive("lt", left_t.at[0])
    triangle(quad, r_own[...])
    for dz in (0, 1, 3):
        arrive(("ag", dz), r_all.at[pl.ds(0, 7), pl.ds(0, 4)])
    for k in range(1, 8):
        arrive(("ag", 2, k), r_all.at[0, pl.ds(0, 4)])
        at = (quad + 8 - k) % 8
        triangle(at, r_all[at])
    same = col % 2 == core
    for m in range(8):
        at = (col // 2 + m) % 8
        there = 2 * at + core
        if m:
            send(t_send.at[core, at], t_recv.at[col], "t", {"col": there})
        send(
            t_send.at[1 - core, at], t_recv.at[col], "t",
            {"row": high * 2 + 1 - core, "col": there},
        )
    near = col // 2

    @pl.when(same)
    def _():
        pltpu.make_async_copy(
            t_send.at[core, near], t_recv.at[col], sems.at[1, keys["t"]]
        ).start()

    @pl.when(jnp.logical_not(same))
    def _():
        send(t_send.at[core, near], t_recv.at[col], "t", {"col": 2 * near + core})

    arrive("t", t_recv)
    bulks["t"] = t_recv.at[pl.ds(0, S - 1)]
    moved = swap_blocks(t_recv[...].astype(F32).reshape(N, C), 8)
    for j in range(S):
        row_scr[pl.ds(j, S, stride=S), :] = moved[j * S : (j + 1) * S]
    centred, inverse = centred_inverse(row_scr[...])
    tri_normed = (centred * inverse * tri_out_gain[...]).astype(BF16)
    tile = pair[...].astype(F32).reshape(N, C)
    updated = tile + gate_scr[...] * dot(tri_normed, tri_out[...])
    upd_scr[...] = updated
    centred, inverse = centred_inverse(updated)
    bias_in = (centred * inverse * bias_gain[...]).astype(BF16)
    bias_in_scr[...] = bias_in
    by_head = dot_nt(bw_pad[:S, :], bias_in)
    ids = chain[...].astype(F32)
    eye = iota((N, N), 0) == iota((N, N), 1)
    ids_col = jnp.sum(jnp.where(eye, ids, 0.0), -1, keepdims=True)
    lane = iota((N, N), 1)
    row_of = mine * S + lane // S == iota((N, N), 0)
    row_chain = jnp.sum(jnp.where(row_of, ids_col, 0.0), 0, keepdims=True)
    col_of = col * S + lane % S == iota((N, N), 0)
    col_chain = jnp.sum(jnp.where(col_of, ids_col, 0.0), 0, keepdims=True)
    head_bias = jnp.sum(
        jnp.where(iota((S, S), 1) == iota((S, S), 0), chain_bias[...], 0.0), -1, keepdims=True
    )
    by_head = by_head + jnp.where(row_chain == col_chain, head_bias, 0.0)
    for k in range(S):
        b_send[k] = by_head[k : k + 1]
    for d in range(1, S):
        send(b_send.at[col_at(d)], b_recv.at[col], "b", to_col(d))
    arrive("w", w_rem.at[0])
    for k in range(1, 8):
        send(w_rem.at[mine], w_rem.at[mine], "wg", to_quad(k))
    send(w_rem.at[mine], w_rem.at[mine], "wf", partner)
    b_recv[col] = b_send[col]
    pair_next[...] = updated.astype(BF16)
    stores[0].start()
    arrive("b", b_recv.at[pl.ds(0, S - 1)])
    by_row = swap_rows(jnp.concatenate([b_recv[k] for k in range(S)], axis=0))
    b_all[mine] = by_row.astype(BF16)
    for d in range(1, S):
        send(b_all.at[mine], b_all.at[mine], "ba", to_line(d))
    arrive("ba", b_all.at[pl.ds(0, S - 1)])

    bias = b_all[...].reshape(N, N).astype(F32)
    copies = range(T)
    exponent = [jnp.exp(score_scr[t] + bias) for t in copies]
    attention = [e / jnp.sum(e, -1, keepdims=True) for e in exponent]
    attention_b = [a.astype(BF16) for a in attention]
    grad_score = [
        a * (prob_scr[t] - jnp.sum(a * prob_scr[t], -1, keepdims=True))
        for t, a in enumerate(attention)
    ]
    bs_send[...] = sum(grad_score[1:], grad_score[0]).astype(BF16).reshape(S, S, N)
    for d in range(1, S):
        send(bs_send.at[(mine + d) % S], bs_recv.at[mine], "bs", to_line(d))
    bs_recv[mine] = bs_send[mine]
    score_b = [g.astype(BF16) for g in grad_score]
    attended = [dot(attention_b[t], qkv_scr[t, 2]) for t in copies]
    grad_values = [dot_tn(attention_b[t], ga_scr[t]).astype(BF16) for t in copies]
    grad_queries = [(dot(score_b[t], qkv_scr[t, 1]) * inverse_root).astype(BF16) for t in copies]
    grad_keys = [(dot_tn(score_b[t], qkv_scr[t, 0]) * inverse_root).astype(BF16) for t in copies]
    gated = [(sig_scr[t] * attended[t]).astype(BF16) for t in copies]
    grad_gate = [(slope_scr[t] * attended[t]).astype(BF16) for t in copies]
    for t in copies:
        side = jnp.concatenate(
            [grad_queries[t], grad_keys[t], grad_values[t], grad_gate[t], gated[t]], axis=1
        )
        raw[t] = dot(side, place[...]).astype(BF16).reshape(4, 64, N)
    def spread_raw(t):
        for d in (2, 1, 3):
            there = (zed + 4 - d) % 4
            send(raw.at[t, there], raw_z.at[t, d - 1], ("z", t), {"col": there * 4 + ex})

    spread_raw(0)
    raw_t = raw[...].reshape(T * N, N).astype(F32).T.astype(BF16)
    grads_part = dot(raw_t[: 4 * E], hid_scr[...].reshape(T * N, D))
    out_part = dot(raw_t[4 * E :], cot[...].reshape(T * N, D))
    turned = jnp.concatenate([grads_part, out_part], axis=0).T
    for k in range(S):
        ws_send[k % 2, k // 2] = turned[k * E : (k + 1) * E].astype(BF16)
    send(ws_send.at[1 - core], ws_half, "wh", partner)
    arrive("wg", w_rem.at[pl.ds(0, 7)])
    for k in range(1, 8):
        at = from_quad(k, core)
        send(w_rem.at[at], w_rem.at[at], "wf", partner)
    def project(t):
        arrive(("z", t), raw_z.at[t])
        total = jnp.zeros((C, D), F32)
        first = iota((64, N), 1) < 4 * E
        for d in range(4):
            piece = (raw_z[t, d - 1] if d else raw[t, zed]).astype(F32)
            weights = w_rem[:, d - 1] if d else w_own[...]
            both = jnp.concatenate(
                [jnp.where(first, piece, 0.0), jnp.where(first, 0.0, piece)], axis=0
            ).astype(BF16)
            total = total + dot(both, weights.reshape(N, D))
        total = total.astype(BF16)
        for x in range(4):
            part[t, x, 0] = total[x * S : (x + 1) * S]
            part[t, x, 1] = total[64 + x * S : 64 + (x + 1) * S]
        for d in range(1, 4):
            there = (ex + d) % 4
            send(part.at[t, there], part_x.at[t, d - 1], ("x", t), {"col": zed * 4 + there})

    def finish(t):
        arrive(("x", t), part_x.at[t])
        sums = part[t, ex].astype(F32)
        for d in range(3):
            sums = sums + part_x[t, d].astype(F32)
        first = pl.multiple_of(col * S, S)
        scaled = tokens[t, pl.ds(first, S), :].astype(F32) * scale_of[t]
        cot_mine = cot[t, pl.ds(first, S), :].astype(F32)
        denoised[t] = (scaled + sums[1]).astype(BF16)
        back = norm_back(sums[0], scaled, attn_gain[...].reshape(1, D))
        token_grad[t] = (scale_of[t] * (cot_mine + back)).astype(BF16)

    arrive("bs", bs_recv.at[pl.ds(0, S - 1)])
    by_tile = swap_rows(jnp.sum(bs_recv[...].astype(F32), axis=0))
    for k in range(S):
        bb_send[k] = by_tile[k : k + 1]
    for d in range(1, S):
        send(bb_send.at[col_at(d)], bb_recv.at[col], "bb", to_col(d))
    bb_recv[col] = bb_send[col]
    spread_raw(1)
    spread_raw(2)
    arrive("wh", ws_half)
    ws_sum[...] = (ws_send[core].astype(F32) + ws_half[...].astype(F32)).astype(BF16)
    arrive("wf", w_rem.at[pl.ds(0, 8)])
    project(0)
    arrive("bb", bb_recv.at[pl.ds(0, S - 1)])
    grad_bias = jnp.concatenate([bb_recv[k] for k in range(S)], axis=0).astype(BF16)
    ar_one[...] = dot(grad_bias, bias_in_scr[...]).astype(BF16)
    for k in range(1, 32):
        send(ar_one, ar_all.at[row * 4 + ex], "a1", to_plane(k))
    ar_all[row * 4 + ex] = ar_one[...]
    grad_in = dot_tn(grad_bias, bw_pad[:S, :])
    pair_grad[...] = norm_back(grad_in, upd_scr[...], bias_gain[...])
    stores[1].start()
    for k in range(1, 8):
        send(ws_sum.at[(quad + k) % 8], ws_recv.at[quad], "ws", to_quad(k))
    ws_recv[quad] = ws_sum[quad]
    project(1)
    project(2)
    arrive("a1", ar_all.at[pl.ds(0, 31)])
    ar_two[...] = jnp.sum(ar_all[...].astype(F32), axis=0).astype(BF16)
    for k in range(1, 8):
        send(ar_two, ar_fin.at[group * 4 + zed], "a2", to_depth(k))
    ar_fin[group * 4 + zed] = ar_two[...]
    finish(0)
    finish(1)
    finish(2)
    stores[3].start()
    stores[4].start()
    arrive("ws", ws_recv.at[pl.ds(0, 7)])
    weight_grad[...] = jnp.sum(ws_recv[...].astype(F32), axis=0)
    stores[5].start()
    arrive("a2", ar_fin.at[pl.ds(0, 7)])
    bias_weight_grad[...] = jnp.sum(ar_fin[...].astype(F32), axis=0)
    stores[2].start()
    @pl.when(jnp.logical_not(same))
    def _():
        extra = t_recv.at[0]
        pltpu.make_async_copy(extra, extra, sems.at[0, keys["t"]]).wait()

    for key, bulk in bulks.items():
        pltpu.make_async_copy(bulk, bulk, sems.at[0, keys[key]]).wait()
    for copy in stores:
        copy.wait()


def finisher(*refs):
    sums = refs[5]
    for at in range(5):
        refs[6 + at][...] = refs[at][...]
    for g in range(4):
        refs[11][g] = sums[:, g * E : (g + 1) * E]
    refs[12][...] = pltpu.roll(sums[:, C:], C // 2, 1).T[:E]


def shards(
    pair_repr, pair_mask, chain_id, tri_in_gain, tri_proj, tri_gate, tri_out_gain, tri_out,
    bias_gain, bias_weight, chain_bias, tokens, noise_level, attn_gain, attn_weight, out_weight,
    cotangent,
):
    vmem = pl.BlockSpec(memory_space=pltpu.VMEM)
    hbm = pl.BlockSpec(memory_space=pltpu.HBM)

    def buf(*shape, kind=BF16):
        return pltpu.VMEM(shape, kind)

    outs = pl.pallas_call(
        kernel,
        out_shape=(
            jax.ShapeDtypeStruct((N, C), BF16),
            jax.ShapeDtypeStruct((N, C), F32),
            jax.ShapeDtypeStruct((S, C), F32),
            jax.ShapeDtypeStruct((T, S, D), BF16),
            jax.ShapeDtypeStruct((T, S, D), BF16),
            jax.ShapeDtypeStruct((E, N), F32),
        ),
        in_specs=[hbm] * 17,
        out_specs=(hbm,) * 6,
        scratch_shapes=[
            buf(S, S, C), buf(S, S, kind=jnp.int32), buf(1, N, kind=jnp.int32),
            buf(1, C, kind=F32), buf(C, 4 * C), buf(C, C), buf(1, C, kind=F32), buf(C, C),
            buf(1, C, kind=F32), buf(S, C), buf(1, S, kind=F32), buf(T, N, D),
            pltpu.SMEM((T,), jnp.int32), buf(D, kind=F32), buf(4, E, D), buf(E, D), buf(T, N, D),
            pltpu.SemaphoreType.DMA((17,)),
            buf(N, C, kind=F32),
            buf(S, S, C), buf(S, S, C), buf(S, S, C), buf(S, S, C),
            buf(8, S, S, C),
            buf(2, C, N),
            buf(2, 8, S, C), buf(S, S, C),
            buf(N, C, kind=F32), buf(N, C, kind=F32),
            buf(N, C), buf(C, C),
            buf(S, 1, N, kind=F32), buf(S, 1, N, kind=F32), buf(S, S, N),
            buf(4 * C, D), buf(C, D), buf(5 * C, N),
            buf(S, S, D), buf(S, 3, S, D),
            buf(T, N, D), buf(T, 3, N, C),
            buf(T, N, C, kind=F32), buf(T, N, C, kind=F32), buf(T, N, C),
            buf(T, N, N, kind=F32), buf(T, N, N, kind=F32),
            buf(T, 4, 64, N), buf(T, 3, 64, N),
            buf(T, 4, 2, S, D), buf(T, 3, 2, S, D),
            buf(S, S, N), buf(S, S, N),
            buf(S, 1, N, kind=F32), buf(S, 1, N, kind=F32),
            buf(2, 8, E, N), buf(8, E, N), buf(8, E, N), buf(8, E, N),
            buf(S, C), buf(32, S, C), buf(S, C), buf(8, S, C),
            pltpu.SemaphoreType.DMA((2, 35)),
            buf(N, C), buf(N, C, kind=F32), buf(S, C, kind=F32), buf(T, S, D), buf(T, S, D),
            buf(E, N, kind=F32), pltpu.SemaphoreType.DMA((6,)),
        ],
        compiler_params=pltpu.CompilerParams(
            collective_id=0, has_side_effects=True, vmem_limit_bytes=30 * 1024 * 1024
        ),
    )(*[pltpu.with_memory_space_constraint(array, pltpu.HBM) for array in (
        pair_repr, pair_mask, chain_id.reshape(1, N), tri_in_gain.reshape(1, C), tri_proj,
        tri_gate, tri_out_gain.reshape(1, C), tri_out, bias_gain.reshape(1, C), bias_weight.T,
        chain_bias.reshape(1, S), tokens, noise_level, attn_gain,
        jnp.transpose(attn_weight, (0, 2, 1)), out_weight, cotangent,
    )])
    outs = pl.pallas_call(
        finisher,
        out_shape=(
            jax.ShapeDtypeStruct((N, C), BF16),
            jax.ShapeDtypeStruct((N, C), F32),
            jax.ShapeDtypeStruct((S, C), F32),
            jax.ShapeDtypeStruct((T, S, D), BF16),
            jax.ShapeDtypeStruct((T, S, D), BF16),
            jax.ShapeDtypeStruct((4, E, E), F32),
            jax.ShapeDtypeStruct((E, E), F32),
        ),
        in_specs=[vmem] * 6,
        out_specs=(vmem,) * 7,
        compiler_params=pltpu.CompilerParams(vmem_limit_bytes=4 * 1024 * 1024),
    )(*outs)
    pair_next, pair_grad, bias_weight_grad, denoised, token_grad, weight_grad, out_grad = outs
    return (
        pair_next.reshape(S, S, C),
        pair_grad.reshape(S, S, C),
        bias_weight_grad.T,
        denoised,
        token_grad,
        weight_grad,
        out_grad,
    )


def solution(mesh):
    line, col = ("group", "row"), "col"
    return jax.shard_map(
        shards,
        mesh=mesh,
        in_specs=(
            P(line, col, None), P(line, col), P(), P(), P(), P(), P(), P(), P(), P(), P(),
            P(line, None, None), P(line), P(), P(None, None, col), P(col, None),
            P(line, None, None),
        ),
        out_specs=(
            P(line, col, None), P(line, col, None), P(), P(line, col, None),
            P(line, col, None), P(None, line, col), P(col, line),
        ),
        check_vma=False,
    )
```

```python
import math

import jax
import jax.numpy as jnp
from jax import lax
from jax.experimental import pallas as pl
from jax.experimental.pallas import tpu as pltpu
from jax.sharding import PartitionSpec as P

MESH = pl.DeviceIdType.MESH
LEVELS = 200
EPSILON = 1e-05
SIGMA_LOW = 0.1
SIGMA_SPAN = 100.0
F32 = jnp.float32
BF16 = jnp.bfloat16
S = 16
C = 128
E = 48
D = 768
N = 256
T = 3
NT = (((1,), (1,)), ((), ()))
TN = (((0,), (0,)), ((), ()))


def iota(shape, dim):
    return lax.broadcasted_iota(jnp.int32, shape, dim)


def dot(a, b):
    return jnp.dot(a, b, preferred_element_type=F32)


def dot_nt(a, b):
    return lax.dot_general(a, b, NT, preferred_element_type=F32)


def dot_tn(a, b):
    return lax.dot_general(a, b, TN, preferred_element_type=F32)


def sigmoid(v):
    return 1.0 / (1.0 + jnp.exp(-v))


def centred_inverse(v):
    centred = v - jnp.mean(v, -1, keepdims=True)
    return centred, lax.rsqrt(jnp.mean(centred * centred, -1, keepdims=True) + EPSILON)


def norm_back(gradient, values, gain):
    centred, inverse = centred_inverse(values)
    normed = centred * inverse
    weighted = gradient * gain
    return inverse * (
        weighted
        - jnp.mean(weighted, -1, keepdims=True)
        - normed * jnp.mean(weighted * normed, -1, keepdims=True)
    )


def swap_blocks(x, unit):
    arr = iota(x.shape, 0) // S
    blk = iota(x.shape, 1) // unit
    for bit in (1, 2, 4, 8):
        rows = bit * S
        other = jnp.concatenate(
            [x[(k ^ 1) * rows : (k ^ 1) * rows + rows] for k in range(N // rows)], axis=0
        )
        up = pltpu.roll(other, bit * unit, 1)
        down = pltpu.roll(other, C - bit * unit, 1)
        in_arr, in_blk = (arr & bit) != 0, (blk & bit) != 0
        x = jnp.where(in_arr == in_blk, x, jnp.where(in_blk, up, down))
    return x


def swap_rows(x):
    arr, blk = iota(x.shape, 0), iota(x.shape, 1) // S
    for bit in (1, 2, 4, 8):
        in_arr, in_blk = (arr & bit) != 0, (blk & bit) != 0
        other = jnp.where(in_arr, pltpu.roll(x, bit, 0), pltpu.roll(x, S - bit, 0))
        up = pltpu.roll(other, bit * S, 1)
        down = pltpu.roll(other, N - bit * S, 1)
        x = jnp.where(in_arr == in_blk, x, jnp.where(in_blk, up, down))
    return x


def kernel(
    *refs,
):
    (
        pair, mask, chain, tri_in_gain, tri_proj, tri_gate, tri_out_gain, tri_out, bias_gain,
        bias_weight, chain_bias, tokens, level, attn_gain, attn_weight, out_weight, cot,
    ) = refs[23:40]
    results, sem_out = refs[-7:-1], refs[-1]
    pair_next, pair_grad, bias_weight_grad, denoised, token_grad, weight_grad = results
    work(
        refs[:17], refs[23:40], refs[40], refs[17:23], results, sem_out,
        pair, mask, chain, tri_in_gain, tri_proj, tri_gate, tri_out_gain, tri_out, bias_gain,
        bias_weight, chain_bias, tokens, level, attn_gain, attn_weight, out_weight, cot,
        pair_next, pair_grad, bias_weight_grad, denoised, token_grad, weight_grad, *refs[41:-7],
    )


def work(
    stored, loaded, sem_in, given, results, sem_out,
    pair, mask, chain, tri_in_gain, tri_proj, tri_gate, tri_out_gain, tri_out, bias_gain,
    bias_weight, chain_bias, tokens, level, attn_gain, attn_weight, out_weight, cot,
    pair_next, pair_grad, bias_weight_grad, denoised, token_grad, weight_grad,
    gate_scr, r_send, l_send, r_own, l_own, r_all, left_t, t_send, t_recv, row_scr, upd_scr,
    bias_in_scr, bw_pad, b_send, b_recv, b_all, w_four, ow_pad, place, w_own, w_rem, hid_scr, qkv_scr,
    sig_scr, slope_scr, ga_scr, score_scr, prob_scr, raw, raw_z, part, part_x, bs_send, bs_recv, bb_send, bb_recv, ws_send,
    ws_half, ws_sum, ws_recv, ar_one, ar_all, ar_two, ar_fin,
    sems,
):
    group, row, col = lax.axis_index("group"), lax.axis_index("row"), lax.axis_index("col")
    mine = group * 8 + row
    core, high = row % 2, row // 2
    quad = group * 4 + high
    zed, ex = col // 4, col % 4
    keys, bulks = {}, {}

    def send(src, dst, key, device):
        at = keys.setdefault(key, len(keys))
        pltpu.make_async_remote_copy(
            src_ref=src, dst_ref=dst, send_sem=sems.at[0, at], recv_sem=sems.at[1, at],
            device_id=device, device_id_type=MESH,
        ).start()

    def arrive(key, bulk):
        bulks[key] = bulk
        pltpu.make_async_copy(bulk, bulk, sems.at[1, keys[key]]).wait()

    def col_at(step):
        return (zed + step // 4) % 4 * 4 + (ex + step % 4) % 4

    def to_col(step):
        return {"col": col_at(step)}

    def to_line(step):
        there = (mine + step) % S
        return {"group": there // 8, "row": there % 8}

    stores = [
        pltpu.make_async_copy(src, dst, sem_out.at[k])
        for k, (src, dst) in enumerate(zip(results, given, strict=True))
    ]
    def to_plane(step):
        return {"row": (row + step % 8) % 8, "col": zed * 4 + (ex + step // 8) % 4}

    def to_depth(step):
        return {"group": (group + step) % 2, "col": (zed + step // 2) % 4 * 4 + ex}

    barrier = pltpu.get_barrier_semaphore()
    for step in range(1, S):
        pl.semaphore_signal(barrier, inc=1, device_id=to_col(step), device_id_type=MESH)
        pl.semaphore_signal(barrier, inc=1, device_id=to_line(step), device_id_type=MESH)
    greeted = 2 * (S - 1)
    others = [to_plane(k) for k in range(9, 32) if k % 8]
    others += [to_depth(k) for k in (3, 5, 7)]
    others += [{"row": high * 2 + 1 - core, "col": col_at(d)} for d in range(4, S)]
    for there in others:
        pl.semaphore_signal(barrier, inc=1, device_id=there, device_id_type=MESH)
    greeted += len(others)

    loads = [
        pltpu.make_async_copy(src, dst, sem_in.at[k])
        for k, (src, dst) in enumerate(zip(stored, loaded, strict=True))
    ]
    first, second = (0, 1, 3, 4, 5), (14, 15, 9, 11, 12, 13, 16, 2, 6, 7, 8, 10)
    for k in first + second:
        loads[k].start()
    for k in first:
        loads[k].wait()
    tile = pair[...].astype(F32).reshape(N, C)
    centred, inverse = centred_inverse(tile)
    pair_in = (centred * inverse * tri_in_gain[...]).astype(BF16)
    pick = (iota((N, S), 0) // S == iota((N, S), 1)).astype(BF16)
    spread = dot(pick, mask[...].astype(F32).astype(BF16))
    mask_col = jnp.sum(
        jnp.where(iota((N, S), 0) % S == iota((N, S), 1), spread, 0.0), -1, keepdims=True
    )
    right = dot(pair_in, tri_proj[:, 2 * C : 4 * C])
    right = sigmoid(right[:, :C]) * right[:, C:] * mask_col
    r_send[...] = swap_blocks(right, 8).astype(BF16).reshape(S, S, C)
    pl.semaphore_wait(barrier, greeted)
    for d in range(1, S):
        send(r_send.at[col_at(d)], r_own.at[col], ("r", d // 4), to_col(d))
    r_own[col] = r_send[col]
    left = dot(pair_in, tri_proj[:, : 2 * C])
    left = sigmoid(left[:, :C]) * left[:, C:] * mask_col
    l_send[...] = swap_blocks(left, 8).astype(BF16).reshape(S, S, C)
    for d in range(1, S):
        send(l_send.at[col_at(d)], l_own.at[col], "l", to_col(d))
    l_own[col] = l_send[col]
    gate_scr[...] = sigmoid(dot(pair_in, tri_gate[...]))

    for k in second:
        loads[k].wait()
    for g in range(4):
        w_own[3 * g : 3 * g + 3] = attn_weight[g].reshape(3, S, D)
    w_own[12:15] = out_weight[...].reshape(3, S, D)
    w_own[15] = jnp.zeros((S, D), BF16)
    w_four[...] = jnp.zeros_like(w_four)
    for g in range(4):
        w_four[g * C : g * C + E, :] = attn_weight[g]
    ow_pad[...] = jnp.zeros_like(ow_pad)
    ow_pad[:E, :] = out_weight[...]
    bw_pad[...] = jnp.zeros_like(bw_pad)
    bw_pad[:S, :] = bias_weight[...]
    place_row = iota((5 * C, N), 0)
    inner = place_row % C
    place[...] = jnp.where(
        (inner < E) & (iota((5 * C, N), 1) == place_row // C * E + inner), 1.0, 0.0
    ).astype(BF16)

    scale_of = []
    for t in range(T):
        power = jnp.full((1, C), level[t].astype(F32)) * (math.log(SIGMA_SPAN) / (LEVELS - 1))
        sigma = SIGMA_LOW * jnp.exp(power)
        scale_of.append(lax.rsqrt(1.0 + sigma * sigma)[:, :1])
    inverse_root = 1.0 / math.sqrt(E)

    def before_bias(t):
        scaled = tokens[t].astype(F32) * scale_of[t]
        mid, inv = centred_inverse(scaled)
        hidden = (mid * inv * attn_gain[...].reshape(1, D)).astype(BF16)
        hid_scr[t] = hidden
        projections = dot_nt(hidden, w_four[...])
        for g in range(3):
            qkv_scr[t, g] = projections[:, g * C : (g + 1) * C].astype(BF16)
        gate_sig = sigmoid(projections[:, 3 * C :])
        grad_gated = dot_nt(cot[t], ow_pad[...])
        grad_attended = (grad_gated * gate_sig).astype(BF16)
        sig_scr[t] = gate_sig
        slope_scr[t] = grad_gated * gate_sig * (1.0 - gate_sig)
        ga_scr[t] = grad_attended
        score_scr[t] = dot_nt(qkv_scr[t, 0], qkv_scr[t, 1]) * inverse_root
        prob_scr[t] = dot_nt(grad_attended, qkv_scr[t, 2])

    before_bias(0)

    partner = {"row": high * 2 + 1 - core}

    def to_quad(k):
        return {"group": (quad + k) % 8 // 4, "row": (quad + k) % 4 * 2 + core}

    def from_quad(k, side):
        there = (quad + 8 - k) % 8
        return there // 4 * 8 + there % 4 * 2 + side

    def z_block(dz):
        return pl.ds((zed + 4 - dz) % 4 * 4, 4)

    def ag_key(dz, k):
        return ("ag", dz, k) if dz == 2 else ("ag", dz)

    def spread_right(dz):
        arrive(("r", dz), r_own.at[pl.ds(0, 4 if dz else 3)])
        for k in range(1, 8):
            send(r_own.at[z_block(dz)], r_all.at[quad, z_block(dz)], ag_key(dz, k), to_quad(k))

    spread_right(0)
    spread_right(1)
    spread_right(3)
    spread_right(2)
    before_bias(1)
    arrive("l", l_own.at[pl.ds(0, S - 1)])
    for d in range(1, 4):
        send(w_own.at[mine], w_rem.at[mine, d - 1], "w", {"col": (zed + 4 - d) % 4 * 4 + ex})
    left_t[core] = l_own[...].reshape(N, C).astype(F32).T.astype(BF16)
    send(left_t.at[core], left_t.at[core], "lt", partner)
    diagonal = iota((2 * C, C), 0) % 8 == iota((2 * C, C), 1) % 8

    def triangle(at, block):
        product = dot(left_t[...].reshape(2 * C, N), block.reshape(N, C))
        product = jnp.where(diagonal, product, 0.0).reshape(2 * S, 8, C)
        product = jnp.sum(product, axis=1).astype(BF16)
        t_send[0, at] = product[:S]
        t_send[1, at] = product[S:]

    before_bias(2)
    arrive("lt", left_t.at[0])
    triangle(quad, r_own[...])
    for dz in (0, 1, 3):
        arrive(("ag", dz), r_all.at[pl.ds(0, 7), pl.ds(0, 4)])
    for k in range(1, 8):
        arrive(("ag", 2, k), r_all.at[0, pl.ds(0, 4)])
        at = (quad + 8 - k) % 8
        triangle(at, r_all[at])
    same = col % 2 == core
    for m in range(8):
        at = (col // 2 + m) % 8
        there = 2 * at + core
        if m:
            send(t_send.at[core, at], t_recv.at[col], "t", {"col": there})
        send(
            t_send.at[1 - core, at], t_recv.at[col], "t",
            {"row": high * 2 + 1 - core, "col": there},
        )
    near = col // 2

    @pl.when(same)
    def _():
        pltpu.make_async_copy(
            t_send.at[core, near], t_recv.at[col], sems.at[1, keys["t"]]
        ).start()

    @pl.when(jnp.logical_not(same))
    def _():
        send(t_send.at[core, near], t_recv.at[col], "t", {"col": 2 * near + core})

    def to_high(k):
        return {"row": (high + k) % 4 * 2 + core}

    arrive("w", w_rem.at[0])
    send(w_rem.at[mine], w_rem.at[mine], "wz", {"group": 1 - group})
    for k in range(1, 4):
        send(w_rem.at[mine], w_rem.at[mine], "wy", to_high(k))
    send(w_rem.at[mine], w_rem.at[mine], "wf", partner)
    arrive("t", t_recv)
    bulks["t"] = t_recv.at[pl.ds(0, S - 1)]
    moved = swap_blocks(t_recv[...].astype(F32).reshape(N, C), 8)
    for j in range(S):
        row_scr[pl.ds(j, S, stride=S), :] = moved[j * S : (j + 1) * S]
    centred, inverse = centred_inverse(row_scr[...])
    tri_normed = (centred * inverse * tri_out_gain[...]).astype(BF16)
    tile = pair[...].astype(F32).reshape(N, C)
    updated = tile + gate_scr[...] * dot(tri_normed, tri_out[...])
    upd_scr[...] = updated
    centred, inverse = centred_inverse(updated)
    bias_in = (centred * inverse * bias_gain[...]).astype(BF16)
    bias_in_scr[...] = bias_in
    by_head = dot_nt(bw_pad[:S, :], bias_in)
    ids = chain[...].astype(F32)
    eye = iota((N, N), 0) == iota((N, N), 1)
    ids_col = jnp.sum(jnp.where(eye, ids, 0.0), -1, keepdims=True)
    lane = iota((N, N), 1)
    row_of = mine * S + lane // S == iota((N, N), 0)
    row_chain = jnp.sum(jnp.where(row_of, ids_col, 0.0), 0, keepdims=True)
    col_of = col * S + lane % S == iota((N, N), 0)
    col_chain = jnp.sum(jnp.where(col_of, ids_col, 0.0), 0, keepdims=True)
    head_bias = jnp.sum(
        jnp.where(iota((S, S), 1) == iota((S, S), 0), chain_bias[...], 0.0), -1, keepdims=True
    )
    by_head = by_head + jnp.where(row_chain == col_chain, head_bias, 0.0)
    for k in range(S):
        b_send[k] = by_head[k : k + 1]
    for d in range(1, S):
        send(b_send.at[col_at(d)], b_recv.at[col], "b", to_col(d))
    arrive("wz", w_rem.at[0])
    beside = (1 - group) * 8 + row
    for k in range(1, 4):
        send(w_rem.at[beside], w_rem.at[beside], "wyz", to_high(k))
    b_recv[col] = b_send[col]
    pair_next[...] = updated.astype(BF16)
    stores[0].start()
    arrive("b", b_recv.at[pl.ds(0, S - 1)])
    by_row = swap_rows(jnp.concatenate([b_recv[k] for k in range(S)], axis=0))
    b_all[mine] = by_row.astype(BF16)
    for d in range(1, S):
        send(b_all.at[mine], b_all.at[mine], "ba", to_line(d))
    arrive("ba", b_all.at[pl.ds(0, S - 1)])

    bias = b_all[...].reshape(N, N).astype(F32)
    copies = range(T)
    exponent = [jnp.exp(score_scr[t] + bias) for t in copies]
    attention = [e / jnp.sum(e, -1, keepdims=True) for e in exponent]
    attention_b = [a.astype(BF16) for a in attention]
    grad_score = [
        a * (prob_scr[t] - jnp.sum(a * prob_scr[t], -1, keepdims=True))
        for t, a in enumerate(attention)
    ]
    bs_send[...] = sum(grad_score[1:], grad_score[0]).astype(BF16).reshape(S, S, N)
    for d in range(1, S):
        send(bs_send.at[(mine + d) % S], bs_recv.at[mine], "bs", to_line(d))
    bs_recv[mine] = bs_send[mine]
    score_b = [g.astype(BF16) for g in grad_score]
    attended = [dot(attention_b[t], qkv_scr[t, 2]) for t in copies]
    grad_values = [dot_tn(attention_b[t], ga_scr[t]).astype(BF16) for t in copies]
    grad_queries = [(dot(score_b[t], qkv_scr[t, 1]) * inverse_root).astype(BF16) for t in copies]
    grad_keys = [(dot_tn(score_b[t], qkv_scr[t, 0]) * inverse_root).astype(BF16) for t in copies]
    gated = [(sig_scr[t] * attended[t]).astype(BF16) for t in copies]
    grad_gate = [(slope_scr[t] * attended[t]).astype(BF16) for t in copies]
    for t in copies:
        side = jnp.concatenate(
            [grad_queries[t], grad_keys[t], grad_values[t], grad_gate[t], gated[t]], axis=1
        )
        raw[t] = dot(side, place[...]).astype(BF16).reshape(4, 64, N)
    def spread_raw(t):
        for d in (2, 1, 3):
            there = (zed + 4 - d) % 4
            send(raw.at[t, there], raw_z.at[t, d - 1], ("z", t), {"col": there * 4 + ex})

    spread_raw(0)
    raw_t = raw[...].reshape(T * N, N).astype(F32).T.astype(BF16)
    grads_part = dot(raw_t[: 4 * E], hid_scr[...].reshape(T * N, D))
    out_part = dot(raw_t[4 * E :], cot[...].reshape(T * N, D))
    turned = jnp.concatenate([grads_part, out_part], axis=0).T
    for k in range(S):
        ws_send[k % 2, k // 2] = turned[k * E : (k + 1) * E].astype(BF16)
    send(ws_send.at[1 - core], ws_half, "wh", partner)
    arrive("wy", w_rem.at[pl.ds(0, 3)])
    arrive("wyz", w_rem.at[pl.ds(0, 3)])
    for k in range(1, 8):
        at = from_quad(k, core)
        send(w_rem.at[at], w_rem.at[at], "wf", partner)
    def project(t):
        arrive(("z", t), raw_z.at[t])
        total = jnp.zeros((C, D), F32)
        first = iota((64, N), 1) < 4 * E
        for d in range(4):
            piece = (raw_z[t, d - 1] if d else raw[t, zed]).astype(F32)
            weights = w_rem[:, d - 1] if d else w_own[...]
            both = jnp.concatenate(
                [jnp.where(first, piece, 0.0), jnp.where(first, 0.0, piece)], axis=0
            ).astype(BF16)
            total = total + dot(both, weights.reshape(N, D))
        total = total.astype(BF16)
        for x in range(4):
            part[t, x, 0] = total[x * S : (x + 1) * S]
            part[t, x, 1] = total[64 + x * S : 64 + (x + 1) * S]
        for d in range(1, 4):
            there = (ex + d) % 4
            send(part.at[t, there], part_x.at[t, d - 1], ("x", t), {"col": zed * 4 + there})

    def finish(t):
        arrive(("x", t), part_x.at[t])
        sums = part[t, ex].astype(F32)
        for d in range(3):
            sums = sums + part_x[t, d].astype(F32)
        first = pl.multiple_of(col * S, S)
        scaled = tokens[t, pl.ds(first, S), :].astype(F32) * scale_of[t]
        cot_mine = cot[t, pl.ds(first, S), :].astype(F32)
        denoised[t] = (scaled + sums[1]).astype(BF16)
        back = norm_back(sums[0], scaled, attn_gain[...].reshape(1, D))
        token_grad[t] = (scale_of[t] * (cot_mine + back)).astype(BF16)

    arrive("bs", bs_recv.at[pl.ds(0, S - 1)])
    by_tile = swap_rows(jnp.sum(bs_recv[...].astype(F32), axis=0))
    for k in range(S):
        bb_send[k] = by_tile[k : k + 1]
    for d in range(1, S):
        send(bb_send.at[col_at(d)], bb_recv.at[col], "bb", to_col(d))
    bb_recv[col] = bb_send[col]
    spread_raw(1)
    spread_raw(2)
    arrive("wh", ws_half)
    ws_sum[...] = (ws_send[core].astype(F32) + ws_half[...].astype(F32)).astype(BF16)
    arrive("wf", w_rem.at[pl.ds(0, 8)])
    project(0)
    arrive("bb", bb_recv.at[pl.ds(0, S - 1)])
    grad_bias = jnp.concatenate([bb_recv[k] for k in range(S)], axis=0).astype(BF16)
    ar_one[...] = dot(grad_bias, bias_in_scr[...]).astype(BF16)
    for k in range(1, 32):
        send(ar_one, ar_all.at[row * 4 + ex], "a1", to_plane(k))
    ar_all[row * 4 + ex] = ar_one[...]
    grad_in = dot_tn(grad_bias, bw_pad[:S, :])
    pair_grad[...] = norm_back(grad_in, upd_scr[...], bias_gain[...])
    stores[1].start()
    for k in range(1, 8):
        send(ws_sum.at[(quad + k) % 8], ws_recv.at[quad], "ws", to_quad(k))
    ws_recv[quad] = ws_sum[quad]
    project(1)
    project(2)
    arrive("a1", ar_all.at[pl.ds(0, 31)])
    ar_two[...] = jnp.sum(ar_all[...].astype(F32), axis=0).astype(BF16)
    for k in range(1, 8):
        send(ar_two, ar_fin.at[group * 4 + zed], "a2", to_depth(k))
    ar_fin[group * 4 + zed] = ar_two[...]
    finish(0)
    finish(1)
    finish(2)
    stores[3].start()
    stores[4].start()
    arrive("ws", ws_recv.at[pl.ds(0, 7)])
    weight_grad[...] = jnp.sum(ws_recv[...].astype(F32), axis=0)
    stores[5].start()
    arrive("a2", ar_fin.at[pl.ds(0, 7)])
    bias_weight_grad[...] = jnp.sum(ar_fin[...].astype(F32), axis=0)
    stores[2].start()
    @pl.when(jnp.logical_not(same))
    def _():
        extra = t_recv.at[0]
        pltpu.make_async_copy(extra, extra, sems.at[0, keys["t"]]).wait()

    for key, bulk in bulks.items():
        pltpu.make_async_copy(bulk, bulk, sems.at[0, keys[key]]).wait()
    for copy in stores:
        copy.wait()


def finisher(*refs):
    sums = refs[5]
    for at in range(5):
        refs[6 + at][...] = refs[at][...]
    for g in range(4):
        refs[11][g] = sums[:, g * E : (g + 1) * E]
    refs[12][...] = pltpu.roll(sums[:, C:], C // 2, 1).T[:E]


def shards(
    pair_repr, pair_mask, chain_id, tri_in_gain, tri_proj, tri_gate, tri_out_gain, tri_out,
    bias_gain, bias_weight, chain_bias, tokens, noise_level, attn_gain, attn_weight, out_weight,
    cotangent,
):
    vmem = pl.BlockSpec(memory_space=pltpu.VMEM)
    hbm = pl.BlockSpec(memory_space=pltpu.HBM)

    def buf(*shape, kind=BF16):
        return pltpu.VMEM(shape, kind)

    outs = pl.pallas_call(
        kernel,
        out_shape=(
            jax.ShapeDtypeStruct((N, C), BF16),
            jax.ShapeDtypeStruct((N, C), F32),
            jax.ShapeDtypeStruct((S, C), F32),
            jax.ShapeDtypeStruct((T, S, D), BF16),
            jax.ShapeDtypeStruct((T, S, D), BF16),
            jax.ShapeDtypeStruct((E, N), F32),
        ),
        in_specs=[hbm] * 17,
        out_specs=(hbm,) * 6,
        scratch_shapes=[
            buf(S, S, C), buf(S, S, kind=jnp.int32), buf(1, N, kind=jnp.int32),
            buf(1, C, kind=F32), buf(C, 4 * C), buf(C, C), buf(1, C, kind=F32), buf(C, C),
            buf(1, C, kind=F32), buf(S, C), buf(1, S, kind=F32), buf(T, N, D),
            pltpu.SMEM((T,), jnp.int32), buf(D, kind=F32), buf(4, E, D), buf(E, D), buf(T, N, D),
            pltpu.SemaphoreType.DMA((17,)),
            buf(N, C, kind=F32),
            buf(S, S, C), buf(S, S, C), buf(S, S, C), buf(S, S, C),
            buf(8, S, S, C),
            buf(2, C, N),
            buf(2, 8, S, C), buf(S, S, C),
            buf(N, C, kind=F32), buf(N, C, kind=F32),
            buf(N, C), buf(C, C),
            buf(S, 1, N, kind=F32), buf(S, 1, N, kind=F32), buf(S, S, N),
            buf(4 * C, D), buf(C, D), buf(5 * C, N),
            buf(S, S, D), buf(S, 3, S, D),
            buf(T, N, D), buf(T, 3, N, C),
            buf(T, N, C, kind=F32), buf(T, N, C, kind=F32), buf(T, N, C),
            buf(T, N, N, kind=F32), buf(T, N, N, kind=F32),
            buf(T, 4, 64, N), buf(T, 3, 64, N),
            buf(T, 4, 2, S, D), buf(T, 3, 2, S, D),
            buf(S, S, N), buf(S, S, N),
            buf(S, 1, N, kind=F32), buf(S, 1, N, kind=F32),
            buf(2, 8, E, N), buf(8, E, N), buf(8, E, N), buf(8, E, N),
            buf(S, C), buf(32, S, C), buf(S, C), buf(8, S, C),
            pltpu.SemaphoreType.DMA((2, 37)),
            buf(N, C), buf(N, C, kind=F32), buf(S, C, kind=F32), buf(T, S, D), buf(T, S, D),
            buf(E, N, kind=F32), pltpu.SemaphoreType.DMA((6,)),
        ],
        compiler_params=pltpu.CompilerParams(
            collective_id=0, has_side_effects=True, vmem_limit_bytes=30 * 1024 * 1024
        ),
    )(*[pltpu.with_memory_space_constraint(array, pltpu.HBM) for array in (
        pair_repr, pair_mask, chain_id.reshape(1, N), tri_in_gain.reshape(1, C), tri_proj,
        tri_gate, tri_out_gain.reshape(1, C), tri_out, bias_gain.reshape(1, C), bias_weight.T,
        chain_bias.reshape(1, S), tokens, noise_level, attn_gain,
        jnp.transpose(attn_weight, (0, 2, 1)), out_weight, cotangent,
    )])
    outs = pl.pallas_call(
        finisher,
        out_shape=(
            jax.ShapeDtypeStruct((N, C), BF16),
            jax.ShapeDtypeStruct((N, C), F32),
            jax.ShapeDtypeStruct((S, C), F32),
            jax.ShapeDtypeStruct((T, S, D), BF16),
            jax.ShapeDtypeStruct((T, S, D), BF16),
            jax.ShapeDtypeStruct((4, E, E), F32),
            jax.ShapeDtypeStruct((E, E), F32),
        ),
        in_specs=[vmem] * 6,
        out_specs=(vmem,) * 7,
        compiler_params=pltpu.CompilerParams(vmem_limit_bytes=4 * 1024 * 1024),
    )(*outs)
    pair_next, pair_grad, bias_weight_grad, denoised, token_grad, weight_grad, out_grad = outs
    return (
        pair_next.reshape(S, S, C),
        pair_grad.reshape(S, S, C),
        bias_weight_grad.T,
        denoised,
        token_grad,
        weight_grad,
        out_grad,
    )


def solution(mesh):
    line, col = ("group", "row"), "col"
    return jax.shard_map(
        shards,
        mesh=mesh,
        in_specs=(
            P(line, col, None), P(line, col), P(), P(), P(), P(), P(), P(), P(), P(), P(),
            P(line, None, None), P(line), P(), P(None, None, col), P(col, None),
            P(line, None, None),
        ),
        out_specs=(
            P(line, col, None), P(line, col, None), P(), P(line, col, None),
            P(line, col, None), P(None, line, col), P(col, line),
        ),
        check_vma=False,
    )
```

```python
import math

import jax
import jax.numpy as jnp
from jax import lax
from jax.experimental import pallas as pl
from jax.experimental.pallas import tpu as pltpu
from jax.sharding import PartitionSpec as P

MESH = pl.DeviceIdType.MESH
LEVELS = 200
EPSILON = 1e-05
SIGMA_LOW = 0.1
SIGMA_SPAN = 100.0
F32 = jnp.float32
BF16 = jnp.bfloat16
S = 16
C = 128
E = 48
D = 768
N = 256
T = 3
NT = (((1,), (1,)), ((), ()))
TN = (((0,), (0,)), ((), ()))


def iota(shape, dim):
    return lax.broadcasted_iota(jnp.int32, shape, dim)


def dot(a, b):
    return jnp.dot(a, b, preferred_element_type=F32)


def dot_nt(a, b):
    return lax.dot_general(a, b, NT, preferred_element_type=F32)


def dot_tn(a, b):
    return lax.dot_general(a, b, TN, preferred_element_type=F32)


def sigmoid(v):
    return 1.0 / (1.0 + jnp.exp(-v))


def centred_inverse(v):
    centred = v - jnp.mean(v, -1, keepdims=True)
    return centred, lax.rsqrt(jnp.mean(centred * centred, -1, keepdims=True) + EPSILON)


def norm_back(gradient, values, gain):
    centred, inverse = centred_inverse(values)
    normed = centred * inverse
    weighted = gradient * gain
    return inverse * (
        weighted
        - jnp.mean(weighted, -1, keepdims=True)
        - normed * jnp.mean(weighted * normed, -1, keepdims=True)
    )


def swap_blocks(x, unit):
    arr = iota(x.shape, 0) // S
    blk = iota(x.shape, 1) // unit
    for bit in (1, 2, 4, 8):
        rows = bit * S
        other = jnp.concatenate(
            [x[(k ^ 1) * rows : (k ^ 1) * rows + rows] for k in range(N // rows)], axis=0
        )
        up = pltpu.roll(other, bit * unit, 1)
        down = pltpu.roll(other, C - bit * unit, 1)
        in_arr, in_blk = (arr & bit) != 0, (blk & bit) != 0
        x = jnp.where(in_arr == in_blk, x, jnp.where(in_blk, up, down))
    return x


def swap_rows(x):
    arr, blk = iota(x.shape, 0), iota(x.shape, 1) // S
    for bit in (1, 2, 4, 8):
        in_arr, in_blk = (arr & bit) != 0, (blk & bit) != 0
        other = jnp.where(in_arr, pltpu.roll(x, bit, 0), pltpu.roll(x, S - bit, 0))
        up = pltpu.roll(other, bit * S, 1)
        down = pltpu.roll(other, N - bit * S, 1)
        x = jnp.where(in_arr == in_blk, x, jnp.where(in_blk, up, down))
    return x


def kernel(
    *refs,
):
    (
        pair, mask, chain, tri_in_gain, tri_proj, tri_gate, tri_out_gain, tri_out, bias_gain,
        bias_weight, chain_bias, tokens, level, attn_gain, attn_weight, out_weight, cot,
    ) = refs[23:40]
    results, sem_out = refs[-7:-1], refs[-1]
    pair_next, pair_grad, bias_weight_grad, denoised, token_grad, weight_grad = results
    work(
        refs[:17], refs[23:40], refs[40], refs[17:23], results, sem_out,
        pair, mask, chain, tri_in_gain, tri_proj, tri_gate, tri_out_gain, tri_out, bias_gain,
        bias_weight, chain_bias, tokens, level, attn_gain, attn_weight, out_weight, cot,
        pair_next, pair_grad, bias_weight_grad, denoised, token_grad, weight_grad, *refs[41:-7],
    )


def work(
    stored, loaded, sem_in, given, results, sem_out,
    pair, mask, chain, tri_in_gain, tri_proj, tri_gate, tri_out_gain, tri_out, bias_gain,
    bias_weight, chain_bias, tokens, level, attn_gain, attn_weight, out_weight, cot,
    pair_next, pair_grad, bias_weight_grad, denoised, token_grad, weight_grad,
    gate_scr, r_send, l_send, r_own, l_own, r_all, left_t, t_send, t_recv, row_scr, upd_scr,
    bias_in_scr, bw_pad, b_send, b_recv, b_all, w_four, ow_pad, place, w_own, w_rem, hid_scr, qkv_scr,
    sig_scr, slope_scr, ga_scr, score_scr, prob_scr, raw, raw_z, part, part_x, bs_send, bs_recv, bb_send, bb_recv, ws_send,
    ws_half, ws_sum, ws_recv, ar_one, ar_all, ar_two, ar_fin,
    sems,
):
    group, row, col = lax.axis_index("group"), lax.axis_index("row"), lax.axis_index("col")
    mine = group * 8 + row
    core, high = row % 2, row // 2
    quad = group * 4 + high
    zed, ex = col // 4, col % 4
    keys, bulks = {}, {}

    def send(src, dst, key, device):
        at = keys.setdefault(key, len(keys))
        pltpu.make_async_remote_copy(
            src_ref=src, dst_ref=dst, send_sem=sems.at[0, at], recv_sem=sems.at[1, at],
            device_id=device, device_id_type=MESH,
        ).start()

    def arrive(key, bulk):
        bulks[key] = bulk
        pltpu.make_async_copy(bulk, bulk, sems.at[1, keys[key]]).wait()

    def col_at(step):
        return (zed + step // 4) % 4 * 4 + (ex + step % 4) % 4

    def to_col(step):
        return {"col": col_at(step)}

    def to_line(step):
        there = (mine + step) % S
        return {"group": there // 8, "row": there % 8}

    stores = [
        pltpu.make_async_copy(src, dst, sem_out.at[k])
        for k, (src, dst) in enumerate(zip(results, given, strict=True))
    ]
    def to_plane(step):
        return {"row": (row + step % 8) % 8, "col": zed * 4 + (ex + step // 8) % 4}

    def to_depth(step):
        return {"group": (group + step) % 2, "col": (zed + step // 2) % 4 * 4 + ex}

    barrier = pltpu.get_barrier_semaphore()
    for step in range(1, S):
        pl.semaphore_signal(barrier, inc=1, device_id=to_col(step), device_id_type=MESH)
        pl.semaphore_signal(barrier, inc=1, device_id=to_line(step), device_id_type=MESH)
    greeted = 2 * (S - 1)
    others = [to_plane(k) for k in range(9, 32) if k % 8]
    others += [to_depth(k) for k in (3, 5, 7)]
    others += [{"row": high * 2 + 1 - core, "col": col_at(d)} for d in range(4, S)]
    for there in others:
        pl.semaphore_signal(barrier, inc=1, device_id=there, device_id_type=MESH)
    greeted += len(others)

    loads = [
        pltpu.make_async_copy(src, dst, sem_in.at[k])
        for k, (src, dst) in enumerate(zip(stored, loaded, strict=True))
    ]
    first, second = (0, 1, 3, 4, 5), (14, 15, 9, 11, 12, 13, 16, 2, 6, 7, 8, 10)
    for k in first + second:
        loads[k].start()
    for k in first:
        loads[k].wait()
    tile = pair[...].astype(F32).reshape(N, C)
    centred, inverse = centred_inverse(tile)
    pair_in = (centred * inverse * tri_in_gain[...]).astype(BF16)
    pick = (iota((N, S), 0) // S == iota((N, S), 1)).astype(BF16)
    spread = dot(pick, mask[...].astype(F32).astype(BF16))
    mask_col = jnp.sum(
        jnp.where(iota((N, S), 0) % S == iota((N, S), 1), spread, 0.0), -1, keepdims=True
    )
    right = dot(pair_in, tri_proj[:, 2 * C : 4 * C])
    right = sigmoid(right[:, :C]) * right[:, C:] * mask_col
    r_send[...] = swap_blocks(right, 8).astype(BF16).reshape(S, S, C)
    left = dot(pair_in, tri_proj[:, : 2 * C])
    left = sigmoid(left[:, :C]) * left[:, C:] * mask_col
    l_send[...] = swap_blocks(left, 8).astype(BF16).reshape(S, S, C)
    pl.semaphore_wait(barrier, greeted)
    for d in range(1, S):
        send(r_send.at[col_at(d)], r_own.at[col], ("r", d // 4), to_col(d))
    r_own[col] = r_send[col]
    for d in range(1, S):
        send(l_send.at[col_at(d)], l_own.at[col], "l", to_col(d))
    l_own[col] = l_send[col]
    gate_scr[...] = sigmoid(dot(pair_in, tri_gate[...]))

    for k in second:
        loads[k].wait()
    for g in range(4):
        w_own[3 * g : 3 * g + 3] = attn_weight[g].reshape(3, S, D)
    w_own[12:15] = out_weight[...].reshape(3, S, D)
    w_own[15] = jnp.zeros((S, D), BF16)
    w_four[...] = jnp.zeros_like(w_four)
    for g in range(4):
        w_four[g * C : g * C + E, :] = attn_weight[g]
    ow_pad[...] = jnp.zeros_like(ow_pad)
    ow_pad[:E, :] = out_weight[...]
    bw_pad[...] = jnp.zeros_like(bw_pad)
    bw_pad[:S, :] = bias_weight[...]
    place_row = iota((5 * C, N), 0)
    inner = place_row % C
    place[...] = jnp.where(
        (inner < E) & (iota((5 * C, N), 1) == place_row // C * E + inner), 1.0, 0.0
    ).astype(BF16)

    scale_of = []
    for t in range(T):
        power = jnp.full((1, C), level[t].astype(F32)) * (math.log(SIGMA_SPAN) / (LEVELS - 1))
        sigma = SIGMA_LOW * jnp.exp(power)
        scale_of.append(lax.rsqrt(1.0 + sigma * sigma)[:, :1])
    inverse_root = 1.0 / math.sqrt(E)

    def before_bias(t):
        scaled = tokens[t].astype(F32) * scale_of[t]
        mid, inv = centred_inverse(scaled)
        hidden = (mid * inv * attn_gain[...].reshape(1, D)).astype(BF16)
        hid_scr[t] = hidden
        projections = dot_nt(hidden, w_four[...])
        for g in range(3):
            qkv_scr[t, g] = projections[:, g * C : (g + 1) * C].astype(BF16)
        gate_sig = sigmoid(projections[:, 3 * C :])
        grad_gated = dot_nt(cot[t], ow_pad[...])
        grad_attended = (grad_gated * gate_sig).astype(BF16)
        sig_scr[t] = gate_sig
        slope_scr[t] = grad_gated * gate_sig * (1.0 - gate_sig)
        ga_scr[t] = grad_attended
        score_scr[t] = dot_nt(qkv_scr[t, 0], qkv_scr[t, 1]) * inverse_root
        prob_scr[t] = dot_nt(grad_attended, qkv_scr[t, 2])

    before_bias(0)

    partner = {"row": high * 2 + 1 - core}

    def to_quad(k):
        return {"group": (quad + k) % 8 // 4, "row": (quad + k) % 4 * 2 + core}

    def from_quad(k, side):
        there = (quad + 8 - k) % 8
        return there // 4 * 8 + there % 4 * 2 + side

    def z_block(dz):
        return pl.ds((zed + 4 - dz) % 4 * 4, 4)

    def ag_key(dz, k):
        return ("ag", dz, k) if dz == 2 else ("ag", dz)

    def spread_right(dz):
        arrive(("r", dz), r_own.at[pl.ds(0, 4 if dz else 3)])
        for k in range(1, 8):
            send(r_own.at[z_block(dz)], r_all.at[quad, z_block(dz)], ag_key(dz, k), to_quad(k))

    spread_right(0)
    spread_right(1)
    spread_right(3)
    spread_right(2)
    before_bias(1)
    arrive("l", l_own.at[pl.ds(0, S - 1)])
    for d in range(1, 4):
        send(w_own.at[mine], w_rem.at[mine, d - 1], "w", {"col": (zed + 4 - d) % 4 * 4 + ex})
    left_t[core] = l_own[...].reshape(N, C).astype(F32).T.astype(BF16)
    send(left_t.at[core], left_t.at[core], "lt", partner)
    diagonal = iota((2 * C, C), 0) % 8 == iota((2 * C, C), 1) % 8

    def triangle(at, block):
        product = dot(left_t[...].reshape(2 * C, N), block.reshape(N, C))
        product = jnp.where(diagonal, product, 0.0).reshape(2 * S, 8, C)
        product = jnp.sum(product, axis=1).astype(BF16)
        t_send[0, at] = product[:S]
        t_send[1, at] = product[S:]

    before_bias(2)
    arrive("lt", left_t.at[0])
    triangle(quad, r_own[...])
    for dz in (0, 1, 3):
        arrive(("ag", dz), r_all.at[pl.ds(0, 7), pl.ds(0, 4)])
    for k in range(1, 8):
        arrive(("ag", 2, k), r_all.at[0, pl.ds(0, 4)])
        at = (quad + 8 - k) % 8
        triangle(at, r_all[at])
    same = col % 2 == core
    for m in range(8):
        at = (col // 2 + m) % 8
        there = 2 * at + core
        if m:
            send(t_send.at[core, at], t_recv.at[col], "t", {"col": there})
        send(
            t_send.at[1 - core, at], t_recv.at[col], "t",
            {"row": high * 2 + 1 - core, "col": there},
        )
    near = col // 2

    @pl.when(same)
    def _():
        pltpu.make_async_copy(
            t_send.at[core, near], t_recv.at[col], sems.at[1, keys["t"]]
        ).start()

    @pl.when(jnp.logical_not(same))
    def _():
        send(t_send.at[core, near], t_recv.at[col], "t", {"col": 2 * near + core})

    def to_high(k):
        return {"row": (high + k) % 4 * 2 + core}

    arrive("w", w_rem.at[0])
    send(w_rem.at[mine], w_rem.at[mine], "wz", {"group": 1 - group})
    for k in range(1, 4):
        send(w_rem.at[mine], w_rem.at[mine], "wy", to_high(k))
    send(w_rem.at[mine], w_rem.at[mine], "wf", partner)
    arrive("t", t_recv)
    bulks["t"] = t_recv.at[pl.ds(0, S - 1)]
    moved = swap_blocks(t_recv[...].astype(F32).reshape(N, C), 8)
    for j in range(S):
        row_scr[pl.ds(j, S, stride=S), :] = moved[j * S : (j + 1) * S]
    centred, inverse = centred_inverse(row_scr[...])
    tri_normed = (centred * inverse * tri_out_gain[...]).astype(BF16)
    tile = pair[...].astype(F32).reshape(N, C)
    updated = tile + gate_scr[...] * dot(tri_normed, tri_out[...])
    upd_scr[...] = updated
    centred, inverse = centred_inverse(updated)
    bias_in = (centred * inverse * bias_gain[...]).astype(BF16)
    bias_in_scr[...] = bias_in
    by_head = dot_nt(bw_pad[:S, :], bias_in)
    ids = chain[...].astype(F32)
    eye = iota((N, N), 0) == iota((N, N), 1)
    ids_col = jnp.sum(jnp.where(eye, ids, 0.0), -1, keepdims=True)
    lane = iota((N, N), 1)
    row_of = mine * S + lane // S == iota((N, N), 0)
    row_chain = jnp.sum(jnp.where(row_of, ids_col, 0.0), 0, keepdims=True)
    col_of = col * S + lane % S == iota((N, N), 0)
    col_chain = jnp.sum(jnp.where(col_of, ids_col, 0.0), 0, keepdims=True)
    head_bias = jnp.sum(
        jnp.where(iota((S, S), 1) == iota((S, S), 0), chain_bias[...], 0.0), -1, keepdims=True
    )
    by_head = by_head + jnp.where(row_chain == col_chain, head_bias, 0.0)
    for k in range(S):
        b_send[k] = by_head[k : k + 1]
    for d in range(1, S):
        send(b_send.at[col_at(d)], b_recv.at[col], "b", to_col(d))
    arrive("wz", w_rem.at[0])
    beside = (1 - group) * 8 + row
    for k in range(1, 4):
        send(w_rem.at[beside], w_rem.at[beside], "wyz", to_high(k))
    b_recv[col] = b_send[col]
    pair_next[...] = updated.astype(BF16)
    stores[0].start()
    arrive("b", b_recv.at[pl.ds(0, S - 1)])
    by_row = swap_rows(jnp.concatenate([b_recv[k] for k in range(S)], axis=0))
    b_all[mine] = by_row.astype(BF16)
    for d in range(1, S):
        send(b_all.at[mine], b_all.at[mine], "ba", to_line(d))
    arrive("ba", b_all.at[pl.ds(0, S - 1)])

    arrive("wy", w_rem.at[pl.ds(0, 3)])
    arrive("wyz", w_rem.at[pl.ds(0, 3)])
    for k in range(1, 8):
        at = from_quad(k, core)
        send(w_rem.at[at], w_rem.at[at], "wf", partner)
    bias = b_all[...].reshape(N, N).astype(F32)
    copies = range(T)
    exponent = [jnp.exp(score_scr[t] + bias) for t in copies]
    attention = [e / jnp.sum(e, -1, keepdims=True) for e in exponent]
    attention_b = [a.astype(BF16) for a in attention]
    grad_score = [
        a * (prob_scr[t] - jnp.sum(a * prob_scr[t], -1, keepdims=True))
        for t, a in enumerate(attention)
    ]
    bs_send[...] = sum(grad_score[1:], grad_score[0]).astype(BF16).reshape(S, S, N)
    for d in range(1, S):
        send(bs_send.at[(mine + d) % S], bs_recv.at[mine], "bs", to_line(d))
    bs_recv[mine] = bs_send[mine]
    score_b = [g.astype(BF16) for g in grad_score]
    attended = [dot(attention_b[t], qkv_scr[t, 2]) for t in copies]
    grad_values = [dot_tn(attention_b[t], ga_scr[t]).astype(BF16) for t in copies]
    grad_queries = [(dot(score_b[t], qkv_scr[t, 1]) * inverse_root).astype(BF16) for t in copies]
    grad_keys = [(dot_tn(score_b[t], qkv_scr[t, 0]) * inverse_root).astype(BF16) for t in copies]
    gated = [(sig_scr[t] * attended[t]).astype(BF16) for t in copies]
    grad_gate = [(slope_scr[t] * attended[t]).astype(BF16) for t in copies]
    for t in copies:
        side = jnp.concatenate(
            [grad_queries[t], grad_keys[t], grad_values[t], grad_gate[t], gated[t]], axis=1
        )
        raw[t] = dot(side, place[...]).astype(BF16).reshape(4, 64, N)
    def spread_raw(t):
        for d in (2, 1, 3):
            there = (zed + 4 - d) % 4
            send(raw.at[t, there], raw_z.at[t, d - 1], ("z", t), {"col": there * 4 + ex})

    spread_raw(0)
    raw_t = raw[...].reshape(T * N, N).astype(F32).T.astype(BF16)
    grads_part = dot(raw_t[: 4 * E], hid_scr[...].reshape(T * N, D))
    out_part = dot(raw_t[4 * E :], cot[...].reshape(T * N, D))
    turned = jnp.concatenate([grads_part, out_part], axis=0).T
    for k in range(S):
        ws_send[k % 2, k // 2] = turned[k * E : (k + 1) * E].astype(BF16)
    send(ws_send.at[1 - core], ws_half, "wh", partner)
    def project(t):
        arrive(("z", t), raw_z.at[t])
        total = jnp.zeros((C, D), F32)
        first = iota((64, N), 1) < 4 * E
        for d in range(4):
            piece = (raw_z[t, d - 1] if d else raw[t, zed]).astype(F32)
            weights = w_rem[:, d - 1] if d else w_own[...]
            both = jnp.concatenate(
                [jnp.where(first, piece, 0.0), jnp.where(first, 0.0, piece)], axis=0
            ).astype(BF16)
            total = total + dot(both, weights.reshape(N, D))
        total = total.astype(BF16)
        for x in range(4):
            part[t, x, 0] = total[x * S : (x + 1) * S]
            part[t, x, 1] = total[64 + x * S : 64 + (x + 1) * S]
        for d in range(1, 4):
            there = (ex + d) % 4
            send(part.at[t, there], part_x.at[t, d - 1], ("x", t), {"col": zed * 4 + there})

    def finish(t):
        arrive(("x", t), part_x.at[t])
        sums = part[t, ex].astype(F32)
        for d in range(3):
            sums = sums + part_x[t, d].astype(F32)
        first = pl.multiple_of(col * S, S)
        scaled = tokens[t, pl.ds(first, S), :].astype(F32) * scale_of[t]
        cot_mine = cot[t, pl.ds(first, S), :].astype(F32)
        denoised[t] = (scaled + sums[1]).astype(BF16)
        back = norm_back(sums[0], scaled, attn_gain[...].reshape(1, D))
        token_grad[t] = (scale_of[t] * (cot_mine + back)).astype(BF16)

    arrive("bs", bs_recv.at[pl.ds(0, S - 1)])
    by_tile = swap_rows(jnp.sum(bs_recv[...].astype(F32), axis=0))
    for k in range(S):
        bb_send[k] = by_tile[k : k + 1]
    for d in range(1, S):
        send(bb_send.at[col_at(d)], bb_recv.at[col], "bb", to_col(d))
    bb_recv[col] = bb_send[col]
    spread_raw(1)
    spread_raw(2)
    arrive("wh", ws_half)
    ws_sum[...] = (ws_send[core].astype(F32) + ws_half[...].astype(F32)).astype(BF16)
    arrive("wf", w_rem.at[pl.ds(0, 8)])
    project(0)
    arrive("bb", bb_recv.at[pl.ds(0, S - 1)])
    grad_bias = jnp.concatenate([bb_recv[k] for k in range(S)], axis=0).astype(BF16)
    ar_one[...] = dot(grad_bias, bias_in_scr[...]).astype(BF16)
    for k in range(1, 32):
        send(ar_one, ar_all.at[row * 4 + ex], "a1", to_plane(k))
    ar_all[row * 4 + ex] = ar_one[...]
    grad_in = dot_tn(grad_bias, bw_pad[:S, :])
    pair_grad[...] = norm_back(grad_in, upd_scr[...], bias_gain[...])
    stores[1].start()
    for k in range(1, 8):
        send(ws_sum.at[(quad + k) % 8], ws_recv.at[quad], "ws", to_quad(k))
    ws_recv[quad] = ws_sum[quad]
    project(1)
    project(2)
    arrive("a1", ar_all.at[pl.ds(0, 31)])
    ar_two[...] = jnp.sum(ar_all[...].astype(F32), axis=0).astype(BF16)
    for k in range(1, 8):
        send(ar_two, ar_fin.at[group * 4 + zed], "a2", to_depth(k))
    ar_fin[group * 4 + zed] = ar_two[...]
    finish(0)
    finish(1)
    finish(2)
    stores[3].start()
    stores[4].start()
    arrive("ws", ws_recv.at[pl.ds(0, 7)])
    weight_grad[...] = jnp.sum(ws_recv[...].astype(F32), axis=0)
    stores[5].start()
    arrive("a2", ar_fin.at[pl.ds(0, 7)])
    bias_weight_grad[...] = jnp.sum(ar_fin[...].astype(F32), axis=0)
    stores[2].start()
    @pl.when(jnp.logical_not(same))
    def _():
        extra = t_recv.at[0]
        pltpu.make_async_copy(extra, extra, sems.at[0, keys["t"]]).wait()

    for key, bulk in bulks.items():
        pltpu.make_async_copy(bulk, bulk, sems.at[0, keys[key]]).wait()
    for copy in stores:
        copy.wait()


def finisher(*refs):
    sums = refs[5]
    for at in range(5):
        refs[6 + at][...] = refs[at][...]
    for g in range(4):
        refs[11][g] = sums[:, g * E : (g + 1) * E]
    refs[12][...] = pltpu.roll(sums[:, C:], C // 2, 1).T[:E]


def shards(
    pair_repr, pair_mask, chain_id, tri_in_gain, tri_proj, tri_gate, tri_out_gain, tri_out,
    bias_gain, bias_weight, chain_bias, tokens, noise_level, attn_gain, attn_weight, out_weight,
    cotangent,
):
    vmem = pl.BlockSpec(memory_space=pltpu.VMEM)
    hbm = pl.BlockSpec(memory_space=pltpu.HBM)

    def buf(*shape, kind=BF16):
        return pltpu.VMEM(shape, kind)

    outs = pl.pallas_call(
        kernel,
        out_shape=(
            jax.ShapeDtypeStruct((N, C), BF16),
            jax.ShapeDtypeStruct((N, C), F32),
            jax.ShapeDtypeStruct((S, C), F32),
            jax.ShapeDtypeStruct((T, S, D), BF16),
            jax.ShapeDtypeStruct((T, S, D), BF16),
            jax.ShapeDtypeStruct((E, N), F32),
        ),
        in_specs=[hbm] * 17,
        out_specs=(hbm,) * 6,
        scratch_shapes=[
            buf(S, S, C), buf(S, S, kind=jnp.int32), buf(1, N, kind=jnp.int32),
            buf(1, C, kind=F32), buf(C, 4 * C), buf(C, C), buf(1, C, kind=F32), buf(C, C),
            buf(1, C, kind=F32), buf(S, C), buf(1, S, kind=F32), buf(T, N, D),
            pltpu.SMEM((T,), jnp.int32), buf(D, kind=F32), buf(4, E, D), buf(E, D), buf(T, N, D),
            pltpu.SemaphoreType.DMA((17,)),
            buf(N, C, kind=F32),
            buf(S, S, C), buf(S, S, C), buf(S, S, C), buf(S, S, C),
            buf(8, S, S, C),
            buf(2, C, N),
            buf(2, 8, S, C), buf(S, S, C),
            buf(N, C, kind=F32), buf(N, C, kind=F32),
            buf(N, C), buf(C, C),
            buf(S, 1, N, kind=F32), buf(S, 1, N, kind=F32), buf(S, S, N),
            buf(4 * C, D), buf(C, D), buf(5 * C, N),
            buf(S, S, D), buf(S, 3, S, D),
            buf(T, N, D), buf(T, 3, N, C),
            buf(T, N, C, kind=F32), buf(T, N, C, kind=F32), buf(T, N, C),
            buf(T, N, N, kind=F32), buf(T, N, N, kind=F32),
            buf(T, 4, 64, N), buf(T, 3, 64, N),
            buf(T, 4, 2, S, D), buf(T, 3, 2, S, D),
            buf(S, S, N), buf(S, S, N),
            buf(S, 1, N, kind=F32), buf(S, 1, N, kind=F32),
            buf(2, 8, E, N), buf(8, E, N), buf(8, E, N), buf(8, E, N),
            buf(S, C), buf(32, S, C), buf(S, C), buf(8, S, C),
            pltpu.SemaphoreType.DMA((2, 37)),
            buf(N, C), buf(N, C, kind=F32), buf(S, C, kind=F32), buf(T, S, D), buf(T, S, D),
            buf(E, N, kind=F32), pltpu.SemaphoreType.DMA((6,)),
        ],
        compiler_params=pltpu.CompilerParams(
            collective_id=0, has_side_effects=True, vmem_limit_bytes=30 * 1024 * 1024
        ),
    )(*[pltpu.with_memory_space_constraint(array, pltpu.HBM) for array in (
        pair_repr, pair_mask, chain_id.reshape(1, N), tri_in_gain.reshape(1, C), tri_proj,
        tri_gate, tri_out_gain.reshape(1, C), tri_out, bias_gain.reshape(1, C), bias_weight.T,
        chain_bias.reshape(1, S), tokens, noise_level, attn_gain,
        jnp.transpose(attn_weight, (0, 2, 1)), out_weight, cotangent,
    )])
    outs = pl.pallas_call(
        finisher,
        out_shape=(
            jax.ShapeDtypeStruct((N, C), BF16),
            jax.ShapeDtypeStruct((N, C), F32),
            jax.ShapeDtypeStruct((S, C), F32),
            jax.ShapeDtypeStruct((T, S, D), BF16),
            jax.ShapeDtypeStruct((T, S, D), BF16),
            jax.ShapeDtypeStruct((4, E, E), F32),
            jax.ShapeDtypeStruct((E, E), F32),
        ),
        in_specs=[vmem] * 6,
        out_specs=(vmem,) * 7,
        compiler_params=pltpu.CompilerParams(vmem_limit_bytes=4 * 1024 * 1024),
    )(*outs)
    pair_next, pair_grad, bias_weight_grad, denoised, token_grad, weight_grad, out_grad = outs
    return (
        pair_next.reshape(S, S, C),
        pair_grad.reshape(S, S, C),
        bias_weight_grad.T,
        denoised,
        token_grad,
        weight_grad,
        out_grad,
    )


def solution(mesh):
    line, col = ("group", "row"), "col"
    return jax.shard_map(
        shards,
        mesh=mesh,
        in_specs=(
            P(line, col, None), P(line, col), P(), P(), P(), P(), P(), P(), P(), P(), P(),
            P(line, None, None), P(line), P(), P(None, None, col), P(col, None),
            P(line, None, None),
        ),
        out_specs=(
            P(line, col, None), P(line, col, None), P(), P(line, col, None),
            P(line, col, None), P(None, line, col), P(col, line),
        ),
        check_vma=False,
    )
```
